32 devices in a mesh: row: 4 (over z), col: 8 (over y, x, core).
Axes of the slice: x: 2, y: 2, z: 4, core: 2. Of those that a mesh axis runs over, the one named last changes fastest.
Arguments:
- hidden_in: bfloat16 [8192, 1536], P(('row', 'col')), may hold values from -6 to 6
- out_grad: bfloat16 [8192, 1536], P(('row', 'col')), may hold values from -6 to 6
- seq_lengths: int32 [4, 16], P('row'), may hold values from 1 to 1024, 2048 in all within a row
- norm1_gain: bfloat16 [1536], P(('row', 'col')), may hold values from 0.25 to 1.75
- q_weight: bfloat16 [1536, 1536], P('row', 'col'), may hold values from -0.15625 to 0.15625
- q_bias: bfloat16 [1536], P(('row', 'col')), may hold values from -3 to 3
- k_weight: bfloat16 [1536, 256], P('row', 'col'), may hold values from -0.15625 to 0.15625
- k_bias: bfloat16 [256], P(('row', 'col')), may hold values from -3 to 3
- v_weight: bfloat16 [1536, 256], P('row', 'col'), may hold values from -0.15625 to 0.15625
- v_bias: bfloat16 [256], P(('row', 'col')), may hold values from -3 to 3
- o_weight: bfloat16 [1536, 1536], P('row', 'col'), may hold values from -0.625 to 0.625
- norm2_gain: bfloat16 [1536], P(('row', 'col')), may hold values from 0.25 to 1.75
- gate_weight: bfloat16 [1536, 8960], P('row', 'col'), may hold values from -0.15625 to 0.15625
- up_weight: bfloat16 [1536, 8960], P('row', 'col'), may hold values from -0.15625 to 0.15625
- down_weight: bfloat16 [8960, 1536], P('col', 'row'), may hold values from -0.375 to 0.375
Outputs:
- layer_out: float32 [8192, 1536], P(('row', 'col'))
- input_grad: float32 [8192, 1536], P(('row', 'col'))
- norm1_gain_grad: float32 [1536], P(('row', 'col'))
- q_weight_grad: float32 [1536, 1536], P('row', 'col')
- q_bias_grad: float32 [1536], P(('row', 'col'))
- k_weight_grad: float32 [1536, 256], P('row', 'col')
- k_bias_grad: float32 [256], P(('row', 'col'))
- v_weight_grad: float32 [1536, 256], P('row', 'col')
- v_bias_grad: float32 [256], P(('row', 'col'))
- o_weight_grad: float32 [1536, 1536], P('row', 'col')
- norm2_gain_grad: float32 [1536], P(('row', 'col'))
- gate_weight_grad: float32 [1536, 8960], P('row', 'col')
- up_weight_grad: float32 [1536, 8960], P('row', 'col')
- down_weight_grad: float32 [8960, 1536], P('col', 'row')
The draws below stay inside these ranges and needn't reach their ends.
Inputs may be any that keep to these rules, and one draw needn't show every extreme that they name: `seq_lengths`: row r lists the lengths of the 16 sequences packed in order into block r of 2048 tokens; they sum to 2048, and the longest is exactly 1024 in every row.
All inputs are finite; a program needn't handle non-finite values.
Results may differ from the reference program's by a relative error of at most 0.03.
Values may be sent and summed in bfloat16 or wider, within the bound.
A program may use at most 192 MiB of HBM per device.

```python
import math
import jax
import jax.numpy as jnp
import numpy as np
from jax import lax

D = 1536
HQ = 12
KVH = 2
HD = 128
FF = 8960
TOK_DEV = 256
MAXLEN = 1024
ROW_TOK = 2048
NSEG = 16
TOKENS = 8192
N_ROW = 4
N_COL = 8


def raised(values, own_key, source, target, blocks, factor):
    def block_of(position):
        return (jnp.arange(values.shape[position]) // (values.shape[position] // blocks)).reshape((-1,) + (1,) * (values.ndim - 1 - position))

    near = jax.random.permutation(own_key, blocks)[block_of(target)]
    far = (block_of(target) + blocks // 2) % blocks
    return jnp.where((block_of(source) == near) | (block_of(source) == far), factor * values, values)


def steps_of(own_key, dims, cuts, smallest, high):
    factor_of, own = 1.0, jax.random.fold_in(own_key, 6)
    for axis_at, blocks in cuts:
        draws = jnp.exp(jax.random.uniform(jax.random.fold_in(own, axis_at), (blocks,), jnp.float32, smallest / len(cuts), high / len(cuts)))
        factor_of = factor_of * jnp.repeat(draws, dims[axis_at] // blocks).reshape([-1 if axis == axis_at else 1 for axis in range(len(dims))])
    return factor_of


def length_profile(number_of, total, most, skew):
    weights = [(1 << 20) // math.isqrt(grade ** skew) + 1 for grade in range(2, number_of + 1)]
    surplus, counts = total - most - (number_of - 1), [1] * (number_of - 1)
    while surplus > 0:
        movable = [i for i in range(number_of - 1) if counts[i] < most]
        mass, budget = sum([weights[i] for i in movable]), surplus
        for i in movable:
            addition = min(most - counts[i], max(1, budget * weights[i] // mass), surplus)
            counts[i] = counts[i] + addition
            surplus = surplus - addition
    return np.array([most] + counts)


def ragged(stream_key, number_of, total, limit, lean):
    if number_of == 2:
        one = jax.random.randint(stream_key, (), max(1, total - limit), min(limit, total - 1) + 1)
        return jnp.stack([one, total - one])
    tallies = jnp.asarray(length_profile(number_of, total, limit, lean), jnp.int32)
    couples = (number_of - 1) // 2
    source_of, receiver = tallies[1:1 + 2 * couples:2], tallies[2:2 + 2 * couples:2]
    slack = jnp.minimum(source_of - 1, limit - receiver)
    shifted = jax.random.randint(jax.random.fold_in(stream_key, 1), (couples,), 0, 1 << 20) % (slack + 1)
    tallies = tallies.at[1:1 + 2 * couples:2].set(source_of - shifted).at[2:2 + 2 * couples:2].set(receiver + shifted)
    return tallies[jax.random.permutation(jax.random.fold_in(stream_key, 2), number_of)]


def scatter_about(key, dims, width, most, pieces=(), kind=jnp.bfloat16):
    entries = width * jax.random.normal(key, dims, jnp.float32)
    if pieces:
        entries = entries * steps_of(key, dims, pieces, -0.22, 0.18)
    return jnp.clip(entries, -most, most).astype(kind)


def gaussian_with(rng, shape, scale, reach, cuts, heavy, kind=jnp.bfloat16):
    drawn = scale * jax.random.normal(rng, shape, jnp.float32)
    if cuts:
        drawn = drawn * steps_of(rng, shape, cuts, -0.22, 0.18)
    return jnp.clip(raised(drawn, jax.random.fold_in(rng, 3), *heavy), -reach, reach).astype(kind)


def setup_inputs(seed: int = 0) -> dict:
    key_list = jax.random.split(jax.random.key(seed), 16)
    return {
        "hidden_in": scatter_about(key_list[0], (TOKENS, D), 1.0, 6.0, ((0, 32),)),
        "out_grad": scatter_about(key_list[1], (TOKENS, D), 1.0, 6.0, ((0, 32),)),
        "seq_lengths": jax.vmap(lambda own: ragged(own, NSEG, ROW_TOK, MAXLEN, 2))(jax.random.split(key_list[2], N_ROW)).reshape((N_ROW, NSEG)).astype(jnp.int32),
        "norm1_gain": jnp.clip(1.0 + 0.15 * jax.random.normal(key_list[3], (D,), jnp.float32), 0.25, 1.75).astype(jnp.bfloat16),
        "q_weight": scatter_about(key_list[4], (D, HQ * HD), D ** -0.5, 0.15625, ((0, 4), (1, 8))),
        "q_bias": scatter_about(key_list[5], (HQ * HD,), 0.5, 3.0, ((0, 32),)),
        "k_weight": scatter_about(key_list[6], (D, KVH * HD), D ** -0.5, 0.15625, ((0, 4), (1, 8))),
        "k_bias": scatter_about(key_list[7], (KVH * HD,), 0.5, 3.0, ((0, 32),)),
        "v_weight": scatter_about(key_list[8], (D, KVH * HD), D ** -0.5, 0.15625, ((0, 4), (1, 8))),
        "v_bias": scatter_about(key_list[9], (KVH * HD,), 0.5, 3.0, ((0, 32),)),
        "o_weight": scatter_about(key_list[10], (HQ * HD, D), (HQ * HD // 16) ** -0.5, 0.625, ((0, 4), (1, 8))),
        "norm2_gain": jnp.clip(1.0 + 0.15 * jax.random.normal(key_list[11], (D,), jnp.float32), 0.25, 1.75).astype(jnp.bfloat16),
        "gate_weight": scatter_about(key_list[12], (D, FF), D ** -0.5, 0.15625, ((0, 4), (1, 8))),
        "up_weight": scatter_about(key_list[13], (D, FF), D ** -0.5, 0.15625, ((0, 4), (1, 8))),
        "down_weight": gaussian_with(key_list[14], (FF, D), (FF // 16) ** -0.5, 0.375, ((0, 8), (1, 4)), (0, 1, 8, 2.0)),
    }


EPSILON = 1e-06
ROPE_BASE = 1000000.0
HIGHEST = lax.Precision.HIGHEST

@jax.custom_vjp
def low(v):
    return lax.optimization_barrier(v.astype(jnp.bfloat16)).astype(jnp.float32)

@jax.custom_vjp
def low_back(v):
    return v

def low_keep(v):
    return (low(v), None)

def low_pass(kept, grad):
    return (grad,)

def back_keep(v):
    return (v, None)

def back_low(kept, grad):
    return (low(grad),)
low.defvjp(low_keep, low_pass)
low_back.defvjp(back_keep, back_low)

def matmul_high(left, right):
    return jnp.dot(left, right, precision=HIGHEST, preferred_element_type=jnp.float32)

def seq_starts(slots, lengths):
    bounds = jnp.cumsum(lengths).astype(jnp.int32)
    picked = jnp.where(bounds[None, :] <= slots[:, None], lengths[None, :], 0)
    return lax.optimization_barrier(jnp.sum(picked, axis=1)).astype(jnp.int32)

def rope_tables(positions, head_dim):
    steps_up = jnp.arange(head_dim // 2, dtype=jnp.float32)
    freqs = jnp.exp(-math.log(ROPE_BASE) * (2.0 * steps_up / head_dim))
    angles = positions.astype(jnp.float32)[:, None] * freqs[None, :]
    angles = jnp.concatenate([angles, angles], axis=1)
    return (jnp.cos(angles)[:, None, :], jnp.sin(angles)[:, None, :])

def rotate_pairs(values, cosines, sines):
    half_dim = values.shape[-1] // 2
    turned = jnp.concatenate([-values[..., half_dim:], values[..., :half_dim]], axis=-1)
    return values * cosines + turned * sines

def rms_scale(values):
    return lax.rsqrt(lax.optimization_barrier(jnp.mean(values * values, axis=-1, keepdims=True)) + EPSILON)

def layer_rows(params, inputs, lengths):
    norm1_gain, q_weight, q_bias, k_weight, k_bias, v_weight, v_bias, o_weight, norm2_gain, gate_weight, up_weight, down_weight = params
    row_count = inputs.shape[0]
    slots = jnp.arange(row_count, dtype=jnp.int32)
    starts = seq_starts(slots, lengths)
    cosines, sines = rope_tables(slots - starts, HD)
    normed_one = low(inputs * rms_scale(inputs) * norm1_gain)
    query_base = low_back(matmul_high(normed_one, q_weight) + q_bias)
    key_base = low_back(matmul_high(normed_one, k_weight) + k_bias)
    values = low_back(low(matmul_high(normed_one, v_weight) + v_bias))
    queries = low_back(low(rotate_pairs(query_base.reshape(row_count, HQ, HD), cosines, sines)))
    keys = low_back(low(rotate_pairs(key_base.reshape(row_count, KVH, HD), cosines, sines)))
    group_size = HQ // KVH
    queries = queries.reshape(row_count, KVH, group_size, HD)
    scores = jnp.einsum('tkgd,skd->kgts', queries, keys, precision=HIGHEST) * (1.0 / math.sqrt(HD))
    scores = low_back(scores)
    visible = (starts[:, None] == starts[None, :]) & (slots[None, :] <= slots[:, None])
    scores = jnp.where(visible, scores, -jnp.inf)
    probs = low(jax.nn.softmax(scores, axis=-1))
    mixed = jnp.einsum('kgts,skd->tkgd', probs, values.reshape(row_count, KVH, HD), precision=HIGHEST)
    mixed = low_back(low(mixed.reshape(row_count, HQ * HD)))
    attended = low_back(matmul_high(mixed, o_weight))
    residual = inputs + attended
    normed_two = low(residual * rms_scale(residual) * norm2_gain)
    gate_act = low_back(matmul_high(normed_two, gate_weight))
    up_act = low_back(matmul_high(normed_two, up_weight))
    hidden = low(jax.nn.silu(gate_act) * up_act)
    return residual + matmul_high(hidden, down_weight)

def reference(hidden_in, out_grad, seq_lengths, norm1_gain, q_weight, q_bias, k_weight, k_bias, v_weight, v_bias, o_weight, norm2_gain, gate_weight, up_weight, down_weight):
    params = tuple((member.astype(jnp.float32) for member in (norm1_gain, q_weight, q_bias, k_weight, k_bias, v_weight, v_bias, o_weight, norm2_gain, gate_weight, up_weight, down_weight)))
    inputs = hidden_in.astype(jnp.float32)
    row_tokens = TOK_DEV * N_COL

    def forward(inputs, params):
        blocks = inputs.reshape(N_ROW, row_tokens, D)

        def one_row(row_pair):
            return layer_rows(params, row_pair[0], row_pair[1])
        outputs = lax.map(jax.checkpoint(one_row), (blocks, seq_lengths))
        return outputs.reshape(N_ROW * row_tokens, D)
    result, pullback = jax.vjp(forward, inputs, params)
    input_grad, param_grads = pullback(out_grad.astype(jnp.float32))
    return (result, input_grad, param_grads[0], param_grads[1], param_grads[2], param_grads[3], param_grads[4], param_grads[5], param_grads[6], param_grads[7], param_grads[8], param_grads[9], param_grads[10], param_grads[11])
```

```python
import math

import jax
import jax.numpy as jnp
from jax import lax
from jax.sharding import PartitionSpec as P

HQ = 12
KVH = 2
HD = 128
MAXLEN = 1024

EPSILON = 1e-06
ROPE_BASE = 1000000.0
BF16 = jnp.bfloat16
F32 = jnp.float32


def seq_starts(slots, lengths):
    bounds = jnp.cumsum(lengths)
    picked = jnp.where(bounds[None, :] <= slots[:, None], lengths[None, :], 0)
    return jnp.sum(picked, axis=1)


def rope_tables(positions, head_dim):
    steps_up = jnp.arange(head_dim // 2, dtype=F32)
    freqs = jnp.exp(-math.log(ROPE_BASE) * (2.0 * steps_up / head_dim))
    angles = positions.astype(F32)[:, None] * freqs[None, :]
    angles = jnp.concatenate([angles, angles], axis=1)
    return (jnp.cos(angles)[:, None, :], jnp.sin(angles)[:, None, :])


def rotate_pairs(values, cosines, sines):
    half_dim = values.shape[-1] // 2
    turned = jnp.concatenate([-values[..., half_dim:], values[..., :half_dim]], axis=-1)
    return values * cosines + turned * sines


def rotate_back(grads_in, cosines, sines):
    half_dim = grads_in.shape[-1] // 2
    moved = grads_in * sines
    return grads_in * cosines + jnp.concatenate(
        [moved[..., half_dim:], -moved[..., :half_dim]], axis=-1
    )


def rms_scale(values):
    return lax.rsqrt(jnp.mean(values * values, axis=-1, keepdims=True) + EPSILON)


def dot_nn(left, right):
    return lax.dot_general(left, right, (((1,), (0,)), ((), ())), preferred_element_type=F32)


def dot_tn(left, right):
    return lax.dot_general(left, right, (((0,), (0,)), ((), ())), preferred_element_type=F32)


def dot_nt(left, right):
    return lax.dot_general(left, right, (((1,), (1,)), ((), ())), preferred_element_type=F32)


def rounded_wide(values):
    return lax.optimization_barrier(values.astype(BF16)).astype(F32)


def masked_scores(query_heads, keys_window, visible, score_scale):
    scores = jnp.einsum("tkgd,skd->kgts", query_heads, keys_window, preferred_element_type=F32)
    return jnp.where(visible, scores * score_scale, -jnp.inf)


def gather_row(block):
    return lax.all_gather(block, "row", axis=1, tiled=True)


def gather_col(block):
    return lax.all_gather(block, "col", axis=0, tiled=True)


def scatter_row(full):
    return lax.psum_scatter(full.astype(BF16), "row", scatter_dimension=1, tiled=True)


def scatter_col(full):
    return lax.psum_scatter(full.astype(BF16), "col", scatter_dimension=0, tiled=True)


def shards(
    hidden_in,
    out_grad,
    seq_lengths,
    norm1_gain,
    q_weight,
    q_bias,
    k_weight,
    k_bias,
    v_weight,
    v_bias,
    o_weight,
    norm2_gain,
    gate_weight,
    up_weight,
    down_weight,
):
    row_parts = lax.axis_size("row")
    col_parts = lax.axis_size("col")
    col_place = lax.axis_index("col")
    depth_own = q_weight.shape[0]
    depth = depth_own * row_parts
    q_own, k_own = q_weight.shape[1], k_weight.shape[1]
    smalls = (q_bias, k_bias, v_bias, norm1_gain, norm2_gain)
    small_sizes = [member.shape[0] for member in smalls]
    small_rows = 16
    packed_small = jnp.concatenate(smalls)
    packed_small = jnp.pad(packed_small, (0, small_rows * depth_own - packed_small.shape[0]))
    packed = jnp.concatenate(
        [
            q_weight.T,
            k_weight.T,
            v_weight.T,
            o_weight.T,
            packed_small.reshape(small_rows, depth_own),
        ],
        axis=0,
    )
    pack_rows = packed.shape[0]
    gathered = gather_col(gather_row(packed)).reshape(col_parts, pack_rows, depth)
    cuts = [0, q_own, q_own + k_own, q_own + 2 * k_own, 2 * q_own + 2 * k_own, pack_rows]
    query_t, key_t, value_t, output_t, small_t = (
        gathered[:, cuts[i] : cuts[i + 1], :] for i in range(5)
    )
    query_t = query_t.reshape(-1, depth)
    key_t = key_t.reshape(-1, depth)
    value_t = value_t.reshape(-1, depth)
    output_t = output_t.reshape(-1, depth)
    small_flat = small_t.reshape(col_parts, small_rows, row_parts, depth_own)
    small_flat = small_flat.transpose(2, 0, 1, 3).reshape(row_parts * col_parts, -1)
    small_full, offset = [], 0
    for size in small_sizes:
        small_full.append(small_flat[:, offset : offset + size].reshape(-1))
        offset += size
    query_offset, key_offset, value_offset, first_gain, second_gain = small_full

    gate_t = gather_row(gate_weight.T)
    up_t = gather_row(up_weight.T)
    down_block = gather_row(down_weight)

    own_rows = hidden_in.shape[0]
    row_tokens = own_rows * col_parts
    lengths = seq_lengths[0]
    query_slots = col_place * own_rows + jnp.arange(own_rows, dtype=jnp.int32)
    query_starts = seq_starts(query_slots, lengths)
    cosines, sines = rope_tables(query_slots - query_starts, HD)
    group_size = HQ // KVH
    score_scale = 1.0 / math.sqrt(HD)
    inputs_wide = hidden_in.astype(F32)
    first_rms = rms_scale(inputs_wide)
    first_unit = inputs_wide * first_rms
    first_normed = (first_unit * first_gain.astype(F32)).astype(BF16)
    query_base = dot_nt(first_normed, query_t) + query_offset.astype(F32)
    key_base = dot_nt(first_normed, key_t) + key_offset.astype(F32)
    value_own = (dot_nt(first_normed, value_t) + value_offset.astype(F32)).astype(BF16)
    queries = rotate_pairs(query_base.reshape(own_rows, HQ, HD), cosines, sines).astype(BF16)
    keys_own = rotate_pairs(key_base.reshape(own_rows, KVH, HD), cosines, sines).astype(BF16)
    both_all = gather_col(
        jnp.concatenate([keys_own.reshape(own_rows, KVH * HD), value_own], axis=1)
    )
    window = min(own_rows + MAXLEN, row_tokens)
    window_start = jnp.clip(col_place * own_rows - MAXLEN, 0, row_tokens - window)
    key_slots = window_start + jnp.arange(window, dtype=jnp.int32)
    key_starts = seq_starts(key_slots, lengths)
    visible = (query_starts[:, None] == key_starts[None, :]) & (
        key_slots[None, :] <= query_slots[:, None]
    )
    both_window = lax.dynamic_slice_in_dim(both_all, window_start, window, 0)
    keys_window = both_window[:, : KVH * HD].reshape(window, KVH, HD)
    values_window = both_window[:, KVH * HD :].reshape(window, KVH, HD)
    query_heads = queries.reshape(own_rows, KVH, group_size, HD)
    scores = masked_scores(query_heads, keys_window, visible, score_scale)
    peak = jnp.max(scores, axis=-1, keepdims=True)
    expanded = jnp.exp(scores - peak)
    totals = jnp.sum(expanded, axis=-1, keepdims=True)
    probs = expanded / totals
    log_total = peak + jnp.log(totals)
    mixed = jnp.einsum(
        "kgts,skd->tkgd", probs.astype(BF16), values_window, preferred_element_type=F32
    )
    mixed = mixed.reshape(own_rows, HQ * HD).astype(BF16)
    residual = inputs_wide + dot_nt(mixed, output_t)
    second_rms = rms_scale(residual)
    second_unit = residual * second_rms
    second_normed = (second_unit * second_gain.astype(F32)).astype(BF16)
    normed_rows = gather_col(second_normed)
    out_rows = gather_col(out_grad)
    gate_act = dot_nt(normed_rows, gate_t)
    up_act = dot_nt(normed_rows, up_t)
    sigmoid_gate = jax.nn.sigmoid(gate_act)
    silu_gate = gate_act * sigmoid_gate
    hidden = (silu_gate * up_act).astype(BF16)
    down_grad = dot_tn(hidden, out_rows)
    hidden_grad = dot_nt(out_rows, down_block)
    up_grad_act = (hidden_grad * silu_gate).astype(BF16)
    gate_grad_act = (
        hidden_grad * up_act * sigmoid_gate * (1.0 + gate_act * (1.0 - sigmoid_gate))
    ).astype(BF16)
    normed_grad = scatter_col(dot_nn(gate_grad_act, gate_t) + dot_nn(up_grad_act, up_t)).astype(
        F32
    )
    branch_out = scatter_col(dot_nn(hidden, down_block)).astype(F32)
    layer_out = residual + branch_out
    gate_grad_t = dot_tn(gate_grad_act, normed_rows)
    up_grad_t = dot_tn(up_grad_act, normed_rows)
    second_gain_grad = jnp.sum(normed_grad * second_unit, axis=0)
    unit_grad = normed_grad * second_gain.astype(F32)
    residual_grad = out_grad.astype(F32) + second_rms * (
        unit_grad - second_unit * jnp.mean(unit_grad * second_unit, axis=-1, keepdims=True)
    )
    attended_grad = residual_grad.astype(BF16)
    mixed_grad = dot_nn(attended_grad, output_t).astype(BF16)
    grad_heads = mixed_grad.reshape(own_rows, KVH, group_size, HD)
    scores = masked_scores(query_heads, keys_window, visible, score_scale)
    probs = jnp.exp(scores - log_total)
    prob_grad = jnp.einsum(
        "tkgd,skd->kgts", grad_heads, values_window, preferred_element_type=F32
    )
    value_part = jnp.einsum(
        "kgts,tkgd->skd", probs.astype(BF16), grad_heads, preferred_element_type=F32
    )
    score_grad = (
        probs * (prob_grad - jnp.sum(probs * prob_grad, axis=-1, keepdims=True))
    ).astype(BF16)
    query_grad = (
        jnp.einsum("kgts,skd->tkgd", score_grad, keys_window, preferred_element_type=F32)
        * score_scale
    )
    key_part = (
        jnp.einsum("kgts,tkgd->skd", score_grad, query_heads, preferred_element_type=F32)
        * score_scale
    )
    both_part = jnp.concatenate(
        [key_part.reshape(window, KVH * HD), value_part.reshape(window, KVH * HD)], axis=1
    ).astype(BF16)
    both_rows = lax.dynamic_update_slice_in_dim(
        jnp.zeros((row_tokens, 2 * KVH * HD), BF16), both_part, window_start, 0
    )
    both_grad = scatter_col(both_rows).astype(F32)
    key_grad, value_grad = both_grad[:, : KVH * HD], both_grad[:, KVH * HD :]
    query_wide = rounded_wide(query_grad.reshape(own_rows, HQ, HD))
    query_base_grad = (
        rotate_back(query_wide, cosines, sines).reshape(own_rows, HQ * HD).astype(BF16)
    )
    key_wide = rounded_wide(key_grad.reshape(own_rows, KVH, HD))
    key_base_grad = (
        rotate_back(key_wide, cosines, sines).reshape(own_rows, KVH * HD).astype(BF16)
    )
    value_base_grad = value_grad.astype(BF16)
    query_b_grad = jnp.sum(query_base_grad.astype(F32), axis=0)
    key_b_grad = jnp.sum(key_base_grad.astype(F32), axis=0)
    value_b_grad = jnp.sum(value_base_grad.astype(F32), axis=0)
    first_normed_grad = (
        dot_nn(query_base_grad, query_t)
        + dot_nn(key_base_grad, key_t)
        + dot_nn(value_base_grad, value_t)
    )
    first_gain_grad = jnp.sum(first_normed_grad * first_unit, axis=0)
    first_unit_grad = first_normed_grad * first_gain.astype(F32)
    input_grad = residual_grad + first_rms * (
        first_unit_grad
        - first_unit * jnp.mean(first_unit_grad * first_unit, axis=-1, keepdims=True)
    )
    small_grads = (query_b_grad, key_b_grad, value_b_grad, first_gain_grad, second_gain_grad)
    small_flat = jnp.concatenate(
        [member.reshape(row_parts * col_parts, -1) for member in small_grads], axis=1
    )
    small_flat = jnp.pad(
        small_flat, ((0, 0), (0, small_rows * depth_own - small_flat.shape[1]))
    ).reshape(row_parts, col_parts, small_rows, depth_own)
    small_flat = small_flat.transpose(1, 2, 0, 3).reshape(col_parts, small_rows, depth)
    packed_grads = jnp.concatenate(
        [
            dot_tn(query_base_grad, first_normed).astype(BF16).reshape(col_parts, q_own, depth),
            dot_tn(key_base_grad, first_normed).astype(BF16).reshape(col_parts, k_own, depth),
            dot_tn(value_base_grad, first_normed).astype(BF16).reshape(col_parts, k_own, depth),
            dot_tn(attended_grad, mixed).astype(BF16).reshape(col_parts, q_own, depth),
            small_flat.astype(BF16),
        ],
        axis=1,
    ).reshape(col_parts * pack_rows, depth)
    packed_out = scatter_row(scatter_col(packed_grads)).astype(F32)
    query_w_out, key_w_out, value_w_out, output_w_out, small_out = (
        packed_out[cuts[i] : cuts[i + 1]] for i in range(5)
    )
    small_out = small_out.reshape(-1)
    small_list, offset = [], 0
    for size in small_sizes:
        small_list.append(small_out[offset : offset + size])
        offset += size
    return (
        layer_out,
        input_grad,
        small_list[3],
        query_w_out.T,
        small_list[0],
        key_w_out.T,
        small_list[1],
        value_w_out.T,
        small_list[2],
        output_w_out.T,
        small_list[4],
        scatter_row(gate_grad_t).astype(F32).T,
        scatter_row(up_grad_t).astype(F32).T,
        scatter_row(down_grad).astype(F32),
    )


def solution(mesh):
    in_specs = (
        P(("row", "col"), None),
        P(("row", "col"), None),
        P("row", None),
        P(("row", "col")),
        P("row", "col"),
        P(("row", "col")),
        P("row", "col"),
        P(("row", "col")),
        P("row", "col"),
        P(("row", "col")),
        P("row", "col"),
        P(("row", "col")),
        P("row", "col"),
        P("row", "col"),
        P("col", "row"),
    )
    out_specs = (
        P(("row", "col"), None),
        P(("row", "col"), None),
        P(("row", "col")),
        P("row", "col"),
        P(("row", "col")),
        P("row", "col"),
        P(("row", "col")),
        P("row", "col"),
        P(("row", "col")),
        P("row", "col"),
        P(("row", "col")),
        P("row", "col"),
        P("row", "col"),
        P("col", "row"),
    )
    return jax.shard_map(shards, mesh=mesh, in_specs=in_specs, out_specs=out_specs, check_vma=False)
```

```python
import functools
import math

import jax
import jax.numpy as jnp
from jax import lax
from jax.experimental import pallas as pl
from jax.experimental.pallas import tpu as pltpu
from jax.sharding import PartitionSpec as P

HQ = 12
KVH = 2
HD = 128
MAXLEN = 1024

EPSILON = 1e-06
ROPE_BASE = 1000000.0
BF16 = jnp.bfloat16
F32 = jnp.float32
MESH = pl.DeviceIdType.MESH


def seq_starts(slots, lengths):
    bounds = jnp.cumsum(lengths)
    picked = jnp.where(bounds[None, :] <= slots[:, None], lengths[None, :], 0)
    return jnp.sum(picked, axis=1)


def rope_tables(positions, head_dim):
    steps_up = jnp.arange(head_dim // 2, dtype=F32)
    freqs = jnp.exp(-math.log(ROPE_BASE) * (2.0 * steps_up / head_dim))
    angles = positions.astype(F32)[:, None] * freqs[None, :]
    angles = jnp.concatenate([angles, angles], axis=1)
    return (jnp.cos(angles)[:, None, :], jnp.sin(angles)[:, None, :])


def rotate_pairs(values, cosines, sines):
    half_dim = values.shape[-1] // 2
    turned = jnp.concatenate([-values[..., half_dim:], values[..., :half_dim]], axis=-1)
    return values * cosines + turned * sines


def rotate_back(grads_in, cosines, sines):
    half_dim = grads_in.shape[-1] // 2
    moved = grads_in * sines
    return grads_in * cosines + jnp.concatenate(
        [moved[..., half_dim:], -moved[..., :half_dim]], axis=-1
    )


def rms_scale(values):
    return lax.rsqrt(jnp.mean(values * values, axis=-1, keepdims=True) + EPSILON)


def dot_nn(left, right):
    return lax.dot_general(left, right, (((1,), (0,)), ((), ())), preferred_element_type=F32)


def dot_tn(left, right):
    return lax.dot_general(left, right, (((0,), (0,)), ((), ())), preferred_element_type=F32)


def dot_nt(left, right):
    return lax.dot_general(left, right, (((1,), (1,)), ((), ())), preferred_element_type=F32)


def rounded_wide(values):
    return lax.optimization_barrier(values.astype(BF16)).astype(F32)


def masked_scores(query_heads, keys_window, visible, score_scale):
    scores = jnp.einsum("tkgd,skd->kgts", query_heads, keys_window, preferred_element_type=F32)
    return jnp.where(visible, scores * score_scale, -jnp.inf)


def plane_places():
    me = lax.axis_index("col")
    chip, core = me // 2, me % 2
    low, high = chip % 2, chip // 2
    beside = high * 2 + (1 - low)
    above = (1 - high) * 2 + low
    across = (1 - high) * 2 + (1 - low)
    return chip, beside, above, across, core


def greet(peers):
    barrier = pltpu.get_barrier_semaphore()
    for peer in peers:
        pl.semaphore_signal(barrier, inc=1, device_id={"col": peer}, device_id_type=MESH)
    pl.semaphore_wait(barrier, len(peers))


def plane_gather_kernel(count, *refs):
    ins, outs = refs[:count], refs[count : 2 * count]
    send_sem, recv_sem, own_sem = refs[2 * count :]
    chip, beside, above, across, core = plane_places()
    mine = chip * 2 + core
    partner = chip * 2 + 1 - core
    to_x, to_y = beside * 2 + core, above * 2 + core
    greet((partner, to_x, to_y))

    def view(i, slot, part):
        size = ins[i].shape[1]
        half = size // 2
        if part is None:
            return outs[i].at[:, pl.ds(pl.multiple_of(slot * size, size), size), :]
        return outs[i].at[:, pl.ds(pl.multiple_of(slot * size + part * half, half), half), :]

    def copies(k, slot, part, peer, own=False):
        return [
            pltpu.make_async_remote_copy(
                src_ref=ins[i] if own else view(i, slot, part),
                dst_ref=view(i, slot, part),
                send_sem=send_sem.at[i, k],
                recv_sem=recv_sem.at[i, k],
                device_id={"col": peer},
                device_id_type=MESH,
            )
            for i in range(count)
        ]

    def start(cs):
        for c in cs:
            c.start()

    def wait_recv(cs):
        for c in cs:
            c.wait_recv()

    sent = [
        copies(1, mine, None, to_x, True),
        copies(2, mine, None, to_y, True),
        copies(0, mine, None, partner, True),
    ]
    for c in sent:
        start(c)
    own = [
        pltpu.make_async_copy(ins[i], view(i, mine, None), own_sem.at[i]) for i in range(count)
    ]
    start(own)
    other = 1 - core
    wait_recv(copies(1, to_x, None, to_x))
    more = [copies(3, to_x, 0, to_y), copies(5, to_x, None, partner)]
    for c in more:
        start(c)
    sent += more
    wait_recv(copies(2, to_y, None, to_y))
    more = [copies(4, to_y, 1, to_x), copies(6, to_y, None, partner)]
    for c in more:
        start(c)
    sent += more
    far = across * 2 + core
    wait_recv(copies(3, far, 0, to_y))
    more = [copies(7, far, 0, partner)]
    start(more[0])
    sent += more
    wait_recv(copies(4, far, 1, to_x))
    more = [copies(8, far, 1, partner)]
    start(more[0])
    sent += more
    wait_recv(copies(0, partner, None, partner))
    wait_recv(copies(5, beside * 2 + other, None, partner))
    wait_recv(copies(6, above * 2 + other, None, partner))
    wait_recv(copies(7, across * 2 + other, 0, partner))
    wait_recv(copies(8, across * 2 + other, 1, partner))
    for cs in sent:
        for c in cs:
            c.wait_send()
    for c in own:
        c.wait()


def plane_gather(shards, ident):
    count = len(shards)
    parts = lax.axis_size("col")
    outs = [
        jax.ShapeDtypeStruct((s.shape[0], s.shape[1] * parts, s.shape[2]), s.dtype)
        for s in shards
    ]
    return pl.pallas_call(
        functools.partial(plane_gather_kernel, count),
        out_shape=outs,
        in_specs=[pl.BlockSpec(memory_space=pl.ANY)] * count,
        out_specs=[pl.BlockSpec(memory_space=pl.ANY)] * count,
        scratch_shapes=[
            pltpu.SemaphoreType.DMA((count, 9)),
            pltpu.SemaphoreType.DMA((count, 9)),
            pltpu.SemaphoreType.DMA((count,)),
        ],
        compiler_params=pltpu.CompilerParams(collective_id=ident, has_side_effects=True),
        name="plane_gather",
    )(*shards)


def plane_scatter_kernel(count, *refs):
    ins, outs = refs[:count], refs[count : 2 * count]
    scratch = refs[2 * count :]
    near, made, side, land = (scratch[i * count : (i + 1) * count] for i in range(4))
    send_sem, recv_sem = scratch[4 * count :]
    chip, beside, above, across, core = plane_places()
    partner = chip * 2 + 1 - core
    to_x, to_y = beside * 2 + core, above * 2 + core
    greet((partner, to_x, to_y))
    order = (across, beside, above, chip)

    def rows(i, slot):
        size = outs[i].shape[1]
        return pl.ds(pl.multiple_of(slot * size, size), size)

    def half(i, part):
        size = outs[i].shape[1] // 2
        return pl.ds(part * size, size)

    def remote(i, k, src, dst, peer):
        return pltpu.make_async_remote_copy(
            src_ref=src,
            dst_ref=dst,
            send_sem=send_sem.at[i, k],
            recv_sem=recv_sem.at[i, k],
            device_id={"col": peer},
            device_id_type=MESH,
        )

    def near_copy(i, j):
        return remote(
            i, j, ins[i].at[:, rows(i, order[j] * 2 + 1 - core), :], near[i].at[j], partner
        )

    def side_copy(i, part):
        return remote(
            i, 4 + part, made[i].at[0, :, half(i, part), :], side[i].at[part],
            to_x if part == 0 else to_y,
        )

    def land_copy(i, which, part):
        return remote(
            i, 6 + which * 2 + part, made[i].at[1 + which, :, half(i, part), :],
            land[i].at[which, :, half(i, part), :], to_x if which == 0 else to_y,
        )

    step = 16

    def each(i, size, body):
        def tile(t, _):
            body(pl.multiple_of(t * step, step))
            return 0

        lax.fori_loop(0, size // step, tile, 0)

    def combine(i, j):
        size = outs[i].shape[1]
        first = (order[j] * 2 + core) * size

        def body(at):
            for a in range(outs[i].shape[0]):
                left = ins[i][a, pl.ds(pl.multiple_of(first + at, step), step), :].astype(F32)
                right = near[i][j, a, pl.ds(at, step), :].astype(F32)
                made[i][j, a, pl.ds(at, step), :] = (left + right).astype(BF16)

        each(i, size, body)

    def fold(i, which, part):
        size = outs[i].shape[1] // 2

        def body(at):
            at2 = pl.multiple_of(part * size + at, step)
            for a in range(outs[i].shape[0]):
                left = made[i][1 + which, a, pl.ds(at2, step), :].astype(F32)
                right = side[i][1 - which, a, pl.ds(at, step), :].astype(F32)
                made[i][1 + which, a, pl.ds(at2, step), :] = (left + right).astype(BF16)

        each(i, size, body)

    every = range(count)
    for j in range(4):
        for i in every:
            near_copy(i, j).start()
    for i in every:
        near_copy(i, 0).wait_recv()
        combine(i, 0)
        side_copy(i, 0).start()
        side_copy(i, 1).start()
    for i in every:
        near_copy(i, 1).wait_recv()
        combine(i, 1)
        land_copy(i, 0, 0).start()
    for i in every:
        near_copy(i, 2).wait_recv()
        combine(i, 2)
        land_copy(i, 1, 1).start()
    for i in every:
        side_copy(i, 0).wait_recv()
        fold(i, 1, 0)
        land_copy(i, 1, 0).start()
        side_copy(i, 1).wait_recv()
        fold(i, 0, 1)
        land_copy(i, 0, 1).start()
    for i in every:
        near_copy(i, 3).wait_recv()
    for i in every:
        for which in range(2):
            for part in range(2):
                land_copy(i, which, part).wait_recv()
        size = outs[i].shape[1]
        first = (chip * 2 + core) * size

        def body(at, i=i, first=first):
            for a in range(outs[i].shape[0]):
                spot = pl.ds(at, step)
                total = ins[i][a, pl.ds(pl.multiple_of(first + at, step), step), :].astype(F32)
                total += near[i][3, a, spot, :].astype(F32)
                total += land[i][0, a, spot, :].astype(F32)
                total += land[i][1, a, spot, :].astype(F32)
                outs[i][a, spot, :] = total.astype(outs[i].dtype)

        each(i, size, body)
    for i in every:
        for j in range(4):
            near_copy(i, j).wait_send()
        for part in range(2):
            side_copy(i, part).wait_send()
            for which in range(2):
                land_copy(i, which, part).wait_send()


def plane_scatter(fulls, ident, out_dtype=F32):
    count = len(fulls)
    parts = lax.axis_size("col")
    shapes = [(f.shape[0], f.shape[1] // parts, f.shape[2]) for f in fulls]
    scratch = []
    scratch += [pltpu.VMEM((4,) + s, BF16) for s in shapes]
    scratch += [pltpu.VMEM((3,) + s, BF16) for s in shapes]
    scratch += [pltpu.VMEM((2, s[0], s[1] // 2, s[2]), BF16) for s in shapes]
    scratch += [pltpu.VMEM((2,) + s, BF16) for s in shapes]
    return pl.pallas_call(
        functools.partial(plane_scatter_kernel, count),
        out_shape=[jax.ShapeDtypeStruct(s, out_dtype) for s in shapes],
        in_specs=[pl.BlockSpec(memory_space=pltpu.VMEM)] * count,
        out_specs=[pl.BlockSpec(memory_space=pltpu.VMEM)] * count,
        scratch_shapes=scratch
        + [pltpu.SemaphoreType.DMA((count, 10)), pltpu.SemaphoreType.DMA((count, 10))],
        compiler_params=pltpu.CompilerParams(collective_id=ident, has_side_effects=True),
        name="plane_scatter",
    )(*fulls)


def gather_row(block):
    return lax.all_gather(block, "row", axis=block.ndim - 1, tiled=True)


def scatter_row(full):
    return lax.psum_scatter(
        full.astype(BF16), "row", scatter_dimension=full.ndim - 1, tiled=True
    )


def gather_col(blocks, ident):
    if lax.axis_size("col") == 8:
        return plane_gather(blocks, ident)
    return [lax.all_gather(block, "col", axis=1, tiled=True) for block in blocks]


def scatter_col(fulls, ident):
    fulls = [full.astype(BF16) for full in fulls]
    if lax.axis_size("col") == 8:
        return plane_scatter(fulls, ident)
    return [
        lax.psum_scatter(full, "col", scatter_dimension=1, tiled=True).astype(F32)
        for full in fulls
    ]


def shards(
    hidden_in,
    out_grad,
    seq_lengths,
    norm1_gain,
    q_weight,
    q_bias,
    k_weight,
    k_bias,
    v_weight,
    v_bias,
    o_weight,
    norm2_gain,
    gate_weight,
    up_weight,
    down_weight,
):
    row_parts = lax.axis_size("row")
    col_parts = lax.axis_size("col")
    col_place = lax.axis_index("col")
    depth_own = q_weight.shape[0]
    depth = depth_own * row_parts
    q_own, k_own = q_weight.shape[1], k_weight.shape[1]
    smalls = (q_bias, k_bias, v_bias, norm1_gain, norm2_gain)
    small_sizes = [member.shape[0] for member in smalls]
    packed_small = jnp.concatenate(smalls)
    packed_small = jnp.pad(packed_small, (0, k_own * depth_own - packed_small.shape[0]))
    wide_own = gather_row(jnp.stack([q_weight.T, o_weight.T]))
    thin_own = gather_row(
        jnp.stack([k_weight.T, v_weight.T, packed_small.reshape(k_own, depth_own)])
    )
    wide_full, thin_full = gather_col([wide_own, thin_own], 1)
    query_t, output_t = wide_full[0], wide_full[1]
    key_t, value_t = thin_full[0], thin_full[1]
    small_flat = thin_full[2].reshape(col_parts, k_own, row_parts, depth_own)
    small_flat = small_flat.transpose(2, 0, 1, 3).reshape(row_parts * col_parts, -1)
    small_full, offset = [], 0
    for size in small_sizes:
        small_full.append(small_flat[:, offset : offset + size].reshape(-1))
        offset += size
    query_offset, key_offset, value_offset, first_gain, second_gain = small_full

    gate_t = gather_row(gate_weight.T)
    up_t = gather_row(up_weight.T)
    down_block = gather_row(down_weight)

    own_rows = hidden_in.shape[0]
    row_tokens = own_rows * col_parts
    lengths = seq_lengths[0]
    query_slots = col_place * own_rows + jnp.arange(own_rows, dtype=jnp.int32)
    query_starts = seq_starts(query_slots, lengths)
    cosines, sines = rope_tables(query_slots - query_starts, HD)
    group_size = HQ // KVH
    score_scale = 1.0 / math.sqrt(HD)
    inputs_wide = hidden_in.astype(F32)
    first_rms = rms_scale(inputs_wide)
    first_unit = inputs_wide * first_rms
    first_normed = (first_unit * first_gain.astype(F32)).astype(BF16)
    query_base = dot_nt(first_normed, query_t) + query_offset.astype(F32)
    key_base = dot_nt(first_normed, key_t) + key_offset.astype(F32)
    value_own = (dot_nt(first_normed, value_t) + value_offset.astype(F32)).astype(BF16)
    queries = rotate_pairs(query_base.reshape(own_rows, HQ, HD), cosines, sines).astype(BF16)
    keys_own = rotate_pairs(key_base.reshape(own_rows, KVH, HD), cosines, sines).astype(BF16)
    both_own = jnp.concatenate([keys_own.reshape(own_rows, KVH * HD), value_own], axis=1)
    both_all = gather_col([both_own[None]], 2)[0][0]
    window = min(own_rows + MAXLEN, row_tokens)
    window_start = jnp.clip(col_place * own_rows - MAXLEN, 0, row_tokens - window)
    key_slots = window_start + jnp.arange(window, dtype=jnp.int32)
    key_starts = seq_starts(key_slots, lengths)
    visible = (query_starts[:, None] == key_starts[None, :]) & (
        key_slots[None, :] <= query_slots[:, None]
    )
    both_window = lax.dynamic_slice_in_dim(both_all, window_start, window, 0)
    keys_window = both_window[:, : KVH * HD].reshape(window, KVH, HD)
    values_window = both_window[:, KVH * HD :].reshape(window, KVH, HD)
    query_heads = queries.reshape(own_rows, KVH, group_size, HD)
    scores = masked_scores(query_heads, keys_window, visible, score_scale)
    peak = jnp.max(scores, axis=-1, keepdims=True)
    expanded = jnp.exp(scores - peak)
    totals = jnp.sum(expanded, axis=-1, keepdims=True)
    probs = expanded / totals
    log_total = peak + jnp.log(totals)
    mixed = jnp.einsum(
        "kgts,skd->tkgd", probs.astype(BF16), values_window, preferred_element_type=F32
    )
    mixed = mixed.reshape(own_rows, HQ * HD).astype(BF16)
    residual = inputs_wide + dot_nt(mixed, output_t)
    second_rms = rms_scale(residual)
    second_unit = residual * second_rms
    second_normed = (second_unit * second_gain.astype(F32)).astype(BF16)
    normed_rows, out_rows = (
        member[0] for member in gather_col([second_normed[None], out_grad[None]], 3)
    )
    gate_act = dot_nt(normed_rows, gate_t)
    up_act = dot_nt(normed_rows, up_t)
    sigmoid_gate = jax.nn.sigmoid(gate_act)
    silu_gate = gate_act * sigmoid_gate
    hidden = (silu_gate * up_act).astype(BF16)
    down_grad = dot_tn(hidden, out_rows).astype(BF16)
    down_grad, out_rows = lax.optimization_barrier((down_grad, out_rows))
    down_grad_own = scatter_row(down_grad)
    hidden_grad = dot_nt(out_rows, down_block)
    up_grad_act = (hidden_grad * silu_gate).astype(BF16)
    gate_grad_act = (
        hidden_grad * up_act * sigmoid_gate * (1.0 + gate_act * (1.0 - sigmoid_gate))
    ).astype(BF16)
    normed_part = (dot_nn(gate_grad_act, gate_t) + dot_nn(up_grad_act, up_t)).astype(BF16)
    branch_part = dot_nn(hidden, down_block).astype(BF16)
    gate_grad_t = dot_tn(gate_grad_act, normed_rows).astype(BF16)
    up_grad_t = dot_tn(up_grad_act, normed_rows).astype(BF16)
    gate_grad_t, up_grad_t, normed_part = lax.optimization_barrier(
        (gate_grad_t, up_grad_t, normed_part)
    )
    gate_grad_own = scatter_row(gate_grad_t)
    up_grad_own = scatter_row(up_grad_t)
    normed_grad, branch_out = (
        member[0] for member in scatter_col([normed_part[None], branch_part[None]], 4)
    )
    layer_out = residual + branch_out
    second_gain_grad = jnp.sum(normed_grad * second_unit, axis=0)
    unit_grad = normed_grad * second_gain.astype(F32)
    residual_grad = out_grad.astype(F32) + second_rms * (
        unit_grad - second_unit * jnp.mean(unit_grad * second_unit, axis=-1, keepdims=True)
    )
    attended_grad = residual_grad.astype(BF16)
    mixed_grad = dot_nn(attended_grad, output_t).astype(BF16)
    grad_heads = mixed_grad.reshape(own_rows, KVH, group_size, HD)
    scores = masked_scores(query_heads, keys_window, visible, score_scale)
    probs = jnp.exp(scores - log_total)
    prob_grad = jnp.einsum(
        "tkgd,skd->kgts", grad_heads, values_window, preferred_element_type=F32
    )
    value_part = jnp.einsum(
        "kgts,tkgd->skd", probs.astype(BF16), grad_heads, preferred_element_type=F32
    )
    score_grad = (
        probs * (prob_grad - jnp.sum(probs * prob_grad, axis=-1, keepdims=True))
    ).astype(BF16)
    query_grad = (
        jnp.einsum("kgts,skd->tkgd", score_grad, keys_window, preferred_element_type=F32)
        * score_scale
    )
    key_part = (
        jnp.einsum("kgts,tkgd->skd", score_grad, query_heads, preferred_element_type=F32)
        * score_scale
    )
    both_part = jnp.concatenate(
        [key_part.reshape(window, KVH * HD), value_part.reshape(window, KVH * HD)], axis=1
    ).astype(BF16)
    both_rows = lax.dynamic_update_slice_in_dim(
        jnp.zeros((row_tokens, 2 * KVH * HD), BF16), both_part, window_start, 0
    )
    both_grad = scatter_col([both_rows[None]], 5)[0][0]
    key_grad, value_grad = both_grad[:, : KVH * HD], both_grad[:, KVH * HD :]
    query_wide = rounded_wide(query_grad.reshape(own_rows, HQ, HD))
    query_base_grad = (
        rotate_back(query_wide, cosines, sines).reshape(own_rows, HQ * HD).astype(BF16)
    )
    key_wide = rounded_wide(key_grad.reshape(own_rows, KVH, HD))
    key_base_grad = (
        rotate_back(key_wide, cosines, sines).reshape(own_rows, KVH * HD).astype(BF16)
    )
    value_base_grad = value_grad.astype(BF16)
    query_b_grad = jnp.sum(query_base_grad.astype(F32), axis=0)
    key_b_grad = jnp.sum(key_base_grad.astype(F32), axis=0)
    value_b_grad = jnp.sum(value_base_grad.astype(F32), axis=0)
    first_normed_grad = (
        dot_nn(query_base_grad, query_t)
        + dot_nn(key_base_grad, key_t)
        + dot_nn(value_base_grad, value_t)
    )
    first_gain_grad = jnp.sum(first_normed_grad * first_unit, axis=0)
    first_unit_grad = first_normed_grad * first_gain.astype(F32)
    input_grad = residual_grad + first_rms * (
        first_unit_grad
        - first_unit * jnp.mean(first_unit_grad * first_unit, axis=-1, keepdims=True)
    )
    small_grads = (query_b_grad, key_b_grad, value_b_grad, first_gain_grad, second_gain_grad)
    small_flat = jnp.concatenate(
        [member.reshape(row_parts * col_parts, -1) for member in small_grads], axis=1
    )
    small_flat = jnp.pad(
        small_flat, ((0, 0), (0, k_own * depth_own - small_flat.shape[1]))
    ).reshape(row_parts, col_parts, k_own, depth_own)
    small_flat = small_flat.transpose(1, 2, 0, 3).reshape(col_parts * k_own, depth)
    wide_grads = jnp.stack(
        [
            dot_tn(query_base_grad, first_normed).astype(BF16),
            dot_tn(attended_grad, mixed).astype(BF16),
        ]
    )
    thin_grads = jnp.stack(
        [
            dot_tn(key_base_grad, first_normed).astype(BF16),
            dot_tn(value_base_grad, first_normed).astype(BF16),
            small_flat.astype(BF16),
        ]
    )
    wide_part, thin_part = scatter_col([wide_grads, thin_grads], 6)
    wide_out = scatter_row(wide_part).astype(F32)
    thin_out = scatter_row(thin_part).astype(F32)
    query_w_out, output_w_out = wide_out[0], wide_out[1]
    key_w_out, value_w_out, small_out = thin_out[0], thin_out[1], thin_out[2]
    small_out = small_out.reshape(-1)
    small_list, offset = [], 0
    for size in small_sizes:
        small_list.append(small_out[offset : offset + size])
        offset += size
    return (
        layer_out,
        input_grad,
        small_list[3],
        query_w_out.T,
        small_list[0],
        key_w_out.T,
        small_list[1],
        value_w_out.T,
        small_list[2],
        output_w_out.T,
        small_list[4],
        gate_grad_own.astype(F32).T,
        up_grad_own.astype(F32).T,
        down_grad_own.astype(F32),
    )


def solution(mesh):
    in_specs = (
        P(("row", "col"), None),
        P(("row", "col"), None),
        P("row", None),
        P(("row", "col")),
        P("row", "col"),
        P(("row", "col")),
        P("row", "col"),
        P(("row", "col")),
        P("row", "col"),
        P(("row", "col")),
        P("row", "col"),
        P(("row", "col")),
        P("row", "col"),
        P("row", "col"),
        P("col", "row"),
    )
    out_specs = (
        P(("row", "col"), None),
        P(("row", "col"), None),
        P(("row", "col")),
        P("row", "col"),
        P(("row", "col")),
        P("row", "col"),
        P(("row", "col")),
        P("row", "col"),
        P(("row", "col")),
        P("row", "col"),
        P(("row", "col")),
        P("row", "col"),
        P("row", "col"),
        P("col", "row"),
    )
    return jax.shard_map(shards, mesh=mesh, in_specs=in_specs, out_specs=out_specs, check_vma=False)
```

```python
import functools
import math

import jax
import jax.numpy as jnp
from jax import lax
from jax.experimental import pallas as pl
from jax.experimental.pallas import tpu as pltpu
from jax.sharding import PartitionSpec as P

HQ = 12
KVH = 2
HD = 128
MAXLEN = 1024

EPSILON = 1e-06
ROPE_BASE = 1000000.0
BF16 = jnp.bfloat16
F32 = jnp.float32
MESH = pl.DeviceIdType.MESH


def seq_starts(slots, lengths):
    bounds = jnp.cumsum(lengths)
    picked = jnp.where(bounds[None, :] <= slots[:, None], lengths[None, :], 0)
    return jnp.sum(picked, axis=1)


def rope_tables(positions, head_dim):
    steps_up = jnp.arange(head_dim // 2, dtype=F32)
    freqs = jnp.exp(-math.log(ROPE_BASE) * (2.0 * steps_up / head_dim))
    angles = positions.astype(F32)[:, None] * freqs[None, :]
    angles = jnp.concatenate([angles, angles], axis=1)
    return (jnp.cos(angles)[:, None, :], jnp.sin(angles)[:, None, :])


def rotate_pairs(values, cosines, sines):
    half_dim = values.shape[-1] // 2
    turned = jnp.concatenate([-values[..., half_dim:], values[..., :half_dim]], axis=-1)
    return values * cosines + turned * sines


def rotate_back(grads_in, cosines, sines):
    half_dim = grads_in.shape[-1] // 2
    moved = grads_in * sines
    return grads_in * cosines + jnp.concatenate(
        [moved[..., half_dim:], -moved[..., :half_dim]], axis=-1
    )


def rms_scale(values):
    return lax.rsqrt(jnp.mean(values * values, axis=-1, keepdims=True) + EPSILON)


def dot_nn(left, right):
    return lax.dot_general(left, right, (((1,), (0,)), ((), ())), preferred_element_type=F32)


def dot_tn(left, right):
    return lax.dot_general(left, right, (((0,), (0,)), ((), ())), preferred_element_type=F32)


def dot_nt(left, right):
    return lax.dot_general(left, right, (((1,), (1,)), ((), ())), preferred_element_type=F32)


def rounded_wide(values):
    return lax.optimization_barrier(values.astype(BF16)).astype(F32)


def masked_scores(query_heads, keys_window, visible, score_scale):
    scores = jnp.einsum("tkgd,skd->kgts", query_heads, keys_window, preferred_element_type=F32)
    return jnp.where(visible, scores * score_scale, -jnp.inf)


def plane_places():
    me = lax.axis_index("col")
    chip, core = me // 2, me % 2
    low, high = chip % 2, chip // 2
    beside = high * 2 + (1 - low)
    above = (1 - high) * 2 + low
    across = (1 - high) * 2 + (1 - low)
    return chip, beside, above, across, core


def greet(peers):
    barrier = pltpu.get_barrier_semaphore()
    for peer in peers:
        pl.semaphore_signal(barrier, inc=1, device_id={"col": peer}, device_id_type=MESH)
    pl.semaphore_wait(barrier, len(peers))


def plane_gather_kernel(count, *refs):
    ins, outs = refs[:count], refs[count : 2 * count]
    send_sem, recv_sem, own_sem = refs[2 * count :]
    chip, beside, above, across, core = plane_places()
    mine = chip * 2 + core
    partner = chip * 2 + 1 - core
    to_x, to_y = beside * 2 + core, above * 2 + core
    greet((partner, to_x, to_y))

    def view(i, slot, part):
        size = ins[i].shape[1]
        half = size // 2
        if part is None:
            return outs[i].at[:, pl.ds(pl.multiple_of(slot * size, size), size), :]
        return outs[i].at[:, pl.ds(pl.multiple_of(slot * size + part * half, half), half), :]

    def copies(k, slot, part, peer, own=False):
        return [
            pltpu.make_async_remote_copy(
                src_ref=ins[i] if own else view(i, slot, part),
                dst_ref=view(i, slot, part),
                send_sem=send_sem.at[i, k],
                recv_sem=recv_sem.at[i, k],
                device_id={"col": peer},
                device_id_type=MESH,
            )
            for i in range(count)
        ]

    def start(cs):
        for c in cs:
            c.start()

    def wait_recv(cs):
        for c in cs:
            c.wait_recv()

    sent = [
        copies(1, mine, None, to_x, True),
        copies(2, mine, None, to_y, True),
        copies(0, mine, None, partner, True),
    ]
    for c in sent:
        start(c)
    own = [
        pltpu.make_async_copy(ins[i], view(i, mine, None), own_sem.at[i]) for i in range(count)
    ]
    start(own)
    other = 1 - core
    wait_recv(copies(1, to_x, None, to_x))
    more = [copies(3, to_x, 0, to_y), copies(5, to_x, None, partner)]
    for c in more:
        start(c)
    sent += more
    wait_recv(copies(2, to_y, None, to_y))
    more = [copies(4, to_y, 1, to_x), copies(6, to_y, None, partner)]
    for c in more:
        start(c)
    sent += more
    far = across * 2 + core
    wait_recv(copies(3, far, 0, to_y))
    more = [copies(7, far, 0, partner)]
    start(more[0])
    sent += more
    wait_recv(copies(4, far, 1, to_x))
    more = [copies(8, far, 1, partner)]
    start(more[0])
    sent += more
    wait_recv(copies(0, partner, None, partner))
    wait_recv(copies(5, beside * 2 + other, None, partner))
    wait_recv(copies(6, above * 2 + other, None, partner))
    wait_recv(copies(7, across * 2 + other, 0, partner))
    wait_recv(copies(8, across * 2 + other, 1, partner))
    for cs in sent:
        for c in cs:
            c.wait_send()
    for c in own:
        c.wait()


def plane_gather(shards, ident):
    count = len(shards)
    parts = lax.axis_size("col")
    outs = [
        jax.ShapeDtypeStruct((s.shape[0], s.shape[1] * parts, s.shape[2]), s.dtype)
        for s in shards
    ]
    return pl.pallas_call(
        functools.partial(plane_gather_kernel, count),
        out_shape=outs,
        in_specs=[pl.BlockSpec(memory_space=pl.ANY)] * count,
        out_specs=[pl.BlockSpec(memory_space=pl.ANY)] * count,
        scratch_shapes=[
            pltpu.SemaphoreType.DMA((count, 9)),
            pltpu.SemaphoreType.DMA((count, 9)),
            pltpu.SemaphoreType.DMA((count,)),
        ],
        compiler_params=pltpu.CompilerParams(collective_id=ident, has_side_effects=True),
        name="plane_gather",
    )(*shards)


def plane_scatter_kernel(count, *refs):
    ins, outs = refs[:count], refs[count : 2 * count]
    scratch = refs[2 * count :]
    near, made, side, land = (scratch[i * count : (i + 1) * count] for i in range(4))
    send_sem, recv_sem = scratch[4 * count :]
    chip, beside, above, across, core = plane_places()
    partner = chip * 2 + 1 - core
    to_x, to_y = beside * 2 + core, above * 2 + core
    greet((partner, to_x, to_y))
    order = (across, beside, above, chip)

    def rows(i, slot):
        size = outs[i].shape[1]
        return pl.ds(pl.multiple_of(slot * size, size), size)

    def half(i, part):
        size = outs[i].shape[1] // 2
        return pl.ds(part * size, size)

    def remote(i, k, src, dst, peer):
        return pltpu.make_async_remote_copy(
            src_ref=src,
            dst_ref=dst,
            send_sem=send_sem.at[i, k],
            recv_sem=recv_sem.at[i, k],
            device_id={"col": peer},
            device_id_type=MESH,
        )

    def near_copy(i, j):
        return remote(
            i, j, ins[i].at[:, rows(i, order[j] * 2 + 1 - core), :], near[i].at[j], partner
        )

    def side_copy(i, part):
        return remote(
            i, 4 + part, made[i].at[0, :, half(i, part), :], side[i].at[part],
            to_x if part == 0 else to_y,
        )

    def land_copy(i, which, part):
        return remote(
            i, 6 + which * 2 + part, made[i].at[1 + which, :, half(i, part), :],
            land[i].at[which, :, half(i, part), :], to_x if which == 0 else to_y,
        )

    step = 16

    def each(i, size, body):
        def tile(t, _):
            body(pl.multiple_of(t * step, step))
            return 0

        lax.fori_loop(0, size // step, tile, 0)

    def combine(i, j):
        size = outs[i].shape[1]
        first = (order[j] * 2 + core) * size

        def body(at):
            for a in range(outs[i].shape[0]):
                left = ins[i][a, pl.ds(pl.multiple_of(first + at, step), step), :].astype(F32)
                right = near[i][j, a, pl.ds(at, step), :].astype(F32)
                made[i][j, a, pl.ds(at, step), :] = (left + right).astype(BF16)

        each(i, size, body)

    def fold(i, which, part):
        size = outs[i].shape[1] // 2

        def body(at):
            at2 = pl.multiple_of(part * size + at, step)
            for a in range(outs[i].shape[0]):
                left = made[i][1 + which, a, pl.ds(at2, step), :].astype(F32)
                right = side[i][1 - which, a, pl.ds(at, step), :].astype(F32)
                made[i][1 + which, a, pl.ds(at2, step), :] = (left + right).astype(BF16)

        each(i, size, body)

    every = range(count)
    for j in range(4):
        for i in every:
            near_copy(i, j).start()
    for i in every:
        near_copy(i, 0).wait_recv()
        combine(i, 0)
        side_copy(i, 0).start()
        side_copy(i, 1).start()
    for i in every:
        near_copy(i, 1).wait_recv()
        combine(i, 1)
        land_copy(i, 0, 0).start()
    for i in every:
        near_copy(i, 2).wait_recv()
        combine(i, 2)
        land_copy(i, 1, 1).start()
    for i in every:
        side_copy(i, 0).wait_recv()
        fold(i, 1, 0)
        land_copy(i, 1, 0).start()
        side_copy(i, 1).wait_recv()
        fold(i, 0, 1)
        land_copy(i, 0, 1).start()
    for i in every:
        near_copy(i, 3).wait_recv()
    for i in every:
        for which in range(2):
            for part in range(2):
                land_copy(i, which, part).wait_recv()
        size = outs[i].shape[1]
        first = (chip * 2 + core) * size

        def body(at, i=i, first=first):
            for a in range(outs[i].shape[0]):
                spot = pl.ds(at, step)
                total = ins[i][a, pl.ds(pl.multiple_of(first + at, step), step), :].astype(F32)
                total += near[i][3, a, spot, :].astype(F32)
                total += land[i][0, a, spot, :].astype(F32)
                total += land[i][1, a, spot, :].astype(F32)
                outs[i][a, spot, :] = total.astype(outs[i].dtype)

        each(i, size, body)
    for i in every:
        for j in range(4):
            near_copy(i, j).wait_send()
        for part in range(2):
            side_copy(i, part).wait_send()
            for which in range(2):
                land_copy(i, which, part).wait_send()


def plane_scatter(fulls, ident, out_dtype=F32):
    count = len(fulls)
    parts = lax.axis_size("col")
    shapes = [(f.shape[0], f.shape[1] // parts, f.shape[2]) for f in fulls]
    scratch = []
    scratch += [pltpu.VMEM((4,) + s, BF16) for s in shapes]
    scratch += [pltpu.VMEM((3,) + s, BF16) for s in shapes]
    scratch += [pltpu.VMEM((2, s[0], s[1] // 2, s[2]), BF16) for s in shapes]
    scratch += [pltpu.VMEM((2,) + s, BF16) for s in shapes]
    return pl.pallas_call(
        functools.partial(plane_scatter_kernel, count),
        out_shape=[jax.ShapeDtypeStruct(s, out_dtype) for s in shapes],
        in_specs=[pl.BlockSpec(memory_space=pltpu.VMEM)] * count,
        out_specs=[pl.BlockSpec(memory_space=pltpu.VMEM)] * count,
        scratch_shapes=scratch
        + [pltpu.SemaphoreType.DMA((count, 10)), pltpu.SemaphoreType.DMA((count, 10))],
        compiler_params=pltpu.CompilerParams(collective_id=ident, has_side_effects=True),
        name="plane_scatter",
    )(*fulls)


def spans(total, most):
    return [(at, min(most, total - at)) for at in range(0, total, most)]


def remote(src, dst, send_sem, recv_sem, peer):
    return pltpu.make_async_remote_copy(
        src_ref=src,
        dst_ref=dst,
        send_sem=send_sem,
        recv_sem=recv_sem,
        device_id={"col": peer},
        device_id_type=MESH,
    )


def ffn_forward_kernel(
    normed,
    cotangent,
    gate_t,
    up_t,
    normed_rows,
    out_rows,
    hidden,
    silu,
    slope,
    land,
    tiles,
    send_sem,
    recv_sem,
    keep_sem,
    tile_sem,
):
    chip, beside, above, across, core = plane_places()
    low, high = chip % 2, chip // 2
    own_rows = normed.shape[0]
    half = own_rows // 2
    mine, partner = chip * 2 + core, chip * 2 + 1 - core
    to_x, to_y, far = beside * 2 + core, above * 2 + core, across * 2 + core
    greet((partner, to_x, to_y))
    sources = (normed, cotangent)
    full_rows = (normed_rows, out_rows)

    def copy(a, k, slot, part, peer, own=False):
        if part is None:
            spot = land.at[a, slot]
            src = sources[a] if own else spot
        else:
            spot = land.at[a, slot, pl.ds(part * half, half), :]
            src = spot
        return remote(src, spot, send_sem.at[a, k], recv_sem.at[a, k], peer)

    def first(a):
        copy(a, 1, mine, None, to_x, True).start()
        copy(a, 2, mine, None, to_y, True).start()
        copy(a, 0, mine, None, partner, True).start()

    def second(a):
        copy(a, 1, to_x, None, to_x).wait_recv()
        copy(a, 3, to_x, 0, to_y).start()
        copy(a, 5, to_x, None, partner).start()
        copy(a, 2, to_y, None, to_y).wait_recv()
        copy(a, 4, to_y, 1, to_x).start()
        copy(a, 6, to_y, None, partner).start()

    def third(a):
        copy(a, 3, far, 0, to_y).wait_recv()
        copy(a, 7, far, 0, partner).start()
        copy(a, 4, far, 1, to_x).wait_recv()
        copy(a, 8, far, 1, partner).start()

    def landed(a, k):
        slot = (partner, beside * 2 + 1 - core, above * 2 + 1 - core)[k]
        copy(a, (0, 5, 6)[k], slot, None, partner).wait_recv()

    def landed_far(a):
        copy(a, 7, across * 2 + 1 - core, 0, partner).wait_recv()
        copy(a, 8, across * 2 + 1 - core, 1, partner).wait_recv()

    def sent(a):
        for k, slot, part in (
            (0, mine, None), (1, mine, None), (2, mine, None), (3, to_x, 0), (4, to_y, 1),
            (5, to_x, None), (6, to_y, None), (7, far, 0), (8, far, 1),
        ):
            copy(a, k, slot, part, partner).wait_send()

    def spread(index):
        return pl.ds(pl.multiple_of(index * own_rows, own_rows), own_rows)

    def keep(a, slot):
        return pltpu.make_async_copy(
            land.at[a, slot], full_rows[a].at[spread(slot), :], keep_sem.at[a, slot]
        )

    def put(kind, slot, parity):
        target = (hidden, silu, slope)[kind]
        return pltpu.make_async_copy(
            tiles.at[kind, parity], target.at[spread(slot), :], tile_sem.at[kind, parity]
        )

    land[0, mine] = normed[...]
    land[1, mine] = cotangent[...]
    first(0)

    def step(s, _):
        flip = s // 2
        at_chip = (high + flip // 2) % 2 * 2 + (low + flip) % 2
        slot = at_chip * 2 + (core + s) % 2
        parity = s % 2

        @pl.when(s == 1)
        def _():
            landed(0, 0)

        @pl.when(s == 2)
        def _():
            second(0)

        @pl.when(s == 3)
        def _():
            landed(0, 1)

        @pl.when(s == 4)
        def _():
            first(1)

        @pl.when(s == 5)
        def _():
            landed(0, 2)
            third(0)

        @pl.when(s == 7)
        def _():
            landed_far(0)

        keep(0, slot).start()

        @pl.when(s >= 2)
        def _():
            for kind in range(3):
                put(kind, slot, parity).wait()

        for at, wide in spans(gate_t.shape[0], 512):
            cut = slice(at, at + wide)
            gate = dot_nt(land[0, slot], gate_t[cut, :])
            up = dot_nt(land[0, slot], up_t[cut, :])
            sigma = 1.0 / (1.0 + jnp.exp(-gate))
            smooth = gate * sigma
            tiles[0, parity, :, cut] = (smooth * up).astype(BF16)
            tiles[1, parity, :, cut] = smooth.astype(BF16)
            tiles[2, parity, :, cut] = (up * sigma * (1.0 + gate * (1.0 - sigma))).astype(BF16)
        for kind in range(3):
            put(kind, slot, parity).start()
        return 0

    lax.fori_loop(0, 8, step, 0)
    second(1)
    landed(1, 0)
    third(1)
    landed(1, 1)
    landed(1, 2)
    landed_far(1)

    def store(slot, _):
        keep(1, slot).start()
        return 0

    lax.fori_loop(0, 8, store, 0)

    def drain(slot, _):
        keep(0, slot).wait()
        keep(1, slot).wait()
        return 0

    for parity in range(2):
        for kind in range(3):
            put(kind, 0, parity).wait()
    lax.fori_loop(0, 8, drain, 0)
    sent(0)
    sent(1)


def ffn_forward(normed, cotangent, gate_t, up_t, ident):
    rows, depth = normed.shape
    wide = gate_t.shape[0]
    total = rows * 8
    vmem = pl.BlockSpec(memory_space=pltpu.VMEM)
    anywhere = pl.BlockSpec(memory_space=pl.ANY)
    return pl.pallas_call(
        ffn_forward_kernel,
        out_shape=[jax.ShapeDtypeStruct((total, depth), BF16)] * 2
        + [jax.ShapeDtypeStruct((total, wide), BF16)] * 3,
        in_specs=[vmem] * 4,
        out_specs=[anywhere] * 5,
        scratch_shapes=[
            pltpu.VMEM((2, 8, rows, depth), BF16),
            pltpu.VMEM((3, 2, rows, wide), BF16),
            pltpu.SemaphoreType.DMA((2, 9)),
            pltpu.SemaphoreType.DMA((2, 9)),
            pltpu.SemaphoreType.DMA((2, 8)),
            pltpu.SemaphoreType.DMA((3, 2)),
        ],
        compiler_params=pltpu.CompilerParams(collective_id=ident, has_side_effects=True),
        name="ffn_forward",
    )(normed, cotangent, gate_t, up_t)


def ffn_backward_kernel(
    out_rows,
    hidden,
    silu,
    slope,
    gate_t,
    up_t,
    down,
    gate_grad,
    up_grad,
    branch_own,
    normed_own,
    out_in,
    tiles_in,
    tiles_out,
    give,
    near,
    made,
    side,
    land,
    near_send,
    near_recv,
    side_send,
    side_recv,
    land_send,
    land_recv,
    in_sem,
    tile_sem,
):
    chip, beside, above, across, core = plane_places()
    low, high = chip % 2, chip // 2
    own_rows = branch_own.shape[0]
    half = own_rows // 2
    depth = branch_own.shape[1]
    partner = chip * 2 + 1 - core
    to_x, to_y = beside * 2 + core, above * 2 + core
    greet((partner, to_x, to_y))
    finals = (branch_own, normed_own)

    def spread(index):
        return pl.ds(pl.multiple_of(index * own_rows, own_rows), own_rows)

    def slot_of(s):
        flip = 3 - s // 2
        at_chip = (high + flip // 2) % 2 * 2 + (low + flip) % 2
        return at_chip * 2 + (core + 1 + s) % 2

    def near_copy(a, j):
        return remote(
            give.at[a, j], near.at[a, j], near_send.at[a, j], near_recv.at[a, j], partner
        )

    def side_copy(a, part):
        return remote(
            made.at[a, 0, pl.ds(part * half, half), :], side.at[a, part],
            side_send.at[a, part], side_recv.at[a, part], to_x if part == 0 else to_y,
        )

    def land_copy(a, which, part):
        k = which * 2 + part
        return remote(
            made.at[a, 1 + which, pl.ds(part * half, half), :],
            land.at[a, which, pl.ds(part * half, half), :],
            land_send.at[a, k], land_recv.at[a, k], to_x if which == 0 else to_y,
        )

    def fold(a, which, part):
        def tile(t, _):
            at = pl.multiple_of(t * 16, 16)
            spot = pl.ds(pl.multiple_of(part * half + at, 16), 16)
            left = made[a, 1 + which, spot, :].astype(F32)
            right = side[a, 1 - which, pl.ds(at, 16), :].astype(F32)
            made[a, 1 + which, spot, :] = (left + right).astype(BF16)
            return 0

        lax.fori_loop(0, half // 16, tile, 0)

    def fetch(kind, s, parity):
        if kind == 0:
            return pltpu.make_async_copy(
                out_rows.at[spread(slot_of(s)), :], out_in.at[parity], in_sem.at[0, parity]
            )
        source = (hidden, silu, slope)[kind - 1]
        return pltpu.make_async_copy(
            source.at[spread(slot_of(s)), :], tiles_in.at[kind - 1, parity], in_sem.at[kind, parity]
        )

    def put(kind, s, parity):
        target = (gate_grad, up_grad)[kind]
        return pltpu.make_async_copy(
            tiles_out.at[kind, parity], target.at[spread(slot_of(s)), :],
            tile_sem.at[kind, parity],
        )

    def sides(a):
        side_copy(a, 0).wait_recv()
        fold(a, 1, 0)
        land_copy(a, 1, 0).start()
        side_copy(a, 1).wait_recv()
        fold(a, 0, 1)
        land_copy(a, 0, 1).start()

    def deliver(a, s, partial):
        j = s // 2

        @pl.when(s % 2 == 0)
        def _():
            give[a, j] = partial().astype(BF16)
            near_copy(a, j).start()

        @pl.when(s % 2 == 1)
        def _():
            total = partial()
            near_copy(a, j).wait_recv()
            total = total + near[a, j].astype(F32)

            @pl.when(j < 3)
            def _():
                made[a, (3 - j) % 3] = total.astype(BF16)

            @pl.when(j == 0)
            def _():
                side_copy(a, 0).start()
                side_copy(a, 1).start()

            @pl.when(j == 1)
            def _():
                land_copy(a, 1, 1).start()

            @pl.when(j == 2)
            def _():
                land_copy(a, 0, 0).start()
                sides(a)

            @pl.when(j == 3)
            def _():
                finals[a][...] = total

    fetch(1, 0, 0).start()

    def branch_step(s, _):
        parity = s % 2

        @pl.when(s < 7)
        def _():
            fetch(1, s + 1, (s + 1) % 2).start()

        @pl.when(s == 6)
        def _():
            for kind in (0, 2, 3):
                fetch(kind, 0, 0).start()

        fetch(1, s, parity).wait()
        deliver(0, s, lambda: dot_nn(tiles_in[0, parity], down[...]))
        return 0

    lax.fori_loop(0, 8, branch_step, 0)

    def normed_step(s, _):
        parity = s % 2

        @pl.when(s < 7)
        def _():
            for kind in (0, 2, 3):
                fetch(kind, s + 1, (s + 1) % 2).start()

        for kind in (0, 2, 3):
            fetch(kind, s, parity).wait()

        @pl.when(s >= 2)
        def _():
            for kind in range(2):
                put(kind, s, parity).wait()

        for at, wide in spans(down.shape[0], 512):
            cut = slice(at, at + wide)
            hidden_grad = dot_nt(out_in[parity], down[cut, :])
            tiles_out[0, parity, :, cut] = (
                hidden_grad * tiles_in[2, parity, :, cut].astype(F32)
            ).astype(BF16)
            tiles_out[1, parity, :, cut] = (
                hidden_grad * tiles_in[1, parity, :, cut].astype(F32)
            ).astype(BF16)
        for kind in range(2):
            put(kind, s, parity).start()
        deliver(
            1, s,
            lambda: dot_nn(tiles_out[0, parity], gate_t[...])
            + dot_nn(tiles_out[1, parity], up_t[...]),
        )
        return 0

    lax.fori_loop(0, 8, normed_step, 0)
    for a in range(2):
        for which in range(2):
            for part in range(2):
                land_copy(a, which, part).wait_recv()

        def tile(t, _, a=a):
            spot = pl.ds(pl.multiple_of(t * 16, 16), 16)
            finals[a][spot, :] = (
                finals[a][spot, :]
                + land[a, 0, spot, :].astype(F32)
                + land[a, 1, spot, :].astype(F32)
            )
            return 0

        lax.fori_loop(0, own_rows // 16, tile, 0)
    for a in range(2):
        for j in range(4):
            near_copy(a, j).wait_send()
        for part in range(2):
            side_copy(a, part).wait_send()
            for which in range(2):
                land_copy(a, which, part).wait_send()
    for kind in range(2):
        for parity in range(2):
            put(kind, parity, parity).wait()


def ffn_backward(out_rows, hidden, silu, slope, gate_t, up_t, down, ident):
    total, depth = out_rows.shape
    wide = down.shape[0]
    rows = total // 8
    vmem = pl.BlockSpec(memory_space=pltpu.VMEM)
    anywhere = pl.BlockSpec(memory_space=pl.ANY)
    dma = pltpu.SemaphoreType.DMA
    return pl.pallas_call(
        ffn_backward_kernel,
        out_shape=[jax.ShapeDtypeStruct((total, wide), BF16)] * 2
        + [jax.ShapeDtypeStruct((rows, depth), F32)] * 2,
        in_specs=[anywhere] * 4 + [vmem] * 3,
        out_specs=[anywhere] * 2 + [vmem] * 2,
        scratch_shapes=[
            pltpu.VMEM((2, rows, depth), BF16),
            pltpu.VMEM((3, 2, rows, wide), BF16),
            pltpu.VMEM((2, 2, rows, wide), BF16),
            pltpu.VMEM((2, 4, rows, depth), BF16),
            pltpu.VMEM((2, 4, rows, depth), BF16),
            pltpu.VMEM((2, 3, rows, depth), BF16),
            pltpu.VMEM((2, 2, rows // 2, depth), BF16),
            pltpu.VMEM((2, 2, rows, depth), BF16),
            dma((2, 4)),
            dma((2, 4)),
            dma((2, 2)),
            dma((2, 2)),
            dma((2, 4)),
            dma((2, 4)),
            dma((4, 2)),
            dma((2, 2)),
        ],
        compiler_params=pltpu.CompilerParams(collective_id=ident, has_side_effects=True),
        name="ffn_backward",
    )(out_rows, hidden, silu, slope, gate_t, up_t, down)


def gather_row(block):
    return lax.all_gather(block, "row", axis=block.ndim - 1, tiled=True)


def scatter_row(full):
    return lax.psum_scatter(
        full.astype(BF16), "row", scatter_dimension=0, tiled=True
    )


def gather_col(blocks, ident):
    if lax.axis_size("col") == 8:
        return plane_gather(blocks, ident)
    return [lax.all_gather(block, "col", axis=1, tiled=True) for block in blocks]


def scatter_col(fulls, ident):
    fulls = [full.astype(BF16) for full in fulls]
    if lax.axis_size("col") == 8:
        return plane_scatter(fulls, ident)
    return [
        lax.psum_scatter(full, "col", scatter_dimension=1, tiled=True).astype(F32)
        for full in fulls
    ]


def shards(
    hidden_in,
    out_grad,
    seq_lengths,
    norm1_gain,
    q_weight,
    q_bias,
    k_weight,
    k_bias,
    v_weight,
    v_bias,
    o_weight,
    norm2_gain,
    gate_weight,
    up_weight,
    down_weight,
):
    row_parts = lax.axis_size("row")
    col_parts = lax.axis_size("col")
    col_place = lax.axis_index("col")
    depth_own = q_weight.shape[0]
    depth = depth_own * row_parts
    q_own, k_own = q_weight.shape[1], k_weight.shape[1]
    smalls = (q_bias, k_bias, v_bias, norm1_gain, norm2_gain)
    small_sizes = [member.shape[0] for member in smalls]
    packed_small = jnp.concatenate(smalls)
    packed_small = jnp.pad(packed_small, (0, k_own * depth_own - packed_small.shape[0]))
    wide_own = gather_row(jnp.stack([q_weight.T, o_weight.T]))
    thin_own = gather_row(
        jnp.stack([k_weight.T, v_weight.T, packed_small.reshape(k_own, depth_own)])
    )
    wide_full, thin_full = gather_col([wide_own, thin_own], 1)
    query_t, output_t = wide_full[0], wide_full[1]
    key_t, value_t = thin_full[0], thin_full[1]
    small_flat = thin_full[2].reshape(col_parts, k_own, row_parts, depth_own)
    small_flat = small_flat.transpose(2, 0, 1, 3).reshape(row_parts * col_parts, -1)
    small_full, offset = [], 0
    for size in small_sizes:
        small_full.append(small_flat[:, offset : offset + size].reshape(-1))
        offset += size
    query_offset, key_offset, value_offset, first_gain, second_gain = small_full

    gate_t = gather_row(gate_weight.T)
    up_t = gather_row(up_weight.T)
    down_block = gather_row(down_weight)

    own_rows = hidden_in.shape[0]
    row_tokens = own_rows * col_parts
    lengths = seq_lengths[0]
    query_slots = col_place * own_rows + jnp.arange(own_rows, dtype=jnp.int32)
    query_starts = seq_starts(query_slots, lengths)
    cosines, sines = rope_tables(query_slots - query_starts, HD)
    group_size = HQ // KVH
    score_scale = 1.0 / math.sqrt(HD)
    inputs_wide = hidden_in.astype(F32)
    first_rms = rms_scale(inputs_wide)
    first_unit = inputs_wide * first_rms
    first_normed = (first_unit * first_gain.astype(F32)).astype(BF16)
    query_base = dot_nt(first_normed, query_t) + query_offset.astype(F32)
    key_base = dot_nt(first_normed, key_t) + key_offset.astype(F32)
    value_own = (dot_nt(first_normed, value_t) + value_offset.astype(F32)).astype(BF16)
    queries = rotate_pairs(query_base.reshape(own_rows, HQ, HD), cosines, sines).astype(BF16)
    keys_own = rotate_pairs(key_base.reshape(own_rows, KVH, HD), cosines, sines).astype(BF16)
    both_own = jnp.concatenate([keys_own.reshape(own_rows, KVH * HD), value_own], axis=1)
    both_all = gather_col([both_own[None]], 2)[0][0]
    window = min(own_rows + MAXLEN, row_tokens)
    window_start = jnp.clip(col_place * own_rows - MAXLEN, 0, row_tokens - window)
    key_slots = window_start + jnp.arange(window, dtype=jnp.int32)
    key_starts = seq_starts(key_slots, lengths)
    visible = (query_starts[:, None] == key_starts[None, :]) & (
        key_slots[None, :] <= query_slots[:, None]
    )
    both_window = lax.dynamic_slice_in_dim(both_all, window_start, window, 0)
    keys_window = both_window[:, : KVH * HD].reshape(window, KVH, HD)
    values_window = both_window[:, KVH * HD :].reshape(window, KVH, HD)
    query_heads = queries.reshape(own_rows, KVH, group_size, HD)
    scores = masked_scores(query_heads, keys_window, visible, score_scale)
    peak = jnp.max(scores, axis=-1, keepdims=True)
    expanded = jnp.exp(scores - peak)
    totals = jnp.sum(expanded, axis=-1, keepdims=True)
    probs = expanded / totals
    log_total = peak + jnp.log(totals)
    mixed = jnp.einsum(
        "kgts,skd->tkgd", probs.astype(BF16), values_window, preferred_element_type=F32
    )
    mixed = mixed.reshape(own_rows, HQ * HD).astype(BF16)
    residual = inputs_wide + dot_nt(mixed, output_t)
    second_rms = rms_scale(residual)
    second_unit = residual * second_rms
    second_normed = (second_unit * second_gain.astype(F32)).astype(BF16)
    kernels = col_parts == 8
    if kernels:
        normed_rows, out_rows, hidden, silu_gate, slope = ffn_forward(
            second_normed, out_grad, gate_t, up_t, 3
        )
    else:
        normed_rows, out_rows = (
            member[0] for member in gather_col([second_normed[None], out_grad[None]], 3)
        )
        gate_act = dot_nt(normed_rows, gate_t)
        up_act = dot_nt(normed_rows, up_t)
        sigmoid_gate = jax.nn.sigmoid(gate_act)
        silu_gate = gate_act * sigmoid_gate
        slope = up_act * sigmoid_gate * (1.0 + gate_act * (1.0 - sigmoid_gate))
        hidden = (silu_gate * up_act).astype(BF16)
    down_grad = dot_tn(out_rows, hidden).astype(BF16)
    down_grad, out_rows = lax.optimization_barrier((down_grad, out_rows))
    down_grad_own = scatter_row(down_grad)
    if kernels:
        gate_grad_act, up_grad_act, branch_out, normed_grad = ffn_backward(
            out_rows, hidden, silu_gate, slope, gate_t, up_t, down_block, 4
        )
    else:
        hidden_grad = dot_nt(out_rows, down_block)
        up_grad_act = (hidden_grad * silu_gate).astype(BF16)
        gate_grad_act = (hidden_grad * slope).astype(BF16)
        normed_part = dot_nn(gate_grad_act, gate_t) + dot_nn(up_grad_act, up_t)
        branch_part = dot_nn(hidden, down_block)
        normed_grad, branch_out = (
            member[0] for member in scatter_col([normed_part[None], branch_part[None]], 4)
        )
    gate_grad = dot_tn(normed_rows, gate_grad_act).astype(BF16)
    up_grad = dot_tn(normed_rows, up_grad_act).astype(BF16)
    gate_grad, up_grad, normed_grad = lax.optimization_barrier(
        (gate_grad, up_grad, normed_grad)
    )
    gate_grad_own = scatter_row(gate_grad)
    up_grad_own = scatter_row(up_grad)
    layer_out = residual + branch_out
    second_gain_grad = jnp.sum(normed_grad * second_unit, axis=0)
    unit_grad = normed_grad * second_gain.astype(F32)
    residual_grad = out_grad.astype(F32) + second_rms * (
        unit_grad - second_unit * jnp.mean(unit_grad * second_unit, axis=-1, keepdims=True)
    )
    attended_grad = residual_grad.astype(BF16)
    mixed_grad = dot_nn(attended_grad, output_t).astype(BF16)
    grad_heads = mixed_grad.reshape(own_rows, KVH, group_size, HD)
    scores = masked_scores(query_heads, keys_window, visible, score_scale)
    probs = jnp.exp(scores - log_total)
    prob_grad = jnp.einsum(
        "tkgd,skd->kgts", grad_heads, values_window, preferred_element_type=F32
    )
    value_part = jnp.einsum(
        "kgts,tkgd->skd", probs.astype(BF16), grad_heads, preferred_element_type=F32
    )
    score_grad = (
        probs * (prob_grad - jnp.sum(probs * prob_grad, axis=-1, keepdims=True))
    ).astype(BF16)
    query_grad = (
        jnp.einsum("kgts,skd->tkgd", score_grad, keys_window, preferred_element_type=F32)
        * score_scale
    )
    key_part = (
        jnp.einsum("kgts,tkgd->skd", score_grad, query_heads, preferred_element_type=F32)
        * score_scale
    )
    both_part = jnp.concatenate(
        [key_part.reshape(window, KVH * HD), value_part.reshape(window, KVH * HD)], axis=1
    ).astype(BF16)
    both_rows = lax.dynamic_update_slice_in_dim(
        jnp.zeros((row_tokens, 2 * KVH * HD), BF16), both_part, window_start, 0
    )
    both_rows, down_grad_own = lax.optimization_barrier((both_rows, down_grad_own))
    both_grad = scatter_col([both_rows[None]], 5)[0][0]
    key_grad, value_grad = both_grad[:, : KVH * HD], both_grad[:, KVH * HD :]
    query_wide = rounded_wide(query_grad.reshape(own_rows, HQ, HD))
    query_base_grad = (
        rotate_back(query_wide, cosines, sines).reshape(own_rows, HQ * HD).astype(BF16)
    )
    key_wide = rounded_wide(key_grad.reshape(own_rows, KVH, HD))
    key_base_grad = (
        rotate_back(key_wide, cosines, sines).reshape(own_rows, KVH * HD).astype(BF16)
    )
    value_base_grad = value_grad.astype(BF16)
    query_b_grad = jnp.sum(query_base_grad.astype(F32), axis=0)
    key_b_grad = jnp.sum(key_base_grad.astype(F32), axis=0)
    value_b_grad = jnp.sum(value_base_grad.astype(F32), axis=0)
    first_normed_grad = (
        dot_nn(query_base_grad, query_t)
        + dot_nn(key_base_grad, key_t)
        + dot_nn(value_base_grad, value_t)
    )
    first_gain_grad = jnp.sum(first_normed_grad * first_unit, axis=0)
    first_unit_grad = first_normed_grad * first_gain.astype(F32)
    input_grad = residual_grad + first_rms * (
        first_unit_grad
        - first_unit * jnp.mean(first_unit_grad * first_unit, axis=-1, keepdims=True)
    )
    small_grads = (query_b_grad, key_b_grad, value_b_grad, first_gain_grad, second_gain_grad)
    small_flat = jnp.concatenate(
        [member.reshape(row_parts * col_parts, -1) for member in small_grads], axis=1
    )
    small_flat = jnp.pad(
        small_flat, ((0, 0), (0, k_own * depth_own - small_flat.shape[1]))
    ).reshape(row_parts, col_parts, k_own, depth_own)
    small_flat = small_flat.transpose(1, 2, 0, 3).reshape(col_parts * k_own, depth)
    wide_grads = jnp.stack(
        [
            dot_tn(query_base_grad, first_normed).astype(BF16),
            dot_tn(attended_grad, mixed).astype(BF16),
        ]
    )
    thin_grads = jnp.stack(
        [
            dot_tn(key_base_grad, first_normed).astype(BF16),
            dot_tn(value_base_grad, first_normed).astype(BF16),
            small_flat.astype(BF16),
        ]
    )
    wide_grads, gate_grad_own, up_grad_own = lax.optimization_barrier(
        (wide_grads, gate_grad_own, up_grad_own)
    )
    wide_part, thin_part = scatter_col([wide_grads, thin_grads], 6)
    wide_out = scatter_row(wide_part.transpose(2, 0, 1)).astype(F32).transpose(1, 2, 0)
    thin_out = scatter_row(thin_part.transpose(2, 0, 1)).astype(F32).transpose(1, 2, 0)
    query_w_out, output_w_out = wide_out[0], wide_out[1]
    key_w_out, value_w_out, small_out = thin_out[0], thin_out[1], thin_out[2]
    small_out = small_out.reshape(-1)
    small_list, offset = [], 0
    for size in small_sizes:
        small_list.append(small_out[offset : offset + size])
        offset += size
    return (
        layer_out,
        input_grad,
        small_list[3],
        query_w_out.T,
        small_list[0],
        key_w_out.T,
        small_list[1],
        value_w_out.T,
        small_list[2],
        output_w_out.T,
        small_list[4],
        gate_grad_own.astype(F32),
        up_grad_own.astype(F32),
        down_grad_own.astype(F32).T,
    )


def solution(mesh):
    in_specs = (
        P(("row", "col"), None),
        P(("row", "col"), None),
        P("row", None),
        P(("row", "col")),
        P("row", "col"),
        P(("row", "col")),
        P("row", "col"),
        P(("row", "col")),
        P("row", "col"),
        P(("row", "col")),
        P("row", "col"),
        P(("row", "col")),
        P("row", "col"),
        P("row", "col"),
        P("col", "row"),
    )
    out_specs = (
        P(("row", "col"), None),
        P(("row", "col"), None),
        P(("row", "col")),
        P("row", "col"),
        P(("row", "col")),
        P("row", "col"),
        P(("row", "col")),
        P("row", "col"),
        P(("row", "col")),
        P("row", "col"),
        P(("row", "col")),
        P("row", "col"),
        P("row", "col"),
        P("col", "row"),
    )
    return jax.shard_map(shards, mesh=mesh, in_specs=in_specs, out_specs=out_specs, check_vma=False)
```

```python
import functools
import math

import jax
import jax.numpy as jnp
from jax import lax
from jax.experimental import pallas as pl
from jax.experimental.pallas import tpu as pltpu
from jax.sharding import PartitionSpec as P

HQ = 12
KVH = 2
HD = 128
MAXLEN = 1024

EPSILON = 1e-06
ROPE_BASE = 1000000.0
BF16 = jnp.bfloat16
F32 = jnp.float32
MESH = pl.DeviceIdType.MESH


def seq_starts(slots, lengths):
    bounds = jnp.cumsum(lengths)
    picked = jnp.where(bounds[None, :] <= slots[:, None], lengths[None, :], 0)
    return jnp.sum(picked, axis=1)


def rope_tables(positions, head_dim):
    steps_up = jnp.arange(head_dim // 2, dtype=F32)
    freqs = jnp.exp(-math.log(ROPE_BASE) * (2.0 * steps_up / head_dim))
    angles = positions.astype(F32)[:, None] * freqs[None, :]
    angles = jnp.concatenate([angles, angles], axis=1)
    return (jnp.cos(angles)[:, None, :], jnp.sin(angles)[:, None, :])


def rotate_pairs(values, cosines, sines):
    half_dim = values.shape[-1] // 2
    turned = jnp.concatenate([-values[..., half_dim:], values[..., :half_dim]], axis=-1)
    return values * cosines + turned * sines


def rotate_back(grads_in, cosines, sines):
    half_dim = grads_in.shape[-1] // 2
    moved = grads_in * sines
    return grads_in * cosines + jnp.concatenate(
        [moved[..., half_dim:], -moved[..., :half_dim]], axis=-1
    )


def rms_scale(values):
    return lax.rsqrt(jnp.mean(values * values, axis=-1, keepdims=True) + EPSILON)


def dot_nn(left, right):
    return lax.dot_general(left, right, (((1,), (0,)), ((), ())), preferred_element_type=F32)


def dot_tn(left, right):
    return lax.dot_general(left, right, (((0,), (0,)), ((), ())), preferred_element_type=F32)


def dot_nt(left, right):
    return lax.dot_general(left, right, (((1,), (1,)), ((), ())), preferred_element_type=F32)


def rounded_wide(values):
    return lax.optimization_barrier(values.astype(BF16)).astype(F32)


def masked_scores(query_heads, keys_window, visible, score_scale):
    scores = jnp.einsum("tkgd,skd->kgts", query_heads, keys_window, preferred_element_type=F32)
    return jnp.where(visible, scores * score_scale, -jnp.inf)


def plane_places():
    me = lax.axis_index("col")
    chip, core = me // 2, me % 2
    low, high = chip % 2, chip // 2
    beside = high * 2 + (1 - low)
    above = (1 - high) * 2 + low
    across = (1 - high) * 2 + (1 - low)
    return chip, beside, above, across, core


def greet(peers):
    barrier = pltpu.get_barrier_semaphore()
    for peer in peers:
        pl.semaphore_signal(barrier, inc=1, device_id={"col": peer}, device_id_type=MESH)
    pl.semaphore_wait(barrier, len(peers))


def plane_gather_kernel(count, *refs):
    ins, outs = refs[:count], refs[count : 2 * count]
    send_sem, recv_sem, own_sem = refs[2 * count :]
    chip, beside, above, across, core = plane_places()
    mine = chip * 2 + core
    partner = chip * 2 + 1 - core
    to_x, to_y = beside * 2 + core, above * 2 + core
    greet((partner, to_x, to_y))

    def view(i, slot, part):
        size = ins[i].shape[1]
        half = size // 2
        if part is None:
            return outs[i].at[:, pl.ds(pl.multiple_of(slot * size, size), size), :]
        return outs[i].at[:, pl.ds(pl.multiple_of(slot * size + part * half, half), half), :]

    def copies(k, slot, part, peer, own=False):
        return [
            pltpu.make_async_remote_copy(
                src_ref=ins[i] if own else view(i, slot, part),
                dst_ref=view(i, slot, part),
                send_sem=send_sem.at[i, k],
                recv_sem=recv_sem.at[i, k],
                device_id={"col": peer},
                device_id_type=MESH,
            )
            for i in range(count)
        ]

    def start(cs):
        for c in cs:
            c.start()

    def wait_recv(cs):
        for c in cs:
            c.wait_recv()

    sent = [
        copies(1, mine, None, to_x, True),
        copies(2, mine, None, to_y, True),
        copies(0, mine, None, partner, True),
    ]
    for c in sent:
        start(c)
    own = [
        pltpu.make_async_copy(ins[i], view(i, mine, None), own_sem.at[i]) for i in range(count)
    ]
    start(own)
    other = 1 - core
    wait_recv(copies(1, to_x, None, to_x))
    more = [copies(3, to_x, 0, to_y), copies(5, to_x, None, partner)]
    for c in more:
        start(c)
    sent += more
    wait_recv(copies(2, to_y, None, to_y))
    more = [copies(4, to_y, 1, to_x), copies(6, to_y, None, partner)]
    for c in more:
        start(c)
    sent += more
    far = across * 2 + core
    wait_recv(copies(3, far, 0, to_y))
    more = [copies(7, far, 0, partner)]
    start(more[0])
    sent += more
    wait_recv(copies(4, far, 1, to_x))
    more = [copies(8, far, 1, partner)]
    start(more[0])
    sent += more
    wait_recv(copies(0, partner, None, partner))
    wait_recv(copies(5, beside * 2 + other, None, partner))
    wait_recv(copies(6, above * 2 + other, None, partner))
    wait_recv(copies(7, across * 2 + other, 0, partner))
    wait_recv(copies(8, across * 2 + other, 1, partner))
    for cs in sent:
        for c in cs:
            c.wait_send()
    for c in own:
        c.wait()


def plane_gather(shards, ident):
    count = len(shards)
    parts = lax.axis_size("col")
    outs = [
        jax.ShapeDtypeStruct((s.shape[0], s.shape[1] * parts, s.shape[2]), s.dtype)
        for s in shards
    ]
    return pl.pallas_call(
        functools.partial(plane_gather_kernel, count),
        out_shape=outs,
        in_specs=[pl.BlockSpec(memory_space=pl.ANY)] * count,
        out_specs=[pl.BlockSpec(memory_space=pl.ANY)] * count,
        scratch_shapes=[
            pltpu.SemaphoreType.DMA((count, 9)),
            pltpu.SemaphoreType.DMA((count, 9)),
            pltpu.SemaphoreType.DMA((count,)),
        ],
        compiler_params=pltpu.CompilerParams(collective_id=ident, has_side_effects=True),
        name="plane_gather",
    )(*shards)


def plane_scatter_kernel(count, *refs):
    ins, outs = refs[:count], refs[count : 2 * count]
    scratch = refs[2 * count :]
    near, made, side, land = (scratch[i * count : (i + 1) * count] for i in range(4))
    send_sem, recv_sem = scratch[4 * count :]
    chip, beside, above, across, core = plane_places()
    partner = chip * 2 + 1 - core
    to_x, to_y = beside * 2 + core, above * 2 + core
    greet((partner, to_x, to_y))
    order = (across, beside, above, chip)

    def rows(i, slot):
        size = outs[i].shape[1]
        return pl.ds(pl.multiple_of(slot * size, size), size)

    def half(i, part):
        size = outs[i].shape[1] // 2
        return pl.ds(part * size, size)

    def remote(i, k, src, dst, peer):
        return pltpu.make_async_remote_copy(
            src_ref=src,
            dst_ref=dst,
            send_sem=send_sem.at[i, k],
            recv_sem=recv_sem.at[i, k],
            device_id={"col": peer},
            device_id_type=MESH,
        )

    def near_copy(i, j):
        return remote(
            i, j, ins[i].at[:, rows(i, order[j] * 2 + 1 - core), :], near[i].at[j], partner
        )

    def side_copy(i, part):
        return remote(
            i, 4 + part, made[i].at[0, :, half(i, part), :], side[i].at[part],
            to_x if part == 0 else to_y,
        )

    def land_copy(i, which, part):
        return remote(
            i, 6 + which * 2 + part, made[i].at[1 + which, :, half(i, part), :],
            land[i].at[which, :, half(i, part), :], to_x if which == 0 else to_y,
        )

    step = 16

    def each(i, size, body):
        def tile(t, _):
            body(pl.multiple_of(t * step, step))
            return 0

        lax.fori_loop(0, size // step, tile, 0)

    def combine(i, j):
        size = outs[i].shape[1]
        first = (order[j] * 2 + core) * size

        def body(at):
            for a in range(outs[i].shape[0]):
                left = ins[i][a, pl.ds(pl.multiple_of(first + at, step), step), :].astype(F32)
                right = near[i][j, a, pl.ds(at, step), :].astype(F32)
                made[i][j, a, pl.ds(at, step), :] = (left + right).astype(BF16)

        each(i, size, body)

    def fold(i, which, part):
        size = outs[i].shape[1] // 2

        def body(at):
            at2 = pl.multiple_of(part * size + at, step)
            for a in range(outs[i].shape[0]):
                left = made[i][1 + which, a, pl.ds(at2, step), :].astype(F32)
                right = side[i][1 - which, a, pl.ds(at, step), :].astype(F32)
                made[i][1 + which, a, pl.ds(at2, step), :] = (left + right).astype(BF16)

        each(i, size, body)

    every = range(count)
    for j in range(4):
        for i in every:
            near_copy(i, j).start()
    for i in every:
        near_copy(i, 0).wait_recv()
        combine(i, 0)
        side_copy(i, 0).start()
        side_copy(i, 1).start()
    for i in every:
        near_copy(i, 1).wait_recv()
        combine(i, 1)
        land_copy(i, 0, 0).start()
    for i in every:
        near_copy(i, 2).wait_recv()
        combine(i, 2)
        land_copy(i, 1, 1).start()
    for i in every:
        side_copy(i, 0).wait_recv()
        fold(i, 1, 0)
        land_copy(i, 1, 0).start()
        side_copy(i, 1).wait_recv()
        fold(i, 0, 1)
        land_copy(i, 0, 1).start()
    for i in every:
        near_copy(i, 3).wait_recv()
    for i in every:
        for which in range(2):
            for part in range(2):
                land_copy(i, which, part).wait_recv()
        size = outs[i].shape[1]
        first = (chip * 2 + core) * size

        def body(at, i=i, first=first):
            for a in range(outs[i].shape[0]):
                spot = pl.ds(at, step)
                total = ins[i][a, pl.ds(pl.multiple_of(first + at, step), step), :].astype(F32)
                total += near[i][3, a, spot, :].astype(F32)
                total += land[i][0, a, spot, :].astype(F32)
                total += land[i][1, a, spot, :].astype(F32)
                outs[i][a, spot, :] = total.astype(outs[i].dtype)

        each(i, size, body)
    for i in every:
        for j in range(4):
            near_copy(i, j).wait_send()
        for part in range(2):
            side_copy(i, part).wait_send()
            for which in range(2):
                land_copy(i, which, part).wait_send()


def plane_scatter(fulls, ident, out_dtype=F32):
    count = len(fulls)
    parts = lax.axis_size("col")
    shapes = [(f.shape[0], f.shape[1] // parts, f.shape[2]) for f in fulls]
    scratch = []
    scratch += [pltpu.VMEM((4,) + s, BF16) for s in shapes]
    scratch += [pltpu.VMEM((3,) + s, BF16) for s in shapes]
    scratch += [pltpu.VMEM((2, s[0], s[1] // 2, s[2]), BF16) for s in shapes]
    scratch += [pltpu.VMEM((2,) + s, BF16) for s in shapes]
    return pl.pallas_call(
        functools.partial(plane_scatter_kernel, count),
        out_shape=[jax.ShapeDtypeStruct(s, out_dtype) for s in shapes],
        in_specs=[pl.BlockSpec(memory_space=pltpu.VMEM)] * count,
        out_specs=[pl.BlockSpec(memory_space=pltpu.VMEM)] * count,
        scratch_shapes=scratch
        + [pltpu.SemaphoreType.DMA((count, 10)), pltpu.SemaphoreType.DMA((count, 10))],
        compiler_params=pltpu.CompilerParams(collective_id=ident, has_side_effects=True),
        name="plane_scatter",
    )(*fulls)


def spans(total, most):
    return [(at, min(most, total - at)) for at in range(0, total, most)]


def remote(src, dst, send_sem, recv_sem, peer):
    return pltpu.make_async_remote_copy(
        src_ref=src,
        dst_ref=dst,
        send_sem=send_sem,
        recv_sem=recv_sem,
        device_id={"col": peer},
        device_id_type=MESH,
    )


def block_gather(source, land, send_sem, recv_sem):
    chip, beside, above, across, core = plane_places()
    half = source.shape[0] // 2
    mine, partner, other = chip * 2 + core, chip * 2 + 1 - core, 1 - core
    to_x, to_y, far = beside * 2 + core, above * 2 + core, across * 2 + core

    def copy(k, slot, part, peer, own=False):
        spot = land.at[slot] if part is None else land.at[slot, pl.ds(part * half, half), :]
        return remote(source if own else spot, spot, send_sem.at[k], recv_sem.at[k], peer)

    def first():
        greet((partner, to_x, to_y))
        copy(1, mine, None, to_x, True).start()
        copy(2, mine, None, to_y, True).start()
        copy(0, mine, None, partner, True).start()

    def second():
        copy(1, to_x, None, to_x).wait_recv()
        copy(3, to_x, 0, to_y).start()
        copy(5, to_x, None, partner).start()
        copy(2, to_y, None, to_y).wait_recv()
        copy(4, to_y, 1, to_x).start()
        copy(6, to_y, None, partner).start()

    def third():
        copy(3, far, 0, to_y).wait_recv()
        copy(7, far, 0, partner).start()
        copy(4, far, 1, to_x).wait_recv()
        copy(8, far, 1, partner).start()

    def landed(k):
        slot = (partner, beside * 2 + other, above * 2 + other)[k]
        copy((0, 5, 6)[k], slot, None, partner).wait_recv()

    def landed_far():
        copy(7, across * 2 + other, 0, partner).wait_recv()
        copy(8, across * 2 + other, 1, partner).wait_recv()

    def sent():
        for k, slot, part in (
            (0, mine, None), (1, mine, None), (2, mine, None), (3, to_x, 0), (4, to_y, 1),
            (5, to_x, None), (6, to_y, None), (7, far, 0), (8, far, 1),
        ):
            copy(k, slot, part, partner).wait_send()

    return first, second, third, landed, landed_far, sent


def spread(index, rows):
    return pl.ds(pl.multiple_of(index * rows, rows), rows)


def ffn_gate_kernel(
    normed, gate_t, normed_rows, gate_act, land, tiles, send_sem, recv_sem, keep_sem, tile_sem
):
    chip, _, _, _, core = plane_places()
    low, high = chip % 2, chip // 2
    rows = normed.shape[0]
    first, second, third, landed, landed_far, sent = block_gather(
        normed, land, send_sem, recv_sem
    )

    def keep(slot):
        return pltpu.make_async_copy(
            land.at[slot], normed_rows.at[spread(slot, rows), :], keep_sem.at[slot]
        )

    def put(slot, parity):
        return pltpu.make_async_copy(
            tiles.at[parity], gate_act.at[spread(slot, rows), :], tile_sem.at[parity]
        )

    first()
    land[chip * 2 + core] = normed[...]

    def step(s, _):
        flip = s // 2
        at_chip = (high + flip // 2) % 2 * 2 + (low + flip) % 2
        slot = at_chip * 2 + (core + s) % 2
        parity = s % 2

        @pl.when(s == 1)
        def _():
            landed(0)

        @pl.when(s == 2)
        def _():
            second()

        @pl.when(s == 3)
        def _():
            landed(1)

        @pl.when(s == 5)
        def _():
            landed(2)

        @pl.when(s == 6)
        def _():
            third()

        @pl.when(s == 7)
        def _():
            landed_far()

        keep(slot).start()

        @pl.when(s >= 2)
        def _():
            put(slot, parity).wait()

        for at, wide in spans(gate_t.shape[0], 512):
            tiles[parity, :, at : at + wide] = dot_nt(land[slot], gate_t[at : at + wide, :])
        put(slot, parity).start()
        return 0

    lax.fori_loop(0, 8, step, 0)
    for parity in range(2):
        put(0, parity).wait()

    def drain(slot, _):
        keep(slot).wait()
        return 0

    lax.fori_loop(0, 8, drain, 0)
    sent()


def ffn_gate(normed, gate_t, ident):
    rows, depth = normed.shape
    wide = gate_t.shape[0]
    dma = pltpu.SemaphoreType.DMA
    return pl.pallas_call(
        ffn_gate_kernel,
        out_shape=[
            jax.ShapeDtypeStruct((rows * 8, depth), BF16),
            jax.ShapeDtypeStruct((rows * 8, wide), F32),
        ],
        in_specs=[pl.BlockSpec(memory_space=pltpu.VMEM)] * 2,
        out_specs=[pl.BlockSpec(memory_space=pl.ANY)] * 2,
        scratch_shapes=[
            pltpu.VMEM((8, rows, depth), BF16),
            pltpu.VMEM((2, rows, wide), F32),
            dma((9,)),
            dma((9,)),
            dma((8,)),
            dma((2,)),
        ],
        compiler_params=pltpu.CompilerParams(collective_id=ident, has_side_effects=True),
        name="ffn_gate",
    )(normed, gate_t)


def ffn_up_kernel(
    cotangent,
    up_t,
    normed_rows,
    gate_act,
    out_rows,
    hidden,
    silu,
    slope,
    land,
    rows_in,
    gate_in,
    tiles,
    send_sem,
    recv_sem,
    keep_sem,
    in_sem,
    tile_sem,
):
    chip, _, _, _, core = plane_places()
    rows = cotangent.shape[0]
    first, second, third, landed, landed_far, sent = block_gather(
        cotangent, land, send_sem, recv_sem
    )

    def fetch(kind, s, parity):
        source = (normed_rows, gate_act)[kind]
        target = (rows_in, gate_in)[kind]
        return pltpu.make_async_copy(
            source.at[spread(s, rows), :], target.at[parity], in_sem.at[kind, parity]
        )

    def keep(slot):
        return pltpu.make_async_copy(
            land.at[slot], out_rows.at[spread(slot, rows), :], keep_sem.at[slot]
        )

    def put(kind, s, parity):
        target = (hidden, silu, slope)[kind]
        return pltpu.make_async_copy(
            tiles.at[kind, parity], target.at[spread(s, rows), :], tile_sem.at[kind, parity]
        )

    first()
    fetch(0, 0, 0).start()
    fetch(1, 0, 0).start()
    land[chip * 2 + core] = cotangent[...]

    def step(s, _):
        parity = s % 2

        @pl.when(s < 7)
        def _():
            fetch(0, s + 1, 1 - parity).start()
            fetch(1, s + 1, 1 - parity).start()

        @pl.when(s == 7)
        def _():
            second()

        @pl.when(s >= 2)
        def _():
            for kind in range(3):
                put(kind, s, parity).wait()

        fetch(0, s, parity).wait()
        fetch(1, s, parity).wait()
        for at, wide in spans(up_t.shape[0], 512):
            cut = slice(at, at + wide)
            up = dot_nt(rows_in[parity], up_t[cut, :])
            gate = gate_in[parity, :, cut]
            sigma = 1.0 / (1.0 + jnp.exp(-gate))
            smooth = gate * sigma
            tiles[0, parity, :, cut] = (smooth * up).astype(BF16)
            tiles[1, parity, :, cut] = smooth.astype(BF16)
            tiles[2, parity, :, cut] = (up * sigma * (1.0 + gate * (1.0 - sigma))).astype(BF16)
        for kind in range(3):
            put(kind, s, parity).start()
        return 0

    lax.fori_loop(0, 8, step, 0)
    landed(0)
    third()
    landed(1)
    landed(2)
    landed_far()

    def store(slot, _):
        keep(slot).start()
        return 0

    def drain(slot, _):
        keep(slot).wait()
        return 0

    lax.fori_loop(0, 8, store, 0)
    for parity in range(2):
        for kind in range(3):
            put(kind, 0, parity).wait()
    lax.fori_loop(0, 8, drain, 0)
    sent()


def ffn_up(cotangent, up_t, normed_rows, gate_act, ident):
    rows, depth = cotangent.shape
    wide = up_t.shape[0]
    dma = pltpu.SemaphoreType.DMA
    vmem = pl.BlockSpec(memory_space=pltpu.VMEM)
    anywhere = pl.BlockSpec(memory_space=pl.ANY)
    return pl.pallas_call(
        ffn_up_kernel,
        out_shape=[jax.ShapeDtypeStruct((rows * 8, depth), BF16)]
        + [jax.ShapeDtypeStruct((rows * 8, wide), BF16)] * 3,
        in_specs=[vmem, vmem, anywhere, anywhere],
        out_specs=[anywhere] * 4,
        scratch_shapes=[
            pltpu.VMEM((8, rows, depth), BF16),
            pltpu.VMEM((2, rows, depth), BF16),
            pltpu.VMEM((2, rows, wide), F32),
            pltpu.VMEM((3, 2, rows, wide), BF16),
            dma((9,)),
            dma((9,)),
            dma((8,)),
            dma((2, 2)),
            dma((3, 2)),
        ],
        compiler_params=pltpu.CompilerParams(collective_id=ident, has_side_effects=True),
        name="ffn_up",
    )(cotangent, up_t, normed_rows, gate_act)


def ffn_backward_kernel(
    out_rows,
    hidden,
    silu,
    slope,
    gate_t,
    up_t,
    down,
    gate_grad,
    up_grad,
    branch_own,
    normed_own,
    out_in,
    tiles_in,
    tiles_out,
    give,
    near,
    made,
    side,
    land,
    near_send,
    near_recv,
    side_send,
    side_recv,
    land_send,
    land_recv,
    in_sem,
    tile_sem,
):
    chip, beside, above, across, core = plane_places()
    low, high = chip % 2, chip // 2
    own_rows = branch_own.shape[0]
    half = own_rows // 2
    depth = branch_own.shape[1]
    partner = chip * 2 + 1 - core
    to_x, to_y = beside * 2 + core, above * 2 + core
    greet((partner, to_x, to_y))
    finals = (branch_own, normed_own)

    def spread(index):
        return pl.ds(pl.multiple_of(index * own_rows, own_rows), own_rows)

    def slot_of(s):
        flip = 3 - s // 2
        at_chip = (high + flip // 2) % 2 * 2 + (low + flip) % 2
        return at_chip * 2 + (core + 1 + s) % 2

    def near_copy(a, j):
        return remote(
            give.at[a, j], near.at[a, j], near_send.at[a, j], near_recv.at[a, j], partner
        )

    def side_copy(a, part):
        return remote(
            made.at[a, 0, pl.ds(part * half, half), :], side.at[a, part],
            side_send.at[a, part], side_recv.at[a, part], to_x if part == 0 else to_y,
        )

    def land_copy(a, which, part):
        k = which * 2 + part
        return remote(
            made.at[a, 1 + which, pl.ds(part * half, half), :],
            land.at[a, which, pl.ds(part * half, half), :],
            land_send.at[a, k], land_recv.at[a, k], to_x if which == 0 else to_y,
        )

    def fold(a, which, part):
        def tile(t, _):
            at = pl.multiple_of(t * 16, 16)
            spot = pl.ds(pl.multiple_of(part * half + at, 16), 16)
            left = made[a, 1 + which, spot, :].astype(F32)
            right = side[a, 1 - which, pl.ds(at, 16), :].astype(F32)
            made[a, 1 + which, spot, :] = (left + right).astype(BF16)
            return 0

        lax.fori_loop(0, half // 16, tile, 0)

    def fetch(kind, s, parity):
        if kind == 0:
            return pltpu.make_async_copy(
                out_rows.at[spread(slot_of(s)), :], out_in.at[parity], in_sem.at[0, parity]
            )
        source = (hidden, silu, slope)[kind - 1]
        return pltpu.make_async_copy(
            source.at[spread(slot_of(s)), :], tiles_in.at[kind - 1, parity], in_sem.at[kind, parity]
        )

    def put(kind, s, parity):
        target = (gate_grad, up_grad)[kind]
        return pltpu.make_async_copy(
            tiles_out.at[kind, parity], target.at[spread(slot_of(s)), :],
            tile_sem.at[kind, parity],
        )

    def sides(a):
        side_copy(a, 0).wait_recv()
        fold(a, 1, 0)
        land_copy(a, 1, 0).start()
        side_copy(a, 1).wait_recv()
        fold(a, 0, 1)
        land_copy(a, 0, 1).start()

    def deliver(a, s, partial):
        j = s // 2

        @pl.when(s % 2 == 0)
        def _():
            give[a, j] = partial().astype(BF16)
            near_copy(a, j).start()

        @pl.when(s % 2 == 1)
        def _():
            total = partial()
            near_copy(a, j).wait_recv()
            total = total + near[a, j].astype(F32)

            @pl.when(j < 3)
            def _():
                made[a, (3 - j) % 3] = total.astype(BF16)

            @pl.when(j == 0)
            def _():
                side_copy(a, 0).start()
                side_copy(a, 1).start()

            @pl.when(j == 1)
            def _():
                land_copy(a, 1, 1).start()

            @pl.when(j == 2)
            def _():
                land_copy(a, 0, 0).start()
                sides(a)

            @pl.when(j == 3)
            def _():
                finals[a][...] = total

    fetch(1, 0, 0).start()

    def branch_step(s, _):
        parity = s % 2

        @pl.when(s < 7)
        def _():
            fetch(1, s + 1, (s + 1) % 2).start()

        @pl.when(s == 6)
        def _():
            for kind in (0, 2, 3):
                fetch(kind, 0, 0).start()

        fetch(1, s, parity).wait()
        deliver(0, s, lambda: dot_nn(tiles_in[0, parity], down[...]))
        return 0

    lax.fori_loop(0, 8, branch_step, 0)

    def normed_step(s, _):
        parity = s % 2

        @pl.when(s < 7)
        def _():
            for kind in (0, 2, 3):
                fetch(kind, s + 1, (s + 1) % 2).start()

        for kind in (0, 2, 3):
            fetch(kind, s, parity).wait()

        @pl.when(s >= 2)
        def _():
            for kind in range(2):
                put(kind, s, parity).wait()

        for at, wide in spans(down.shape[0], 512):
            cut = slice(at, at + wide)
            hidden_grad = dot_nt(out_in[parity], down[cut, :])
            tiles_out[0, parity, :, cut] = (
                hidden_grad * tiles_in[2, parity, :, cut].astype(F32)
            ).astype(BF16)
            tiles_out[1, parity, :, cut] = (
                hidden_grad * tiles_in[1, parity, :, cut].astype(F32)
            ).astype(BF16)
        for kind in range(2):
            put(kind, s, parity).start()
        deliver(
            1, s,
            lambda: dot_nn(tiles_out[0, parity], gate_t[...])
            + dot_nn(tiles_out[1, parity], up_t[...]),
        )
        return 0

    lax.fori_loop(0, 8, normed_step, 0)
    for a in range(2):
        for which in range(2):
            for part in range(2):
                land_copy(a, which, part).wait_recv()

        def tile(t, _, a=a):
            spot = pl.ds(pl.multiple_of(t * 16, 16), 16)
            finals[a][spot, :] = (
                finals[a][spot, :]
                + land[a, 0, spot, :].astype(F32)
                + land[a, 1, spot, :].astype(F32)
            )
            return 0

        lax.fori_loop(0, own_rows // 16, tile, 0)
    for a in range(2):
        for j in range(4):
            near_copy(a, j).wait_send()
        for part in range(2):
            side_copy(a, part).wait_send()
            for which in range(2):
                land_copy(a, which, part).wait_send()
    for kind in range(2):
        for parity in range(2):
            put(kind, parity, parity).wait()


def ffn_backward(out_rows, hidden, silu, slope, gate_t, up_t, down, ident):
    total, depth = out_rows.shape
    wide = down.shape[0]
    rows = total // 8
    vmem = pl.BlockSpec(memory_space=pltpu.VMEM)
    anywhere = pl.BlockSpec(memory_space=pl.ANY)
    dma = pltpu.SemaphoreType.DMA
    return pl.pallas_call(
        ffn_backward_kernel,
        out_shape=[jax.ShapeDtypeStruct((total, wide), BF16)] * 2
        + [jax.ShapeDtypeStruct((rows, depth), F32)] * 2,
        in_specs=[anywhere] * 4 + [vmem] * 3,
        out_specs=[anywhere] * 2 + [vmem] * 2,
        scratch_shapes=[
            pltpu.VMEM((2, rows, depth), BF16),
            pltpu.VMEM((3, 2, rows, wide), BF16),
            pltpu.VMEM((2, 2, rows, wide), BF16),
            pltpu.VMEM((2, 4, rows, depth), BF16),
            pltpu.VMEM((2, 4, rows, depth), BF16),
            pltpu.VMEM((2, 3, rows, depth), BF16),
            pltpu.VMEM((2, 2, rows // 2, depth), BF16),
            pltpu.VMEM((2, 2, rows, depth), BF16),
            dma((2, 4)),
            dma((2, 4)),
            dma((2, 2)),
            dma((2, 2)),
            dma((2, 4)),
            dma((2, 4)),
            dma((4, 2)),
            dma((2, 2)),
        ],
        compiler_params=pltpu.CompilerParams(collective_id=ident, has_side_effects=True),
        name="ffn_backward",
    )(out_rows, hidden, silu, slope, gate_t, up_t, down)


def gather_row(block):
    return lax.all_gather(block, "row", axis=block.ndim - 1, tiled=True)


def scatter_row(full):
    return lax.psum_scatter(
        full.astype(BF16), "row", scatter_dimension=0, tiled=True
    )


def gather_col(blocks, ident):
    if lax.axis_size("col") == 8:
        return plane_gather(blocks, ident)
    return [lax.all_gather(block, "col", axis=1, tiled=True) for block in blocks]


def scatter_col(fulls, ident):
    fulls = [full.astype(BF16) for full in fulls]
    if lax.axis_size("col") == 8:
        return plane_scatter(fulls, ident)
    return [
        lax.psum_scatter(full, "col", scatter_dimension=1, tiled=True).astype(F32)
        for full in fulls
    ]


def line_remote(src, dst, send_sem, recv_sem, peer):
    return pltpu.make_async_remote_copy(
        src_ref=src,
        dst_ref=dst,
        send_sem=send_sem,
        recv_sem=recv_sem,
        device_id={"row": peer},
        device_id_type=MESH,
    )


def greet_grid(peers, place, places):
    barrier = pltpu.get_barrier_semaphore()
    for peer in peers:
        pl.semaphore_signal(barrier, inc=1, device_id={"col": peer}, device_id_type=MESH)

    @pl.when(place > 0)
    def _():
        pl.semaphore_signal(barrier, inc=1, device_id={"row": place - 1}, device_id_type=MESH)

    @pl.when(place < places - 1)
    def _():
        pl.semaphore_signal(barrier, inc=1, device_id={"row": place + 1}, device_id_type=MESH)

    edge = (place == 0) | (place == places - 1)

    @pl.when(edge)
    def _():
        pl.semaphore_wait(barrier, len(peers) + 1)

    @pl.when(jnp.logical_not(edge))
    def _():
        pl.semaphore_wait(barrier, len(peers) + 2)


def grid_gather_kernel(count, places, *refs):
    ins, outs = refs[:count], refs[count : 2 * count]
    send_sem, recv_sem, line_send, line_recv, own_sem = refs[2 * count :]
    place = lax.axis_index("row")
    chip, beside, above, across, core = plane_places()
    mine, partner, other = chip * 2 + core, chip * 2 + 1 - core, 1 - core
    to_x, to_y, far = beside * 2 + core, above * 2 + core, across * 2 + core
    every = range(count)
    greet_grid((partner, to_x, to_y), place, places)

    def view(i, slot, line, part):
        size, wide = ins[i].shape
        spot = pl.ds(pl.multiple_of(line * wide, wide), wide)
        if part is None:
            return outs[i].at[pl.ds(pl.multiple_of(slot * size, size), size), spot]
        half = size // 2
        return outs[i].at[pl.ds(pl.multiple_of(slot * size + part * half, half), half), spot]

    def copies(k, slot, line, part, peer, own=False):
        return [
            remote(
                ins[i] if own else view(i, slot, line, part),
                view(i, slot, line, part),
                send_sem.at[i, line, k],
                recv_sem.at[i, line, k],
                peer,
            )
            for i in every
        ]

    def line_copies(line, sem_at, peer, own=False):
        return [
            line_remote(
                ins[i] if own else view(i, mine, line, None),
                view(i, mine, line, None),
                line_send.at[i, sem_at],
                line_recv.at[i, line],
                peer,
            )
            for i in every
        ]

    def start(cs):
        for c in cs:
            c.start()

    def wait_recv(cs):
        for c in cs:
            c.wait_recv()

    def first(line, own=False):
        start(copies(1, mine, line, None, to_x, own))
        start(copies(2, mine, line, None, to_y, own))
        start(copies(0, mine, line, None, partner, own))

    def second(line):
        wait_recv(copies(1, to_x, line, None, to_x))
        start(copies(3, to_x, line, 0, to_y))
        start(copies(5, to_x, line, None, partner))
        wait_recv(copies(2, to_y, line, None, to_y))
        start(copies(4, to_y, line, 1, to_x))
        start(copies(6, to_y, line, None, partner))

    def third(line):
        wait_recv(copies(3, far, line, 0, to_y))
        start(copies(7, far, line, 0, partner))
        wait_recv(copies(4, far, line, 1, to_x))
        start(copies(8, far, line, 1, partner))

    def last(line):
        wait_recv(copies(0, partner, line, None, partner))
        wait_recv(copies(5, beside * 2 + other, line, None, partner))
        wait_recv(copies(6, above * 2 + other, line, None, partner))
        wait_recv(copies(7, across * 2 + other, line, 0, partner))
        wait_recv(copies(8, across * 2 + other, line, 1, partner))
        for k, slot, part in (
            (0, mine, None), (1, mine, None), (2, mine, None), (3, to_x, 0), (4, to_y, 1),
            (5, to_x, None), (6, to_y, None), (7, far, 0), (8, far, 1),
        ):
            for c in copies(k, slot, line, part, partner):
                c.wait_send()

    def both(distance, body):
        @pl.when((distance >= 1) & (place - distance >= 0))
        def _():
            body(place - distance)

        @pl.when((distance >= 1) & (place + distance < places))
        def _():
            body(place + distance)

        @pl.when(distance == 0)
        def _():
            body(place)

    @pl.when(place < places - 1)
    def _():
        start(line_copies(place, place, place + 1, True))

    @pl.when(place > 0)
    def _():
        start(line_copies(place, places, place - 1, True))

    first(place, True)
    own = [
        pltpu.make_async_copy(ins[i], view(i, mine, place, None), own_sem.at[i]) for i in every
    ]
    start(own)

    def step(t, _):
        @pl.when((t >= 1) & (place - t >= 0))
        def _():
            line = place - t
            wait_recv(line_copies(line, line, place))

            @pl.when(place < places - 1)
            def _():
                start(line_copies(line, line, place + 1))

            first(line)

        @pl.when((t >= 1) & (place + t < places))
        def _():
            line = place + t
            wait_recv(line_copies(line, line, place))

            @pl.when(place > 0)
            def _():
                start(line_copies(line, line, place - 1))

            first(line)

        both(t - 1, second)
        both(t - 2, third)
        return 0

    lax.fori_loop(0, places + 2, step, 0)

    def finish(line, _):
        last(line)

        @pl.when((line < place) & (place < places - 1))
        def _():
            for c in line_copies(line, line, place):
                c.wait_send()

        @pl.when((line > place) & (place > 0))
        def _():
            for c in line_copies(line, line, place):
                c.wait_send()

        return 0

    lax.fori_loop(0, places, finish, 0)

    @pl.when(place < places - 1)
    def _():
        for c in line_copies(place, place, place):
            c.wait_send()

    @pl.when(place > 0)
    def _():
        for c in line_copies(place, places, place):
            c.wait_send()

    for c in own:
        c.wait()


def grid_gather(shards, ident):
    count = len(shards)
    places, parts = lax.axis_size("row"), lax.axis_size("col")
    dma = pltpu.SemaphoreType.DMA
    anywhere = pl.BlockSpec(memory_space=pl.ANY)
    return pl.pallas_call(
        functools.partial(grid_gather_kernel, count, places),
        out_shape=[
            jax.ShapeDtypeStruct((s.shape[0] * parts, s.shape[1] * places), s.dtype)
            for s in shards
        ],
        in_specs=[anywhere] * count,
        out_specs=[anywhere] * count,
        scratch_shapes=[
            dma((count, places, 9)),
            dma((count, places, 9)),
            dma((count, places + 1)),
            dma((count, places)),
            dma((count,)),
        ],
        compiler_params=pltpu.CompilerParams(collective_id=ident, has_side_effects=True),
        name="grid_gather",
    )(*shards)


def grid_scatter_kernel(count, places, *refs):
    ins, outs = refs[:count], refs[count : 2 * count]
    scratch = refs[2 * count :]
    near, made, side, land, line_in, line_out = (
        scratch[i * count : (i + 1) * count] for i in range(6)
    )
    (
        near_send, near_recv, side_send, side_recv, land_send, land_recv, line_send, line_recv,
    ) = scratch[6 * count :]
    place = lax.axis_index("row")
    chip, beside, above, across, core = plane_places()
    partner = chip * 2 + 1 - core
    to_x, to_y = beside * 2 + core, above * 2 + core
    order = (across, beside, above, chip)
    every = range(count)
    greet_grid((partner, to_x, to_y), place, places)

    def source(i, slot, line, at, size):
        rows, wide = outs[i].shape
        return (
            pl.ds(pl.multiple_of(slot * rows + at, size), size),
            pl.ds(pl.multiple_of(line * wide, wide), wide),
        )

    def near_copy(i, line, j):
        rows = outs[i].shape[0]
        return remote(
            ins[i].at[source(i, order[j] * 2 + 1 - core, line, 0, rows)],
            near[i].at[line, j],
            near_send.at[i, line, j], near_recv.at[i, line, j], partner,
        )

    def halves(i, part):
        half = outs[i].shape[0] // 2
        return pl.ds(part * half, half)

    def side_copy(i, line, part):
        return remote(
            made[i].at[line, 0, halves(i, part), :], side[i].at[line, part],
            side_send.at[i, line, part], side_recv.at[i, line, part],
            to_x if part == 0 else to_y,
        )

    def land_copy(i, line, which, part):
        k = which * 2 + part
        return remote(
            made[i].at[line, 1 + which, halves(i, part), :],
            land[i].at[line, which, halves(i, part), :],
            land_send.at[i, line, k], land_recv.at[i, line, k],
            to_x if which == 0 else to_y,
        )

    def up_copy(i, line):
        return line_remote(
            line_out[i].at[line], line_in[i].at[line],
            line_send.at[i, line], line_recv.at[i, line], place + 1,
        )

    def down_copy(i, line):
        target = jnp.where(line == place - 1, places, line)
        return line_remote(
            line_out[i].at[line], line_in[i].at[target],
            line_send.at[i, line], line_recv.at[i, target], place - 1,
        )

    def each(size, body):
        def tile(t, _):
            body(pl.multiple_of(t * 16, 16))
            return 0

        lax.fori_loop(0, size // 16, tile, 0)

    def combine(i, line, j):
        def body(at):
            spot = pl.ds(at, 16)
            left = ins[i][source(i, order[j] * 2 + core, line, at, 16)].astype(F32)
            made[i][line, j, spot, :] = (left + near[i][line, j, spot, :].astype(F32)).astype(
                BF16
            )

        each(outs[i].shape[0], body)

    def fold(i, line, which, part):
        half = outs[i].shape[0] // 2

        def body(at):
            spot = pl.ds(pl.multiple_of(part * half + at, 16), 16)
            left = made[i][line, 1 + which, spot, :].astype(F32)
            right = side[i][line, 1 - which, pl.ds(at, 16), :].astype(F32)
            made[i][line, 1 + which, spot, :] = (left + right).astype(BF16)

        each(half, body)

    def sequence(q):
        up = places - 1 - place
        return jnp.where(q < up, places - 1 - q, q - up)

    def first(line):
        for i in every:
            near_copy(i, line, 0).wait_recv()
            combine(i, line, 0)
            side_copy(i, line, 0).start()
            side_copy(i, line, 1).start()
        for i in every:
            near_copy(i, line, 1).wait_recv()
            combine(i, line, 1)
            land_copy(i, line, 0, 0).start()
            near_copy(i, line, 2).wait_recv()
            combine(i, line, 2)
            land_copy(i, line, 1, 1).start()

    def second(line):
        for i in every:
            side_copy(i, line, 0).wait_recv()
            fold(i, line, 1, 0)
            land_copy(i, line, 1, 0).start()
            side_copy(i, line, 1).wait_recv()
            fold(i, line, 0, 1)
            land_copy(i, line, 0, 1).start()

    def arrived(i, slot):
        line_remote(
            line_out[i].at[0], line_in[i].at[slot],
            line_send.at[i, 0], line_recv.at[i, slot], place,
        ).wait_recv()

    def third(line):
        for i in every:
            near_copy(i, line, 3).wait_recv()
            for which in range(2):
                for part in range(2):
                    land_copy(i, line, which, part).wait_recv()

        @pl.when((line > place) & (place > 0))
        def _():
            for i in every:
                arrived(i, line)

        @pl.when((line < place) & (place < places - 1))
        def _():
            for i in every:
                arrived(i, line)

        @pl.when((line == place) & (place > 0))
        def _():
            for i in every:
                arrived(i, place)

        @pl.when((line == place) & (place < places - 1))
        def _():
            for i in every:
                arrived(i, places)

        def total(i, at):
            spot = pl.ds(at, 16)
            value = ins[i][source(i, chip * 2 + core, line, at, 16)].astype(F32)
            value += near[i][line, 3, spot, :].astype(F32)
            value += land[i][line, 0, spot, :].astype(F32)
            value += land[i][line, 1, spot, :].astype(F32)
            return value

        for i in every:
            relays = ((line > place) & (place > 0)) | ((line < place) & (place < places - 1))

            @pl.when((line != place) & relays)
            def _(i=i):
                def body(at):
                    spot = pl.ds(at, 16)
                    line_out[i][line, spot, :] = (
                        total(i, at) + line_in[i][line, spot, :].astype(F32)
                    ).astype(BF16)

                each(outs[i].shape[0], body)

            @pl.when((line != place) & jnp.logical_not(relays))
            def _(i=i):
                def body(at):
                    line_out[i][line, pl.ds(at, 16), :] = total(i, at).astype(BF16)

                each(outs[i].shape[0], body)

            @pl.when(line > place)
            def _(i=i):
                up_copy(i, line).start()

            @pl.when(line < place)
            def _(i=i):
                down_copy(i, line).start()

            @pl.when(line == place)
            def _(i=i):
                def body(at):
                    outs[i][pl.ds(at, 16), :] = total(i, at)

                each(outs[i].shape[0], body)

                @pl.when(place > 0)
                def _():
                    def more(at):
                        spot = pl.ds(at, 16)
                        outs[i][spot, :] += line_in[i][place, spot, :].astype(F32)

                    each(outs[i].shape[0], more)

                @pl.when(place < places - 1)
                def _():
                    def more(at):
                        spot = pl.ds(at, 16)
                        outs[i][spot, :] += line_in[i][places, spot, :].astype(F32)

                    each(outs[i].shape[0], more)

    def begin(q, _):
        line = sequence(q)
        for j in range(4):
            for i in every:
                near_copy(i, line, j).start()
        return 0

    lax.fori_loop(0, places, begin, 0)

    def step(t, _):
        @pl.when(t < places)
        def _():
            first(sequence(t))

        @pl.when((t >= 1) & (t - 1 < places))
        def _():
            second(sequence(t - 1))

        @pl.when(t >= 2)
        def _():
            third(sequence(t - 2))

        return 0

    lax.fori_loop(0, places + 2, step, 0)

    def finish(line, _):
        for i in every:
            for j in range(4):
                near_copy(i, line, j).wait_send()
            for part in range(2):
                side_copy(i, line, part).wait_send()
                for which in range(2):
                    land_copy(i, line, which, part).wait_send()

            @pl.when(line != place)
            def _(i=i):
                up_copy(i, line).wait_send()

        return 0

    lax.fori_loop(0, places, finish, 0)


def grid_scatter(fulls, ident):
    count = len(fulls)
    places, parts = lax.axis_size("row"), lax.axis_size("col")
    shapes = [(f.shape[0] // parts, f.shape[1] // places) for f in fulls]
    dma = pltpu.SemaphoreType.DMA
    vmem = pl.BlockSpec(memory_space=pltpu.VMEM)
    scratch = []
    scratch += [pltpu.VMEM((places, 4) + s, BF16) for s in shapes]
    scratch += [pltpu.VMEM((places, 3) + s, BF16) for s in shapes]
    scratch += [pltpu.VMEM((places, 2, s[0] // 2, s[1]), BF16) for s in shapes]
    scratch += [pltpu.VMEM((places, 2) + s, BF16) for s in shapes]
    scratch += [pltpu.VMEM((places + 1,) + s, BF16) for s in shapes]
    scratch += [pltpu.VMEM((places,) + s, BF16) for s in shapes]
    return pl.pallas_call(
        functools.partial(grid_scatter_kernel, count, places),
        out_shape=[jax.ShapeDtypeStruct(s, F32) for s in shapes],
        in_specs=[vmem] * count,
        out_specs=[vmem] * count,
        scratch_shapes=scratch
        + [
            dma((count, places, 4)),
            dma((count, places, 4)),
            dma((count, places, 2)),
            dma((count, places, 2)),
            dma((count, places, 4)),
            dma((count, places, 4)),
            dma((count, places)),
            dma((count, places + 1)),
        ],
        compiler_params=pltpu.CompilerParams(collective_id=ident, has_side_effects=True),
        name="grid_scatter",
    )(*fulls)


def gather_weights(blocks, ident):
    places = lax.axis_size("row")
    if lax.axis_size("col") == 8 and places > 1 and blocks[0].shape[1] % 128 == 0:
        return grid_gather(blocks, ident)
    return [
        full[0] for full in gather_col([gather_row(block)[None] for block in blocks], ident)
    ]


def scatter_weights(fulls, ident):
    places = lax.axis_size("row")
    if lax.axis_size("col") == 8 and places > 1 and fulls[0].shape[1] // places % 128 == 0:
        return grid_scatter(fulls, ident)
    return [
        lax.psum_scatter(
            part[0].astype(BF16), "row", scatter_dimension=1, tiled=True
        ).astype(F32)
        for part in scatter_col([full[None] for full in fulls], ident)
    ]


def shards(
    hidden_in,
    out_grad,
    seq_lengths,
    norm1_gain,
    q_weight,
    q_bias,
    k_weight,
    k_bias,
    v_weight,
    v_bias,
    o_weight,
    norm2_gain,
    gate_weight,
    up_weight,
    down_weight,
):
    row_parts = lax.axis_size("row")
    col_parts = lax.axis_size("col")
    col_place = lax.axis_index("col")
    depth_own = q_weight.shape[0]
    depth = depth_own * row_parts
    q_own, k_own = q_weight.shape[1], k_weight.shape[1]
    smalls = (q_bias, k_bias, v_bias, norm1_gain, norm2_gain)
    small_sizes = [member.shape[0] for member in smalls]
    packed_small = jnp.concatenate(smalls)
    packed_small = jnp.pad(packed_small, (0, k_own * depth_own - packed_small.shape[0]))
    query_t, output_t, key_t, value_t, small_t = gather_weights(
        [
            q_weight.T,
            o_weight.T,
            k_weight.T,
            v_weight.T,
            packed_small.reshape(k_own, depth_own),
        ],
        1,
    )
    small_flat = small_t.reshape(col_parts, k_own, row_parts, depth_own)
    small_flat = small_flat.transpose(2, 0, 1, 3).reshape(row_parts * col_parts, -1)
    small_full, offset = [], 0
    for size in small_sizes:
        small_full.append(small_flat[:, offset : offset + size].reshape(-1))
        offset += size
    query_offset, key_offset, value_offset, first_gain, second_gain = small_full

    gate_t = gather_row(gate_weight.T)
    up_t = gather_row(up_weight.T)
    down_block = gather_row(down_weight)

    own_rows = hidden_in.shape[0]
    row_tokens = own_rows * col_parts
    lengths = seq_lengths[0]
    query_slots = col_place * own_rows + jnp.arange(own_rows, dtype=jnp.int32)
    query_starts = seq_starts(query_slots, lengths)
    cosines, sines = rope_tables(query_slots - query_starts, HD)
    group_size = HQ // KVH
    score_scale = 1.0 / math.sqrt(HD)
    inputs_wide = hidden_in.astype(F32)
    first_rms = rms_scale(inputs_wide)
    first_unit = inputs_wide * first_rms
    first_normed = (first_unit * first_gain.astype(F32)).astype(BF16)
    query_base = dot_nt(first_normed, query_t) + query_offset.astype(F32)
    key_base = dot_nt(first_normed, key_t) + key_offset.astype(F32)
    value_own = (dot_nt(first_normed, value_t) + value_offset.astype(F32)).astype(BF16)
    queries = rotate_pairs(query_base.reshape(own_rows, HQ, HD), cosines, sines).astype(BF16)
    keys_own = rotate_pairs(key_base.reshape(own_rows, KVH, HD), cosines, sines).astype(BF16)
    both_own = jnp.concatenate([keys_own.reshape(own_rows, KVH * HD), value_own], axis=1)
    both_all = gather_col([both_own[None]], 2)[0][0]
    window = min(own_rows + MAXLEN, row_tokens)
    window_start = jnp.clip(col_place * own_rows - MAXLEN, 0, row_tokens - window)
    key_slots = window_start + jnp.arange(window, dtype=jnp.int32)
    key_starts = seq_starts(key_slots, lengths)
    visible = (query_starts[:, None] == key_starts[None, :]) & (
        key_slots[None, :] <= query_slots[:, None]
    )
    both_window = lax.dynamic_slice_in_dim(both_all, window_start, window, 0)
    keys_window = both_window[:, : KVH * HD].reshape(window, KVH, HD)
    values_window = both_window[:, KVH * HD :].reshape(window, KVH, HD)
    query_heads = queries.reshape(own_rows, KVH, group_size, HD)
    scores = masked_scores(query_heads, keys_window, visible, score_scale)
    peak = jnp.max(scores, axis=-1, keepdims=True)
    expanded = jnp.exp(scores - peak)
    totals = jnp.sum(expanded, axis=-1, keepdims=True)
    probs = expanded / totals
    log_total = peak + jnp.log(totals)
    mixed = jnp.einsum(
        "kgts,skd->tkgd", probs.astype(BF16), values_window, preferred_element_type=F32
    )
    mixed = mixed.reshape(own_rows, HQ * HD).astype(BF16)
    residual = inputs_wide + dot_nt(mixed, output_t)
    second_rms = rms_scale(residual)
    second_unit = residual * second_rms
    second_normed = (second_unit * second_gain.astype(F32)).astype(BF16)
    kernels = col_parts == 8
    if kernels:
        normed_rows, gate_act = ffn_gate(second_normed, gate_t, 3)
        out_rows, hidden, silu_gate, slope = ffn_up(out_grad, up_t, normed_rows, gate_act, 7)
    else:
        normed_rows, out_rows = (
            member[0] for member in gather_col([second_normed[None], out_grad[None]], 3)
        )
        gate_act = dot_nt(normed_rows, gate_t)
        up_act = dot_nt(normed_rows, up_t)
        sigmoid_gate = jax.nn.sigmoid(gate_act)
        silu_gate = gate_act * sigmoid_gate
        slope = up_act * sigmoid_gate * (1.0 + gate_act * (1.0 - sigmoid_gate))
        hidden = (silu_gate * up_act).astype(BF16)
    down_grad = dot_tn(out_rows, hidden).astype(BF16)
    down_grad, out_rows = lax.optimization_barrier((down_grad, out_rows))
    down_grad_own = scatter_row(down_grad)
    if kernels:
        gate_grad_act, up_grad_act, branch_out, normed_grad = ffn_backward(
            out_rows, hidden, silu_gate, slope, gate_t, up_t, down_block, 4
        )
    else:
        hidden_grad = dot_nt(out_rows, down_block)
        up_grad_act = (hidden_grad * silu_gate).astype(BF16)
        gate_grad_act = (hidden_grad * slope).astype(BF16)
        normed_part = dot_nn(gate_grad_act, gate_t) + dot_nn(up_grad_act, up_t)
        branch_part = dot_nn(hidden, down_block)
        normed_grad, branch_out = (
            member[0] for member in scatter_col([normed_part[None], branch_part[None]], 4)
        )
    gate_grad = dot_tn(normed_rows, gate_grad_act).astype(BF16)
    up_grad = dot_tn(normed_rows, up_grad_act).astype(BF16)
    gate_grad, up_grad, normed_grad = lax.optimization_barrier(
        (gate_grad, up_grad, normed_grad)
    )
    gate_grad_own = scatter_row(gate_grad)
    up_grad_own = scatter_row(up_grad)
    layer_out = residual + branch_out
    second_gain_grad = jnp.sum(normed_grad * second_unit, axis=0)
    unit_grad = normed_grad * second_gain.astype(F32)
    residual_grad = out_grad.astype(F32) + second_rms * (
        unit_grad - second_unit * jnp.mean(unit_grad * second_unit, axis=-1, keepdims=True)
    )
    attended_grad = residual_grad.astype(BF16)
    mixed_grad = dot_nn(attended_grad, output_t).astype(BF16)
    grad_heads = mixed_grad.reshape(own_rows, KVH, group_size, HD)
    scores = masked_scores(query_heads, keys_window, visible, score_scale)
    probs = jnp.exp(scores - log_total)
    prob_grad = jnp.einsum(
        "tkgd,skd->kgts", grad_heads, values_window, preferred_element_type=F32
    )
    value_part = jnp.einsum(
        "kgts,tkgd->skd", probs.astype(BF16), grad_heads, preferred_element_type=F32
    )
    score_grad = (
        probs * (prob_grad - jnp.sum(probs * prob_grad, axis=-1, keepdims=True))
    ).astype(BF16)
    query_grad = (
        jnp.einsum("kgts,skd->tkgd", score_grad, keys_window, preferred_element_type=F32)
        * score_scale
    )
    key_part = (
        jnp.einsum("kgts,tkgd->skd", score_grad, query_heads, preferred_element_type=F32)
        * score_scale
    )
    both_part = jnp.concatenate(
        [key_part.reshape(window, KVH * HD), value_part.reshape(window, KVH * HD)], axis=1
    ).astype(BF16)
    both_rows = lax.dynamic_update_slice_in_dim(
        jnp.zeros((row_tokens, 2 * KVH * HD), BF16), both_part, window_start, 0
    )
    both_rows, down_grad_own = lax.optimization_barrier((both_rows, down_grad_own))
    both_grad = scatter_col([both_rows[None]], 5)[0][0]
    key_grad, value_grad = both_grad[:, : KVH * HD], both_grad[:, KVH * HD :]
    query_wide = rounded_wide(query_grad.reshape(own_rows, HQ, HD))
    query_base_grad = (
        rotate_back(query_wide, cosines, sines).reshape(own_rows, HQ * HD).astype(BF16)
    )
    key_wide = rounded_wide(key_grad.reshape(own_rows, KVH, HD))
    key_base_grad = (
        rotate_back(key_wide, cosines, sines).reshape(own_rows, KVH * HD).astype(BF16)
    )
    value_base_grad = value_grad.astype(BF16)
    query_b_grad = jnp.sum(query_base_grad.astype(F32), axis=0)
    key_b_grad = jnp.sum(key_base_grad.astype(F32), axis=0)
    value_b_grad = jnp.sum(value_base_grad.astype(F32), axis=0)
    first_normed_grad = (
        dot_nn(query_base_grad, query_t)
        + dot_nn(key_base_grad, key_t)
        + dot_nn(value_base_grad, value_t)
    )
    first_gain_grad = jnp.sum(first_normed_grad * first_unit, axis=0)
    first_unit_grad = first_normed_grad * first_gain.astype(F32)
    input_grad = residual_grad + first_rms * (
        first_unit_grad
        - first_unit * jnp.mean(first_unit_grad * first_unit, axis=-1, keepdims=True)
    )
    small_grads = (query_b_grad, key_b_grad, value_b_grad, first_gain_grad, second_gain_grad)
    small_flat = jnp.concatenate(
        [member.reshape(row_parts * col_parts, -1) for member in small_grads], axis=1
    )
    small_flat = jnp.pad(
        small_flat, ((0, 0), (0, k_own * depth_own - small_flat.shape[1]))
    ).reshape(row_parts, col_parts, k_own, depth_own)
    small_flat = small_flat.transpose(1, 2, 0, 3).reshape(col_parts * k_own, depth)
    query_w = dot_tn(query_base_grad, first_normed).astype(BF16)
    query_w, gate_grad_own = lax.optimization_barrier((query_w, gate_grad_own))
    query_w_out, output_w_out, key_w_out, value_w_out, small_out = scatter_weights(
        [
            query_w,
            dot_tn(attended_grad, mixed).astype(BF16),
            dot_tn(key_base_grad, first_normed).astype(BF16),
            dot_tn(value_base_grad, first_normed).astype(BF16),
            small_flat.astype(BF16),
        ],
        6,
    )
    small_out = small_out.reshape(-1)
    small_list, offset = [], 0
    for size in small_sizes:
        small_list.append(small_out[offset : offset + size])
        offset += size
    return (
        layer_out,
        input_grad,
        small_list[3],
        query_w_out.T,
        small_list[0],
        key_w_out.T,
        small_list[1],
        value_w_out.T,
        small_list[2],
        output_w_out.T,
        small_list[4],
        gate_grad_own.astype(F32),
        up_grad_own.astype(F32),
        down_grad_own.astype(F32).T,
    )


def solution(mesh):
    in_specs = (
        P(("row", "col"), None),
        P(("row", "col"), None),
        P("row", None),
        P(("row", "col")),
        P("row", "col"),
        P(("row", "col")),
        P("row", "col"),
        P(("row", "col")),
        P("row", "col"),
        P(("row", "col")),
        P("row", "col"),
        P(("row", "col")),
        P("row", "col"),
        P("row", "col"),
        P("col", "row"),
    )
    out_specs = (
        P(("row", "col"), None),
        P(("row", "col"), None),
        P(("row", "col")),
        P("row", "col"),
        P(("row", "col")),
        P("row", "col"),
        P(("row", "col")),
        P("row", "col"),
        P(("row", "col")),
        P("row", "col"),
        P(("row", "col")),
        P("row", "col"),
        P("row", "col"),
        P("col", "row"),
    )
    return jax.shard_map(shards, mesh=mesh, in_specs=in_specs, out_specs=out_specs, check_vma=False)
```

```python
import functools
import math

import jax
import jax.numpy as jnp
from jax import lax
from jax.experimental import pallas as pl
from jax.experimental.pallas import tpu as pltpu
from jax.sharding import PartitionSpec as P

HQ = 12
KVH = 2
HD = 128
MAXLEN = 1024

EPSILON = 1e-06
ROPE_BASE = 1000000.0
BF16 = jnp.bfloat16
F32 = jnp.float32
MESH = pl.DeviceIdType.MESH


def seq_starts(slots, lengths):
    bounds = jnp.cumsum(lengths)
    picked = jnp.where(bounds[None, :] <= slots[:, None], lengths[None, :], 0)
    return jnp.sum(picked, axis=1)


def rope_tables(positions, head_dim):
    steps_up = jnp.arange(head_dim // 2, dtype=F32)
    freqs = jnp.exp(-math.log(ROPE_BASE) * (2.0 * steps_up / head_dim))
    angles = positions.astype(F32)[:, None] * freqs[None, :]
    angles = jnp.concatenate([angles, angles], axis=1)
    return (jnp.cos(angles)[:, None, :], jnp.sin(angles)[:, None, :])


def rotate_pairs(values, cosines, sines):
    half_dim = values.shape[-1] // 2
    turned = jnp.concatenate([-values[..., half_dim:], values[..., :half_dim]], axis=-1)
    return values * cosines + turned * sines


def rotate_back(grads_in, cosines, sines):
    half_dim = grads_in.shape[-1] // 2
    moved = grads_in * sines
    return grads_in * cosines + jnp.concatenate(
        [moved[..., half_dim:], -moved[..., :half_dim]], axis=-1
    )


def rms_scale(values):
    return lax.rsqrt(jnp.mean(values * values, axis=-1, keepdims=True) + EPSILON)


def dot_nn(left, right):
    return lax.dot_general(left, right, (((1,), (0,)), ((), ())), preferred_element_type=F32)


def dot_tn(left, right):
    return lax.dot_general(left, right, (((0,), (0,)), ((), ())), preferred_element_type=F32)


def dot_nt(left, right):
    return lax.dot_general(left, right, (((1,), (1,)), ((), ())), preferred_element_type=F32)


def rounded_wide(values):
    return lax.optimization_barrier(values.astype(BF16)).astype(F32)


def masked_scores(query_heads, keys_window, visible, score_scale):
    scores = jnp.einsum("tkgd,skd->kgts", query_heads, keys_window, preferred_element_type=F32)
    return jnp.where(visible, scores * score_scale, -jnp.inf)


def plane_places():
    me = lax.axis_index("col")
    chip, core = me // 2, me % 2
    low, high = chip % 2, chip // 2
    beside = high * 2 + (1 - low)
    above = (1 - high) * 2 + low
    across = (1 - high) * 2 + (1 - low)
    return chip, beside, above, across, core


def greet(peers):
    barrier = pltpu.get_barrier_semaphore()
    for peer in peers:
        pl.semaphore_signal(barrier, inc=1, device_id={"col": peer}, device_id_type=MESH)
    pl.semaphore_wait(barrier, len(peers))


def plane_gather_kernel(count, *refs):
    ins, outs = refs[:count], refs[count : 2 * count]
    send_sem, recv_sem, own_sem = refs[2 * count :]
    chip, beside, above, across, core = plane_places()
    mine = chip * 2 + core
    partner = chip * 2 + 1 - core
    to_x, to_y = beside * 2 + core, above * 2 + core
    greet((partner, to_x, to_y))

    def view(i, slot, part):
        size = ins[i].shape[1]
        half = size // 2
        if part is None:
            return outs[i].at[:, pl.ds(pl.multiple_of(slot * size, size), size), :]
        return outs[i].at[:, pl.ds(pl.multiple_of(slot * size + part * half, half), half), :]

    def copies(k, slot, part, peer, own=False):
        return [
            pltpu.make_async_remote_copy(
                src_ref=ins[i] if own else view(i, slot, part),
                dst_ref=view(i, slot, part),
                send_sem=send_sem.at[i, k],
                recv_sem=recv_sem.at[i, k],
                device_id={"col": peer},
                device_id_type=MESH,
            )
            for i in range(count)
        ]

    def start(cs):
        for c in cs:
            c.start()

    def wait_recv(cs):
        for c in cs:
            c.wait_recv()

    sent = [
        copies(1, mine, None, to_x, True),
        copies(2, mine, None, to_y, True),
        copies(0, mine, None, partner, True),
    ]
    for c in sent:
        start(c)
    own = [
        pltpu.make_async_copy(ins[i], view(i, mine, None), own_sem.at[i]) for i in range(count)
    ]
    start(own)
    other = 1 - core
    wait_recv(copies(1, to_x, None, to_x))
    more = [copies(3, to_x, 0, to_y), copies(5, to_x, None, partner)]
    for c in more:
        start(c)
    sent += more
    wait_recv(copies(2, to_y, None, to_y))
    more = [copies(4, to_y, 1, to_x), copies(6, to_y, None, partner)]
    for c in more:
        start(c)
    sent += more
    far = across * 2 + core
    wait_recv(copies(3, far, 0, to_y))
    more = [copies(7, far, 0, partner)]
    start(more[0])
    sent += more
    wait_recv(copies(4, far, 1, to_x))
    more = [copies(8, far, 1, partner)]
    start(more[0])
    sent += more
    wait_recv(copies(0, partner, None, partner))
    wait_recv(copies(5, beside * 2 + other, None, partner))
    wait_recv(copies(6, above * 2 + other, None, partner))
    wait_recv(copies(7, across * 2 + other, 0, partner))
    wait_recv(copies(8, across * 2 + other, 1, partner))
    for cs in sent:
        for c in cs:
            c.wait_send()
    for c in own:
        c.wait()


def plane_gather(shards, ident):
    count = len(shards)
    parts = lax.axis_size("col")
    outs = [
        jax.ShapeDtypeStruct((s.shape[0], s.shape[1] * parts, s.shape[2]), s.dtype)
        for s in shards
    ]
    return pl.pallas_call(
        functools.partial(plane_gather_kernel, count),
        out_shape=outs,
        in_specs=[pl.BlockSpec(memory_space=pl.ANY)] * count,
        out_specs=[pl.BlockSpec(memory_space=pl.ANY)] * count,
        scratch_shapes=[
            pltpu.SemaphoreType.DMA((count, 9)),
            pltpu.SemaphoreType.DMA((count, 9)),
            pltpu.SemaphoreType.DMA((count,)),
        ],
        compiler_params=pltpu.CompilerParams(collective_id=ident, has_side_effects=True),
        name="plane_gather",
    )(*shards)


def plane_scatter_kernel(count, *refs):
    ins, outs = refs[:count], refs[count : 2 * count]
    scratch = refs[2 * count :]
    near, made, side, land = (scratch[i * count : (i + 1) * count] for i in range(4))
    send_sem, recv_sem = scratch[4 * count :]
    chip, beside, above, across, core = plane_places()
    partner = chip * 2 + 1 - core
    to_x, to_y = beside * 2 + core, above * 2 + core
    greet((partner, to_x, to_y))
    order = (across, beside, above, chip)

    def rows(i, slot):
        size = outs[i].shape[1]
        return pl.ds(pl.multiple_of(slot * size, size), size)

    def half(i, part):
        size = outs[i].shape[1] // 2
        return pl.ds(part * size, size)

    def remote(i, k, src, dst, peer):
        return pltpu.make_async_remote_copy(
            src_ref=src,
            dst_ref=dst,
            send_sem=send_sem.at[i, k],
            recv_sem=recv_sem.at[i, k],
            device_id={"col": peer},
            device_id_type=MESH,
        )

    def near_copy(i, j):
        return remote(
            i, j, ins[i].at[:, rows(i, order[j] * 2 + 1 - core), :], near[i].at[j], partner
        )

    def side_copy(i, part):
        return remote(
            i, 4 + part, made[i].at[0, :, half(i, part), :], side[i].at[part],
            to_x if part == 0 else to_y,
        )

    def land_copy(i, which, part):
        return remote(
            i, 6 + which * 2 + part, made[i].at[1 + which, :, half(i, part), :],
            land[i].at[which, :, half(i, part), :], to_x if which == 0 else to_y,
        )

    step = 16

    def each(i, size, body):
        def tile(t, _):
            body(pl.multiple_of(t * step, step))
            return 0

        lax.fori_loop(0, size // step, tile, 0)

    def combine(i, j):
        size = outs[i].shape[1]
        first = (order[j] * 2 + core) * size

        def body(at):
            for a in range(outs[i].shape[0]):
                left = ins[i][a, pl.ds(pl.multiple_of(first + at, step), step), :].astype(F32)
                right = near[i][j, a, pl.ds(at, step), :].astype(F32)
                made[i][j, a, pl.ds(at, step), :] = (left + right).astype(BF16)

        each(i, size, body)

    def fold(i, which, part):
        size = outs[i].shape[1] // 2

        def body(at):
            at2 = pl.multiple_of(part * size + at, step)
            for a in range(outs[i].shape[0]):
                left = made[i][1 + which, a, pl.ds(at2, step), :].astype(F32)
                right = side[i][1 - which, a, pl.ds(at, step), :].astype(F32)
                made[i][1 + which, a, pl.ds(at2, step), :] = (left + right).astype(BF16)

        each(i, size, body)

    every = range(count)
    for j in range(4):
        for i in every:
            near_copy(i, j).start()
    for i in every:
        near_copy(i, 0).wait_recv()
        combine(i, 0)
        side_copy(i, 0).start()
        side_copy(i, 1).start()
    for i in every:
        near_copy(i, 1).wait_recv()
        combine(i, 1)
        land_copy(i, 0, 0).start()
    for i in every:
        near_copy(i, 2).wait_recv()
        combine(i, 2)
        land_copy(i, 1, 1).start()
    for i in every:
        side_copy(i, 0).wait_recv()
        fold(i, 1, 0)
        land_copy(i, 1, 0).start()
        side_copy(i, 1).wait_recv()
        fold(i, 0, 1)
        land_copy(i, 0, 1).start()
    for i in every:
        near_copy(i, 3).wait_recv()
    for i in every:
        for which in range(2):
            for part in range(2):
                land_copy(i, which, part).wait_recv()
        size = outs[i].shape[1]
        first = (chip * 2 + core) * size

        def body(at, i=i, first=first):
            for a in range(outs[i].shape[0]):
                spot = pl.ds(at, step)
                total = ins[i][a, pl.ds(pl.multiple_of(first + at, step), step), :].astype(F32)
                total += near[i][3, a, spot, :].astype(F32)
                total += land[i][0, a, spot, :].astype(F32)
                total += land[i][1, a, spot, :].astype(F32)
                outs[i][a, spot, :] = total.astype(outs[i].dtype)

        each(i, size, body)
    for i in every:
        for j in range(4):
            near_copy(i, j).wait_send()
        for part in range(2):
            side_copy(i, part).wait_send()
            for which in range(2):
                land_copy(i, which, part).wait_send()


def plane_scatter(fulls, ident, out_dtype=F32):
    count = len(fulls)
    parts = lax.axis_size("col")
    shapes = [(f.shape[0], f.shape[1] // parts, f.shape[2]) for f in fulls]
    scratch = []
    scratch += [pltpu.VMEM((4,) + s, BF16) for s in shapes]
    scratch += [pltpu.VMEM((3,) + s, BF16) for s in shapes]
    scratch += [pltpu.VMEM((2, s[0], s[1] // 2, s[2]), BF16) for s in shapes]
    scratch += [pltpu.VMEM((2,) + s, BF16) for s in shapes]
    return pl.pallas_call(
        functools.partial(plane_scatter_kernel, count),
        out_shape=[jax.ShapeDtypeStruct(s, out_dtype) for s in shapes],
        in_specs=[pl.BlockSpec(memory_space=pltpu.VMEM)] * count,
        out_specs=[pl.BlockSpec(memory_space=pltpu.VMEM)] * count,
        scratch_shapes=scratch
        + [pltpu.SemaphoreType.DMA((count, 10)), pltpu.SemaphoreType.DMA((count, 10))],
        compiler_params=pltpu.CompilerParams(collective_id=ident, has_side_effects=True),
        name="plane_scatter",
    )(*fulls)


def spans(total, most):
    return [(at, min(most, total - at)) for at in range(0, total, most)]


def remote(src, dst, send_sem, recv_sem, peer):
    return pltpu.make_async_remote_copy(
        src_ref=src,
        dst_ref=dst,
        send_sem=send_sem,
        recv_sem=recv_sem,
        device_id={"col": peer},
        device_id_type=MESH,
    )


def block_gather(source, land, send_sem, recv_sem):
    chip, beside, above, across, core = plane_places()
    half = source.shape[0] // 2
    mine, partner, other = chip * 2 + core, chip * 2 + 1 - core, 1 - core
    to_x, to_y, far = beside * 2 + core, above * 2 + core, across * 2 + core

    def copy(k, slot, part, peer, own=False):
        spot = land.at[slot] if part is None else land.at[slot, pl.ds(part * half, half), :]
        return remote(source if own else spot, spot, send_sem.at[k], recv_sem.at[k], peer)

    def first():
        greet((partner, to_x, to_y))
        copy(1, mine, None, to_x, True).start()
        copy(2, mine, None, to_y, True).start()
        copy(0, mine, None, partner, True).start()

    def second():
        copy(1, to_x, None, to_x).wait_recv()
        copy(3, to_x, 0, to_y).start()
        copy(5, to_x, None, partner).start()
        copy(2, to_y, None, to_y).wait_recv()
        copy(4, to_y, 1, to_x).start()
        copy(6, to_y, None, partner).start()

    def third():
        copy(3, far, 0, to_y).wait_recv()
        copy(7, far, 0, partner).start()
        copy(4, far, 1, to_x).wait_recv()
        copy(8, far, 1, partner).start()

    def landed(k):
        slot = (partner, beside * 2 + other, above * 2 + other)[k]
        copy((0, 5, 6)[k], slot, None, partner).wait_recv()

    def landed_far():
        copy(7, across * 2 + other, 0, partner).wait_recv()
        copy(8, across * 2 + other, 1, partner).wait_recv()

    def sent():
        for k, slot, part in (
            (0, mine, None), (1, mine, None), (2, mine, None), (3, to_x, 0), (4, to_y, 1),
            (5, to_x, None), (6, to_y, None), (7, far, 0), (8, far, 1),
        ):
            copy(k, slot, part, partner).wait_send()

    return first, second, third, landed, landed_far, sent


def spread(index, rows):
    return pl.ds(pl.multiple_of(index * rows, rows), rows)


def ffn_gate_kernel(
    normed, gate_t, normed_rows, gate_act, land, tiles, send_sem, recv_sem, keep_sem, tile_sem
):
    chip, _, _, _, core = plane_places()
    low, high = chip % 2, chip // 2
    rows = normed.shape[0]
    first, second, third, landed, landed_far, sent = block_gather(
        normed, land, send_sem, recv_sem
    )

    def keep(slot):
        return pltpu.make_async_copy(
            land.at[slot], normed_rows.at[spread(slot, rows), :], keep_sem.at[slot]
        )

    def put(slot, parity):
        return pltpu.make_async_copy(
            tiles.at[parity], gate_act.at[spread(slot, rows), :], tile_sem.at[parity]
        )

    first()
    land[chip * 2 + core] = normed[...]

    def step(s, _):
        flip = s // 2
        at_chip = (high + flip // 2) % 2 * 2 + (low + flip) % 2
        slot = at_chip * 2 + (core + s) % 2
        parity = s % 2

        @pl.when(s == 1)
        def _():
            landed(0)

        @pl.when(s == 2)
        def _():
            second()

        @pl.when(s == 3)
        def _():
            landed(1)

        @pl.when(s == 5)
        def _():
            landed(2)

        @pl.when(s == 6)
        def _():
            third()

        @pl.when(s == 7)
        def _():
            landed_far()

        keep(slot).start()

        @pl.when(s >= 2)
        def _():
            put(slot, parity).wait()

        for at, wide in spans(gate_t.shape[0], 512):
            tiles[parity, :, at : at + wide] = dot_nt(land[slot], gate_t[at : at + wide, :])
        put(slot, parity).start()
        return 0

    lax.fori_loop(0, 8, step, 0)
    for parity in range(2):
        put(0, parity).wait()

    def drain(slot, _):
        keep(slot).wait()
        return 0

    lax.fori_loop(0, 8, drain, 0)
    sent()


def ffn_gate(normed, gate_t, ident):
    rows, depth = normed.shape
    wide = gate_t.shape[0]
    dma = pltpu.SemaphoreType.DMA
    return pl.pallas_call(
        ffn_gate_kernel,
        out_shape=[
            jax.ShapeDtypeStruct((rows * 8, depth), BF16),
            jax.ShapeDtypeStruct((rows * 8, wide), F32),
        ],
        in_specs=[pl.BlockSpec(memory_space=pltpu.VMEM)] * 2,
        out_specs=[pl.BlockSpec(memory_space=pl.ANY)] * 2,
        scratch_shapes=[
            pltpu.VMEM((8, rows, depth), BF16),
            pltpu.VMEM((2, rows, wide), F32),
            dma((9,)),
            dma((9,)),
            dma((8,)),
            dma((2,)),
        ],
        compiler_params=pltpu.CompilerParams(collective_id=ident, has_side_effects=True),
        name="ffn_gate",
    )(normed, gate_t)


def ffn_up_kernel(
    cotangent,
    up_t,
    normed_rows,
    gate_act,
    out_rows,
    hidden,
    silu,
    slope,
    land,
    rows_in,
    gate_in,
    tiles,
    send_sem,
    recv_sem,
    keep_sem,
    in_sem,
    tile_sem,
):
    chip, _, _, _, core = plane_places()
    rows = cotangent.shape[0]
    first, second, third, landed, landed_far, sent = block_gather(
        cotangent, land, send_sem, recv_sem
    )

    def fetch(kind, s, parity):
        source = (normed_rows, gate_act)[kind]
        target = (rows_in, gate_in)[kind]
        return pltpu.make_async_copy(
            source.at[spread(s, rows), :], target.at[parity], in_sem.at[kind, parity]
        )

    def keep(slot):
        return pltpu.make_async_copy(
            land.at[slot], out_rows.at[spread(slot, rows), :], keep_sem.at[slot]
        )

    def put(kind, s, parity):
        target = (hidden, silu, slope)[kind]
        return pltpu.make_async_copy(
            tiles.at[kind, parity], target.at[spread(s, rows), :], tile_sem.at[kind, parity]
        )

    first()
    fetch(0, 0, 0).start()
    fetch(1, 0, 0).start()
    land[chip * 2 + core] = cotangent[...]

    def step(s, _):
        parity = s % 2

        @pl.when(s < 7)
        def _():
            fetch(0, s + 1, 1 - parity).start()
            fetch(1, s + 1, 1 - parity).start()

        @pl.when(s == 7)
        def _():
            second()

        @pl.when(s >= 2)
        def _():
            for kind in range(3):
                put(kind, s, parity).wait()

        fetch(0, s, parity).wait()
        fetch(1, s, parity).wait()
        for at, wide in spans(up_t.shape[0], 512):
            cut = slice(at, at + wide)
            up = dot_nt(rows_in[parity], up_t[cut, :])
            gate = gate_in[parity, :, cut]
            sigma = 1.0 / (1.0 + jnp.exp(-gate))
            smooth = gate * sigma
            tiles[0, parity, :, cut] = (smooth * up).astype(BF16)
            tiles[1, parity, :, cut] = smooth.astype(BF16)
            tiles[2, parity, :, cut] = (up * sigma * (1.0 + gate * (1.0 - sigma))).astype(BF16)
        for kind in range(3):
            put(kind, s, parity).start()
        return 0

    lax.fori_loop(0, 8, step, 0)
    landed(0)
    third()
    landed(1)
    landed(2)
    landed_far()

    def store(slot, _):
        keep(slot).start()
        return 0

    def drain(slot, _):
        keep(slot).wait()
        return 0

    lax.fori_loop(0, 8, store, 0)
    for parity in range(2):
        for kind in range(3):
            put(kind, 0, parity).wait()
    lax.fori_loop(0, 8, drain, 0)
    sent()


def ffn_up(cotangent, up_t, normed_rows, gate_act, ident):
    rows, depth = cotangent.shape
    wide = up_t.shape[0]
    dma = pltpu.SemaphoreType.DMA
    vmem = pl.BlockSpec(memory_space=pltpu.VMEM)
    anywhere = pl.BlockSpec(memory_space=pl.ANY)
    return pl.pallas_call(
        ffn_up_kernel,
        out_shape=[jax.ShapeDtypeStruct((rows * 8, depth), BF16)]
        + [jax.ShapeDtypeStruct((rows * 8, wide), BF16)] * 3,
        in_specs=[vmem, vmem, anywhere, anywhere],
        out_specs=[anywhere] * 4,
        scratch_shapes=[
            pltpu.VMEM((8, rows, depth), BF16),
            pltpu.VMEM((2, rows, depth), BF16),
            pltpu.VMEM((2, rows, wide), F32),
            pltpu.VMEM((3, 2, rows, wide), BF16),
            dma((9,)),
            dma((9,)),
            dma((8,)),
            dma((2, 2)),
            dma((3, 2)),
        ],
        compiler_params=pltpu.CompilerParams(collective_id=ident, has_side_effects=True),
        name="ffn_up",
    )(cotangent, up_t, normed_rows, gate_act)


def ffn_backward_kernel(
    out_rows,
    hidden,
    silu,
    slope,
    gate_t,
    up_t,
    down,
    gate_grad,
    up_grad,
    branch_own,
    normed_own,
    out_in,
    tiles_in,
    tiles_out,
    give,
    near,
    made,
    side,
    land,
    near_send,
    near_recv,
    side_send,
    side_recv,
    land_send,
    land_recv,
    in_sem,
    tile_sem,
):
    chip, beside, above, across, core = plane_places()
    low, high = chip % 2, chip // 2
    own_rows = branch_own.shape[0]
    half = own_rows // 2
    depth = branch_own.shape[1]
    partner = chip * 2 + 1 - core
    to_x, to_y = beside * 2 + core, above * 2 + core
    greet((partner, to_x, to_y))
    finals = (branch_own, normed_own)

    def spread(index):
        return pl.ds(pl.multiple_of(index * own_rows, own_rows), own_rows)

    def slot_of(s):
        flip = 3 - s // 2
        at_chip = (high + flip // 2) % 2 * 2 + (low + flip) % 2
        return at_chip * 2 + (core + 1 + s) % 2

    def near_copy(a, j):
        return remote(
            give.at[a, j], near.at[a, j], near_send.at[a, j], near_recv.at[a, j], partner
        )

    def side_copy(a, part):
        return remote(
            made.at[a, 0, pl.ds(part * half, half), :], side.at[a, part],
            side_send.at[a, part], side_recv.at[a, part], to_x if part == 0 else to_y,
        )

    def land_copy(a, which, part):
        k = which * 2 + part
        return remote(
            made.at[a, 1 + which, pl.ds(part * half, half), :],
            land.at[a, which, pl.ds(part * half, half), :],
            land_send.at[a, k], land_recv.at[a, k], to_x if which == 0 else to_y,
        )

    def fold(a, which, part):
        def tile(t, _):
            at = pl.multiple_of(t * 16, 16)
            spot = pl.ds(pl.multiple_of(part * half + at, 16), 16)
            left = made[a, 1 + which, spot, :].astype(F32)
            right = side[a, 1 - which, pl.ds(at, 16), :].astype(F32)
            made[a, 1 + which, spot, :] = (left + right).astype(BF16)
            return 0

        lax.fori_loop(0, half // 16, tile, 0)

    def fetch(kind, s, parity):
        if kind == 0:
            return pltpu.make_async_copy(
                out_rows.at[spread(slot_of(s)), :], out_in.at[parity], in_sem.at[0, parity]
            )
        source = (hidden, silu, slope)[kind - 1]
        return pltpu.make_async_copy(
            source.at[spread(slot_of(s)), :], tiles_in.at[kind - 1, parity], in_sem.at[kind, parity]
        )

    def put(kind, s, parity):
        target = (gate_grad, up_grad)[kind]
        return pltpu.make_async_copy(
            tiles_out.at[kind, parity], target.at[spread(slot_of(s)), :],
            tile_sem.at[kind, parity],
        )

    def sides(a):
        side_copy(a, 0).wait_recv()
        fold(a, 1, 0)
        land_copy(a, 1, 0).start()
        side_copy(a, 1).wait_recv()
        fold(a, 0, 1)
        land_copy(a, 0, 1).start()

    def deliver(a, s, partial):
        j = s // 2

        @pl.when(s % 2 == 0)
        def _():
            give[a, j] = partial().astype(BF16)
            near_copy(a, j).start()

        @pl.when(s % 2 == 1)
        def _():
            total = partial()
            near_copy(a, j).wait_recv()
            total = total + near[a, j].astype(F32)

            @pl.when(j < 3)
            def _():
                made[a, (3 - j) % 3] = total.astype(BF16)

            @pl.when(j == 0)
            def _():
                side_copy(a, 0).start()
                side_copy(a, 1).start()

            @pl.when(j == 1)
            def _():
                land_copy(a, 1, 1).start()

            @pl.when(j == 2)
            def _():
                land_copy(a, 0, 0).start()
                sides(a)

            @pl.when(j == 3)
            def _():
                finals[a][...] = total

    fetch(1, 0, 0).start()

    def branch_step(s, _):
        parity = s % 2

        @pl.when(s < 7)
        def _():
            fetch(1, s + 1, (s + 1) % 2).start()

        @pl.when(s == 6)
        def _():
            for kind in (0, 2, 3):
                fetch(kind, 0, 0).start()

        fetch(1, s, parity).wait()
        deliver(0, s, lambda: dot_nn(tiles_in[0, parity], down[...]))
        return 0

    lax.fori_loop(0, 8, branch_step, 0)

    def normed_step(s, _):
        parity = s % 2

        @pl.when(s < 7)
        def _():
            for kind in (0, 2, 3):
                fetch(kind, s + 1, (s + 1) % 2).start()

        for kind in (0, 2, 3):
            fetch(kind, s, parity).wait()

        @pl.when(s >= 2)
        def _():
            for kind in range(2):
                put(kind, s, parity).wait()

        for at, wide in spans(down.shape[0], 512):
            cut = slice(at, at + wide)
            hidden_grad = dot_nt(out_in[parity], down[cut, :])
            tiles_out[0, parity, :, cut] = (
                hidden_grad * tiles_in[2, parity, :, cut].astype(F32)
            ).astype(BF16)
            tiles_out[1, parity, :, cut] = (
                hidden_grad * tiles_in[1, parity, :, cut].astype(F32)
            ).astype(BF16)
        for kind in range(2):
            put(kind, s, parity).start()
        deliver(
            1, s,
            lambda: dot_nn(tiles_out[0, parity], gate_t[...])
            + dot_nn(tiles_out[1, parity], up_t[...]),
        )
        return 0

    lax.fori_loop(0, 8, normed_step, 0)
    for a in range(2):
        for which in range(2):
            for part in range(2):
                land_copy(a, which, part).wait_recv()

        def tile(t, _, a=a):
            spot = pl.ds(pl.multiple_of(t * 16, 16), 16)
            finals[a][spot, :] = (
                finals[a][spot, :]
                + land[a, 0, spot, :].astype(F32)
                + land[a, 1, spot, :].astype(F32)
            )
            return 0

        lax.fori_loop(0, own_rows // 16, tile, 0)
    for a in range(2):
        for j in range(4):
            near_copy(a, j).wait_send()
        for part in range(2):
            side_copy(a, part).wait_send()
            for which in range(2):
                land_copy(a, which, part).wait_send()
    for kind in range(2):
        for parity in range(2):
            put(kind, parity, parity).wait()


def ffn_backward(out_rows, hidden, silu, slope, gate_t, up_t, down, ident):
    total, depth = out_rows.shape
    wide = down.shape[0]
    rows = total // 8
    vmem = pl.BlockSpec(memory_space=pltpu.VMEM)
    anywhere = pl.BlockSpec(memory_space=pl.ANY)
    dma = pltpu.SemaphoreType.DMA
    return pl.pallas_call(
        ffn_backward_kernel,
        out_shape=[jax.ShapeDtypeStruct((total, wide), BF16)] * 2
        + [jax.ShapeDtypeStruct((rows, depth), F32)] * 2,
        in_specs=[anywhere] * 4 + [vmem] * 3,
        out_specs=[anywhere] * 2 + [vmem] * 2,
        scratch_shapes=[
            pltpu.VMEM((2, rows, depth), BF16),
            pltpu.VMEM((3, 2, rows, wide), BF16),
            pltpu.VMEM((2, 2, rows, wide), BF16),
            pltpu.VMEM((2, 4, rows, depth), BF16),
            pltpu.VMEM((2, 4, rows, depth), BF16),
            pltpu.VMEM((2, 3, rows, depth), BF16),
            pltpu.VMEM((2, 2, rows // 2, depth), BF16),
            pltpu.VMEM((2, 2, rows, depth), BF16),
            dma((2, 4)),
            dma((2, 4)),
            dma((2, 2)),
            dma((2, 2)),
            dma((2, 4)),
            dma((2, 4)),
            dma((4, 2)),
            dma((2, 2)),
        ],
        compiler_params=pltpu.CompilerParams(collective_id=ident, has_side_effects=True),
        name="ffn_backward",
    )(out_rows, hidden, silu, slope, gate_t, up_t, down)


def weight_grad_kernel(left, right, out):
    for at, wide in spans(right.shape[1], 512):
        out[:, at : at + wide] = lax.dot_general(
            left[...],
            right[:, at : at + wide],
            (((0,), (0,)), ((), ())),
            preferred_element_type=F32,
        ).astype(out.dtype)


def weight_grad(left, right):
    rows, depth = left.shape
    wide = right.shape[1]
    tile = 256
    return pl.pallas_call(
        weight_grad_kernel,
        grid=(depth // tile,),
        out_shape=jax.ShapeDtypeStruct((depth, wide), BF16),
        in_specs=[
            pl.BlockSpec((rows, tile), lambda i: (0, i)),
            pl.BlockSpec((rows, wide), lambda i: (0, 0)),
        ],
        out_specs=pl.BlockSpec((tile, wide), lambda i: (i, 0)),
        cost_estimate=pl.CostEstimate(
            flops=2 * rows * depth * wide,
            bytes_accessed=2 * (rows * depth + rows * wide + depth * wide),
            transcendentals=0,
        ),
        name="weight_grad",
    )(left, right)


def gather_row(block):
    return lax.all_gather(block, "row", axis=block.ndim - 1, tiled=True)


def scatter_row(full):
    return lax.psum_scatter(
        full.astype(BF16), "row", scatter_dimension=0, tiled=True
    )


def gather_col(blocks, ident):
    if lax.axis_size("col") == 8:
        return plane_gather(blocks, ident)
    return [lax.all_gather(block, "col", axis=1, tiled=True) for block in blocks]


def scatter_col(fulls, ident):
    fulls = [full.astype(BF16) for full in fulls]
    if lax.axis_size("col") == 8:
        return plane_scatter(fulls, ident)
    return [
        lax.psum_scatter(full, "col", scatter_dimension=1, tiled=True).astype(F32)
        for full in fulls
    ]


def line_remote(src, dst, send_sem, recv_sem, peer):
    return pltpu.make_async_remote_copy(
        src_ref=src,
        dst_ref=dst,
        send_sem=send_sem,
        recv_sem=recv_sem,
        device_id={"row": peer},
        device_id_type=MESH,
    )


def greet_grid(peers, place, places):
    barrier = pltpu.get_barrier_semaphore()
    for peer in peers:
        pl.semaphore_signal(barrier, inc=1, device_id={"col": peer}, device_id_type=MESH)

    @pl.when(place > 0)
    def _():
        pl.semaphore_signal(barrier, inc=1, device_id={"row": place - 1}, device_id_type=MESH)

    @pl.when(place < places - 1)
    def _():
        pl.semaphore_signal(barrier, inc=1, device_id={"row": place + 1}, device_id_type=MESH)

    edge = (place == 0) | (place == places - 1)

    @pl.when(edge)
    def _():
        pl.semaphore_wait(barrier, len(peers) + 1)

    @pl.when(jnp.logical_not(edge))
    def _():
        pl.semaphore_wait(barrier, len(peers) + 2)


def grid_gather_kernel(count, extra, places, *refs):
    both_count = count + extra
    ins, outs = refs[:both_count], refs[both_count : 2 * both_count]
    send_sem, recv_sem, line_send, line_recv, own_sem = refs[2 * both_count :]
    place = lax.axis_index("row")
    chip, beside, above, across, core = plane_places()
    mine, partner, other = chip * 2 + core, chip * 2 + 1 - core, 1 - core
    to_x, to_y, far = beside * 2 + core, above * 2 + core, across * 2 + core
    every = range(count)
    others = range(count, both_count)
    greet_grid((partner, to_x, to_y), place, places)

    def view(i, slot, line, part):
        size, wide = ins[i].shape
        spot = pl.ds(pl.multiple_of(line * wide, wide), wide)
        if i >= count:
            return outs[i].at[:, spot]
        if part is None:
            return outs[i].at[pl.ds(pl.multiple_of(slot * size, size), size), spot]
        half = size // 2
        return outs[i].at[pl.ds(pl.multiple_of(slot * size + part * half, half), half), spot]

    def copies(k, slot, line, part, peer, own=False):
        return [
            remote(
                ins[i] if own else view(i, slot, line, part),
                view(i, slot, line, part),
                send_sem.at[i, line, k],
                recv_sem.at[i, line, k],
                peer,
            )
            for i in every
        ]

    def line_copies(line, sem_at, peer, own=False, which=every):
        return [
            line_remote(
                ins[i] if own else view(i, mine, line, None),
                view(i, mine, line, None),
                line_send.at[i, sem_at],
                line_recv.at[i, line],
                peer,
            )
            for i in which
        ]

    def start(cs):
        for c in cs:
            c.start()

    def wait_recv(cs):
        for c in cs:
            c.wait_recv()

    def first(line, own=False):
        start(copies(1, mine, line, None, to_x, own))
        start(copies(2, mine, line, None, to_y, own))
        start(copies(0, mine, line, None, partner, own))

    def second(line):
        wait_recv(copies(1, to_x, line, None, to_x))
        start(copies(3, to_x, line, 0, to_y))
        start(copies(5, to_x, line, None, partner))
        wait_recv(copies(2, to_y, line, None, to_y))
        start(copies(4, to_y, line, 1, to_x))
        start(copies(6, to_y, line, None, partner))

    def third(line):
        wait_recv(copies(3, far, line, 0, to_y))
        start(copies(7, far, line, 0, partner))
        wait_recv(copies(4, far, line, 1, to_x))
        start(copies(8, far, line, 1, partner))

    def last(line):
        wait_recv(copies(0, partner, line, None, partner))
        wait_recv(copies(5, beside * 2 + other, line, None, partner))
        wait_recv(copies(6, above * 2 + other, line, None, partner))
        wait_recv(copies(7, across * 2 + other, line, 0, partner))
        wait_recv(copies(8, across * 2 + other, line, 1, partner))
        for k, slot, part in (
            (0, mine, None), (1, mine, None), (2, mine, None), (3, to_x, 0), (4, to_y, 1),
            (5, to_x, None), (6, to_y, None), (7, far, 0), (8, far, 1),
        ):
            for c in copies(k, slot, line, part, partner):
                c.wait_send()

    def both(distance, body):
        @pl.when((distance >= 1) & (place - distance >= 0))
        def _():
            body(place - distance)

        @pl.when((distance >= 1) & (place + distance < places))
        def _():
            body(place + distance)

        @pl.when(distance == 0)
        def _():
            body(place)

    @pl.when(place < places - 1)
    def _():
        start(line_copies(place, place, place + 1, True))
        start(line_copies(place, place, place + 1, True, others))

    @pl.when(place > 0)
    def _():
        start(line_copies(place, places, place - 1, True))
        start(line_copies(place, places, place - 1, True, others))

    first(place, True)
    own = [
        pltpu.make_async_copy(ins[i], view(i, mine, place, None), own_sem.at[i])
        for i in range(both_count)
    ]
    start(own)

    def pass_on(line):
        @pl.when(line != place)
        def _():
            wait_recv(line_copies(line, line, place, False, others))

        @pl.when((line < place) & (place < places - 1))
        def _():
            start(line_copies(line, line, place + 1, False, others))

        @pl.when((line > place) & (place > 0))
        def _():
            start(line_copies(line, line, place - 1, False, others))

    def step(t, _):
        @pl.when((t >= 1) & (place - t >= 0))
        def _():
            line = place - t
            wait_recv(line_copies(line, line, place))

            @pl.when(place < places - 1)
            def _():
                start(line_copies(line, line, place + 1))

            first(line)

        @pl.when((t >= 1) & (place + t < places))
        def _():
            line = place + t
            wait_recv(line_copies(line, line, place))

            @pl.when(place > 0)
            def _():
                start(line_copies(line, line, place - 1))

            first(line)

        both(t - 1, second)
        if extra:
            both(t - 1, pass_on)
        both(t - 2, third)
        return 0

    lax.fori_loop(0, places + 2, step, 0)

    everything = range(both_count)

    def finish(line, _):
        last(line)
        relays = ((line < place) & (place < places - 1)) | ((line > place) & (place > 0))

        @pl.when(relays)
        def _():
            for c in line_copies(line, line, place, False, everything):
                c.wait_send()

        return 0

    lax.fori_loop(0, places, finish, 0)

    @pl.when(place < places - 1)
    def _():
        for c in line_copies(place, place, place, False, everything):
            c.wait_send()

    @pl.when(place > 0)
    def _():
        for c in line_copies(place, places, place, False, everything):
            c.wait_send()

    for c in own:
        c.wait()


def grid_gather(shards, lines, ident):
    count, extra = len(shards), len(lines)
    places, parts = lax.axis_size("row"), lax.axis_size("col")
    dma = pltpu.SemaphoreType.DMA
    anywhere = pl.BlockSpec(memory_space=pl.ANY)
    return pl.pallas_call(
        functools.partial(grid_gather_kernel, count, extra, places),
        out_shape=[
            jax.ShapeDtypeStruct((s.shape[0] * parts, s.shape[1] * places), s.dtype)
            for s in shards
        ]
        + [jax.ShapeDtypeStruct((s.shape[0], s.shape[1] * places), s.dtype) for s in lines],
        in_specs=[anywhere] * (count + extra),
        out_specs=[anywhere] * (count + extra),
        scratch_shapes=[
            dma((count, places, 9)),
            dma((count, places, 9)),
            dma((count + extra, places + 1)),
            dma((count + extra, places)),
            dma((count + extra,)),
        ],
        compiler_params=pltpu.CompilerParams(collective_id=ident, has_side_effects=True),
        name="grid_gather",
    )(*shards, *lines)


def grid_scatter_kernel(count, places, *refs):
    ins, outs = refs[:count], refs[count : 2 * count]
    scratch = refs[2 * count :]
    near, made, side, land, line_in, line_out = (
        scratch[i * count : (i + 1) * count] for i in range(6)
    )
    (
        near_send, near_recv, side_send, side_recv, land_send, land_recv, line_send, line_recv,
    ) = scratch[6 * count :]
    place = lax.axis_index("row")
    chip, beside, above, across, core = plane_places()
    partner = chip * 2 + 1 - core
    to_x, to_y = beside * 2 + core, above * 2 + core
    order = (across, beside, above, chip)
    every = range(count)
    greet_grid((partner, to_x, to_y), place, places)

    def source(i, slot, line, at, size):
        rows, wide = outs[i].shape
        return (
            pl.ds(pl.multiple_of(slot * rows + at, size), size),
            pl.ds(pl.multiple_of(line * wide, wide), wide),
        )

    def near_copy(i, line, j):
        rows = outs[i].shape[0]
        return remote(
            ins[i].at[source(i, order[j] * 2 + 1 - core, line, 0, rows)],
            near[i].at[line, j],
            near_send.at[i, line, j], near_recv.at[i, line, j], partner,
        )

    def halves(i, part):
        half = outs[i].shape[0] // 2
        return pl.ds(part * half, half)

    def side_copy(i, line, part):
        return remote(
            made[i].at[line, 0, halves(i, part), :], side[i].at[line, part],
            side_send.at[i, line, part], side_recv.at[i, line, part],
            to_x if part == 0 else to_y,
        )

    def land_copy(i, line, which, part):
        k = which * 2 + part
        return remote(
            made[i].at[line, 1 + which, halves(i, part), :],
            land[i].at[line, which, halves(i, part), :],
            land_send.at[i, line, k], land_recv.at[i, line, k],
            to_x if which == 0 else to_y,
        )

    def up_copy(i, line):
        return line_remote(
            line_out[i].at[line], line_in[i].at[line],
            line_send.at[i, line], line_recv.at[i, line], place + 1,
        )

    def down_copy(i, line):
        target = jnp.where(line == place - 1, places, line)
        return line_remote(
            line_out[i].at[line], line_in[i].at[target],
            line_send.at[i, line], line_recv.at[i, target], place - 1,
        )

    def each(size, body):
        def tile(t, _):
            body(pl.multiple_of(t * 16, 16))
            return 0

        lax.fori_loop(0, size // 16, tile, 0)

    def combine(i, line, j):
        def body(at):
            spot = pl.ds(at, 16)
            left = ins[i][source(i, order[j] * 2 + core, line, at, 16)].astype(F32)
            made[i][line, j, spot, :] = (left + near[i][line, j, spot, :].astype(F32)).astype(
                BF16
            )

        each(outs[i].shape[0], body)

    def fold(i, line, which, part):
        half = outs[i].shape[0] // 2

        def body(at):
            spot = pl.ds(pl.multiple_of(part * half + at, 16), 16)
            left = made[i][line, 1 + which, spot, :].astype(F32)
            right = side[i][line, 1 - which, pl.ds(at, 16), :].astype(F32)
            made[i][line, 1 + which, spot, :] = (left + right).astype(BF16)

        each(half, body)

    def sequence(q):
        up = places - 1 - place
        return jnp.where(q < up, places - 1 - q, q - up)

    def first(line):
        for i in every:
            near_copy(i, line, 0).wait_recv()
            combine(i, line, 0)
            side_copy(i, line, 0).start()
            side_copy(i, line, 1).start()
        for i in every:
            near_copy(i, line, 1).wait_recv()
            combine(i, line, 1)
            land_copy(i, line, 0, 0).start()
            near_copy(i, line, 2).wait_recv()
            combine(i, line, 2)
            land_copy(i, line, 1, 1).start()

    def second(line):
        for i in every:
            side_copy(i, line, 0).wait_recv()
            fold(i, line, 1, 0)
            land_copy(i, line, 1, 0).start()
            side_copy(i, line, 1).wait_recv()
            fold(i, line, 0, 1)
            land_copy(i, line, 0, 1).start()

    def arrived(i, slot):
        line_remote(
            line_out[i].at[0], line_in[i].at[slot],
            line_send.at[i, 0], line_recv.at[i, slot], place,
        ).wait_recv()

    def third(line):
        for i in every:
            near_copy(i, line, 3).wait_recv()
            for which in range(2):
                for part in range(2):
                    land_copy(i, line, which, part).wait_recv()

        @pl.when((line > place) & (place > 0))
        def _():
            for i in every:
                arrived(i, line)

        @pl.when((line < place) & (place < places - 1))
        def _():
            for i in every:
                arrived(i, line)

        @pl.when((line == place) & (place > 0))
        def _():
            for i in every:
                arrived(i, place)

        @pl.when((line == place) & (place < places - 1))
        def _():
            for i in every:
                arrived(i, places)

        def total(i, at):
            spot = pl.ds(at, 16)
            value = ins[i][source(i, chip * 2 + core, line, at, 16)].astype(F32)
            value += near[i][line, 3, spot, :].astype(F32)
            value += land[i][line, 0, spot, :].astype(F32)
            value += land[i][line, 1, spot, :].astype(F32)
            return value

        for i in every:
            relays = ((line > place) & (place > 0)) | ((line < place) & (place < places - 1))

            @pl.when((line != place) & relays)
            def _(i=i):
                def body(at):
                    spot = pl.ds(at, 16)
                    line_out[i][line, spot, :] = (
                        total(i, at) + line_in[i][line, spot, :].astype(F32)
                    ).astype(BF16)

                each(outs[i].shape[0], body)

            @pl.when((line != place) & jnp.logical_not(relays))
            def _(i=i):
                def body(at):
                    line_out[i][line, pl.ds(at, 16), :] = total(i, at).astype(BF16)

                each(outs[i].shape[0], body)

            @pl.when(line > place)
            def _(i=i):
                up_copy(i, line).start()

            @pl.when(line < place)
            def _(i=i):
                down_copy(i, line).start()

            @pl.when(line == place)
            def _(i=i):
                def body(at):
                    outs[i][pl.ds(at, 16), :] = total(i, at)

                each(outs[i].shape[0], body)

                @pl.when(place > 0)
                def _():
                    def more(at):
                        spot = pl.ds(at, 16)
                        outs[i][spot, :] += line_in[i][place, spot, :].astype(F32)

                    each(outs[i].shape[0], more)

                @pl.when(place < places - 1)
                def _():
                    def more(at):
                        spot = pl.ds(at, 16)
                        outs[i][spot, :] += line_in[i][places, spot, :].astype(F32)

                    each(outs[i].shape[0], more)

    def begin(q, _):
        line = sequence(q)
        for j in range(4):
            for i in every:
                near_copy(i, line, j).start()
        return 0

    lax.fori_loop(0, places, begin, 0)

    def step(t, _):
        @pl.when(t < places)
        def _():
            first(sequence(t))

        @pl.when((t >= 1) & (t - 1 < places))
        def _():
            second(sequence(t - 1))

        @pl.when(t >= 2)
        def _():
            third(sequence(t - 2))

        return 0

    lax.fori_loop(0, places + 2, step, 0)

    def finish(line, _):
        for i in every:
            for j in range(4):
                near_copy(i, line, j).wait_send()
            for part in range(2):
                side_copy(i, line, part).wait_send()
                for which in range(2):
                    land_copy(i, line, which, part).wait_send()

            @pl.when(line != place)
            def _(i=i):
                up_copy(i, line).wait_send()

        return 0

    lax.fori_loop(0, places, finish, 0)


def grid_scatter(fulls, ident):
    count = len(fulls)
    places, parts = lax.axis_size("row"), lax.axis_size("col")
    shapes = [(f.shape[0] // parts, f.shape[1] // places) for f in fulls]
    dma = pltpu.SemaphoreType.DMA
    vmem = pl.BlockSpec(memory_space=pltpu.VMEM)
    scratch = []
    scratch += [pltpu.VMEM((places, 4) + s, BF16) for s in shapes]
    scratch += [pltpu.VMEM((places, 3) + s, BF16) for s in shapes]
    scratch += [pltpu.VMEM((places, 2, s[0] // 2, s[1]), BF16) for s in shapes]
    scratch += [pltpu.VMEM((places, 2) + s, BF16) for s in shapes]
    scratch += [pltpu.VMEM((places + 1,) + s, BF16) for s in shapes]
    scratch += [pltpu.VMEM((places,) + s, BF16) for s in shapes]
    return pl.pallas_call(
        functools.partial(grid_scatter_kernel, count, places),
        out_shape=[jax.ShapeDtypeStruct(s, F32) for s in shapes],
        in_specs=[vmem] * count,
        out_specs=[vmem] * count,
        scratch_shapes=scratch
        + [
            dma((count, places, 4)),
            dma((count, places, 4)),
            dma((count, places, 2)),
            dma((count, places, 2)),
            dma((count, places, 4)),
            dma((count, places, 4)),
            dma((count, places)),
            dma((count, places + 1)),
        ],
        compiler_params=pltpu.CompilerParams(collective_id=ident, has_side_effects=True),
        name="grid_scatter",
    )(*fulls)


def gather_weights(blocks, lines, ident):
    places = lax.axis_size("row")
    if lax.axis_size("col") == 8 and places > 1 and blocks[0].shape[1] % 128 == 0:
        return grid_gather(blocks, lines, ident)
    fulls = gather_col([gather_row(block)[None] for block in blocks], ident)
    return [full[0] for full in fulls] + [gather_row(line) for line in lines]


def scatter_weights(fulls, ident):
    places = lax.axis_size("row")
    if lax.axis_size("col") == 8 and places > 1 and fulls[0].shape[1] // places % 128 == 0:
        return grid_scatter(fulls, ident)
    return [
        lax.psum_scatter(
            part[0].astype(BF16), "row", scatter_dimension=1, tiled=True
        ).astype(F32)
        for part in scatter_col([full[None] for full in fulls], ident)
    ]


def shards(
    hidden_in,
    out_grad,
    seq_lengths,
    norm1_gain,
    q_weight,
    q_bias,
    k_weight,
    k_bias,
    v_weight,
    v_bias,
    o_weight,
    norm2_gain,
    gate_weight,
    up_weight,
    down_weight,
):
    row_parts = lax.axis_size("row")
    col_parts = lax.axis_size("col")
    col_place = lax.axis_index("col")
    depth_own = q_weight.shape[0]
    depth = depth_own * row_parts
    q_own, k_own = q_weight.shape[1], k_weight.shape[1]
    smalls = (q_bias, k_bias, v_bias, norm1_gain, norm2_gain)
    small_sizes = [member.shape[0] for member in smalls]
    packed_small = jnp.concatenate(smalls)
    packed_small = jnp.pad(packed_small, (0, k_own * depth_own - packed_small.shape[0]))
    query_t, key_t, value_t, small_t, output_line = gather_weights(
        [q_weight.T, k_weight.T, v_weight.T, packed_small.reshape(k_own, depth_own)],
        [o_weight.T],
        1,
    )
    gate_own, up_own, down_own, small_t = lax.optimization_barrier(
        (gate_weight.T, up_weight.T, down_weight, small_t)
    )
    gate_t = gather_row(gate_own)
    up_t = gather_row(up_own)
    down_block = gather_row(down_own)
    small_flat = small_t.reshape(col_parts, k_own, row_parts, depth_own)
    small_flat = small_flat.transpose(2, 0, 1, 3).reshape(row_parts * col_parts, -1)
    small_full, offset = [], 0
    for size in small_sizes:
        small_full.append(small_flat[:, offset : offset + size].reshape(-1))
        offset += size
    query_offset, key_offset, value_offset, first_gain, second_gain = small_full


    own_rows = hidden_in.shape[0]
    row_tokens = own_rows * col_parts
    lengths = seq_lengths[0]
    query_slots = col_place * own_rows + jnp.arange(own_rows, dtype=jnp.int32)
    query_starts = seq_starts(query_slots, lengths)
    cosines, sines = rope_tables(query_slots - query_starts, HD)
    group_size = HQ // KVH
    score_scale = 1.0 / math.sqrt(HD)
    inputs_wide = hidden_in.astype(F32)
    first_rms = rms_scale(inputs_wide)
    first_unit = inputs_wide * first_rms
    first_normed = (first_unit * first_gain.astype(F32)).astype(BF16)
    query_base = dot_nt(first_normed, query_t) + query_offset.astype(F32)
    key_base = dot_nt(first_normed, key_t) + key_offset.astype(F32)
    value_own = (dot_nt(first_normed, value_t) + value_offset.astype(F32)).astype(BF16)
    queries = rotate_pairs(query_base.reshape(own_rows, HQ, HD), cosines, sines).astype(BF16)
    keys_own = rotate_pairs(key_base.reshape(own_rows, KVH, HD), cosines, sines).astype(BF16)
    both_own = jnp.concatenate([keys_own.reshape(own_rows, KVH * HD), value_own], axis=1)
    both_all, output_t = (
        member[0] for member in gather_col([both_own[None], output_line[None]], 2)
    )
    window = min(own_rows + MAXLEN, row_tokens)
    window_start = jnp.clip(col_place * own_rows - MAXLEN, 0, row_tokens - window)
    key_slots = window_start + jnp.arange(window, dtype=jnp.int32)
    key_starts = seq_starts(key_slots, lengths)
    visible = (query_starts[:, None] == key_starts[None, :]) & (
        key_slots[None, :] <= query_slots[:, None]
    )
    both_window = lax.dynamic_slice_in_dim(both_all, window_start, window, 0)
    keys_window = both_window[:, : KVH * HD].reshape(window, KVH, HD)
    values_window = both_window[:, KVH * HD :].reshape(window, KVH, HD)
    query_heads = queries.reshape(own_rows, KVH, group_size, HD)
    scores = masked_scores(query_heads, keys_window, visible, score_scale)
    peak = jnp.max(scores, axis=-1, keepdims=True)
    expanded = jnp.exp(scores - peak)
    totals = jnp.sum(expanded, axis=-1, keepdims=True)
    probs = expanded / totals
    log_total = peak + jnp.log(totals)
    mixed = jnp.einsum(
        "kgts,skd->tkgd", probs.astype(BF16), values_window, preferred_element_type=F32
    )
    mixed = mixed.reshape(own_rows, HQ * HD).astype(BF16)
    residual = inputs_wide + dot_nt(mixed, output_t)
    second_rms = rms_scale(residual)
    second_unit = residual * second_rms
    second_normed = (second_unit * second_gain.astype(F32)).astype(BF16)
    kernels = col_parts == 8
    if kernels:
        normed_rows, gate_act = ffn_gate(second_normed, gate_t, 3)
        out_rows, hidden, silu_gate, slope = ffn_up(out_grad, up_t, normed_rows, gate_act, 7)
    else:
        normed_rows, out_rows = (
            member[0] for member in gather_col([second_normed[None], out_grad[None]], 3)
        )
        gate_act = dot_nt(normed_rows, gate_t)
        up_act = dot_nt(normed_rows, up_t)
        sigmoid_gate = jax.nn.sigmoid(gate_act)
        silu_gate = gate_act * sigmoid_gate
        slope = up_act * sigmoid_gate * (1.0 + gate_act * (1.0 - sigmoid_gate))
        hidden = (silu_gate * up_act).astype(BF16)
    down_grad = weight_grad(out_rows, hidden)
    down_grad, out_rows = lax.optimization_barrier((down_grad, out_rows))
    down_grad_own = scatter_row(down_grad)
    if kernels:
        gate_grad_act, up_grad_act, branch_out, normed_grad = ffn_backward(
            out_rows, hidden, silu_gate, slope, gate_t, up_t, down_block, 4
        )
    else:
        hidden_grad = dot_nt(out_rows, down_block)
        up_grad_act = (hidden_grad * silu_gate).astype(BF16)
        gate_grad_act = (hidden_grad * slope).astype(BF16)
        normed_part = dot_nn(gate_grad_act, gate_t) + dot_nn(up_grad_act, up_t)
        branch_part = dot_nn(hidden, down_block)
        normed_grad, branch_out = (
            member[0] for member in scatter_col([normed_part[None], branch_part[None]], 4)
        )
    gate_grad = weight_grad(normed_rows, gate_grad_act)
    gate_grad, up_grad_act = lax.optimization_barrier((gate_grad, up_grad_act))
    gate_grad_own = scatter_row(gate_grad)
    up_grad = weight_grad(normed_rows, up_grad_act)
    up_grad, normed_grad = lax.optimization_barrier((up_grad, normed_grad))
    up_grad_own = scatter_row(up_grad)
    layer_out = residual + branch_out
    second_gain_grad = jnp.sum(normed_grad * second_unit, axis=0)
    unit_grad = normed_grad * second_gain.astype(F32)
    residual_grad = out_grad.astype(F32) + second_rms * (
        unit_grad - second_unit * jnp.mean(unit_grad * second_unit, axis=-1, keepdims=True)
    )
    attended_grad = residual_grad.astype(BF16)
    mixed_grad = dot_nn(attended_grad, output_t).astype(BF16)
    grad_heads = mixed_grad.reshape(own_rows, KVH, group_size, HD)
    scores = masked_scores(query_heads, keys_window, visible, score_scale)
    probs = jnp.exp(scores - log_total)
    prob_grad = jnp.einsum(
        "tkgd,skd->kgts", grad_heads, values_window, preferred_element_type=F32
    )
    value_part = jnp.einsum(
        "kgts,tkgd->skd", probs.astype(BF16), grad_heads, preferred_element_type=F32
    )
    score_grad = (
        probs * (prob_grad - jnp.sum(probs * prob_grad, axis=-1, keepdims=True))
    ).astype(BF16)
    query_grad = (
        jnp.einsum("kgts,skd->tkgd", score_grad, keys_window, preferred_element_type=F32)
        * score_scale
    )
    key_part = (
        jnp.einsum("kgts,tkgd->skd", score_grad, query_heads, preferred_element_type=F32)
        * score_scale
    )
    both_part = jnp.concatenate(
        [key_part.reshape(window, KVH * HD), value_part.reshape(window, KVH * HD)], axis=1
    ).astype(BF16)
    both_rows = lax.dynamic_update_slice_in_dim(
        jnp.zeros((row_tokens, 2 * KVH * HD), BF16), both_part, window_start, 0
    )
    both_rows, down_grad_own = lax.optimization_barrier((both_rows, down_grad_own))
    both_grad = scatter_col([both_rows[None]], 5)[0][0]
    key_grad, value_grad = both_grad[:, : KVH * HD], both_grad[:, KVH * HD :]
    query_wide = rounded_wide(query_grad.reshape(own_rows, HQ, HD))
    query_base_grad = (
        rotate_back(query_wide, cosines, sines).reshape(own_rows, HQ * HD).astype(BF16)
    )
    key_wide = rounded_wide(key_grad.reshape(own_rows, KVH, HD))
    key_base_grad = (
        rotate_back(key_wide, cosines, sines).reshape(own_rows, KVH * HD).astype(BF16)
    )
    value_base_grad = value_grad.astype(BF16)
    query_b_grad = jnp.sum(query_base_grad.astype(F32), axis=0)
    key_b_grad = jnp.sum(key_base_grad.astype(F32), axis=0)
    value_b_grad = jnp.sum(value_base_grad.astype(F32), axis=0)
    first_normed_grad = (
        dot_nn(query_base_grad, query_t)
        + dot_nn(key_base_grad, key_t)
        + dot_nn(value_base_grad, value_t)
    )
    first_gain_grad = jnp.sum(first_normed_grad * first_unit, axis=0)
    first_unit_grad = first_normed_grad * first_gain.astype(F32)
    input_grad = residual_grad + first_rms * (
        first_unit_grad
        - first_unit * jnp.mean(first_unit_grad * first_unit, axis=-1, keepdims=True)
    )
    small_grads = (query_b_grad, key_b_grad, value_b_grad, first_gain_grad, second_gain_grad)
    small_flat = jnp.concatenate(
        [member.reshape(row_parts * col_parts, -1) for member in small_grads], axis=1
    )
    small_flat = jnp.pad(
        small_flat, ((0, 0), (0, k_own * depth_own - small_flat.shape[1]))
    ).reshape(row_parts, col_parts, k_own, depth_own)
    small_flat = small_flat.transpose(1, 2, 0, 3).reshape(col_parts * k_own, depth)
    query_w = dot_tn(query_base_grad, first_normed).astype(BF16)
    query_w, gate_grad_own = lax.optimization_barrier((query_w, gate_grad_own))
    query_w_out, output_w_out, key_w_out, value_w_out, small_out = scatter_weights(
        [
            query_w,
            dot_tn(attended_grad, mixed).astype(BF16),
            dot_tn(key_base_grad, first_normed).astype(BF16),
            dot_tn(value_base_grad, first_normed).astype(BF16),
            small_flat.astype(BF16),
        ],
        6,
    )
    small_out = small_out.reshape(-1)
    small_list, offset = [], 0
    for size in small_sizes:
        small_list.append(small_out[offset : offset + size])
        offset += size
    return (
        layer_out,
        input_grad,
        small_list[3],
        query_w_out.T,
        small_list[0],
        key_w_out.T,
        small_list[1],
        value_w_out.T,
        small_list[2],
        output_w_out.T,
        small_list[4],
        gate_grad_own.astype(F32),
        up_grad_own.astype(F32),
        down_grad_own.astype(F32).T,
    )


def solution(mesh):
    in_specs = (
        P(("row", "col"), None),
        P(("row", "col"), None),
        P("row", None),
        P(("row", "col")),
        P("row", "col"),
        P(("row", "col")),
        P("row", "col"),
        P(("row", "col")),
        P("row", "col"),
        P(("row", "col")),
        P("row", "col"),
        P(("row", "col")),
        P("row", "col"),
        P("row", "col"),
        P("col", "row"),
    )
    out_specs = (
        P(("row", "col"), None),
        P(("row", "col"), None),
        P(("row", "col")),
        P("row", "col"),
        P(("row", "col")),
        P("row", "col"),
        P(("row", "col")),
        P("row", "col"),
        P(("row", "col")),
        P("row", "col"),
        P(("row", "col")),
        P("row", "col"),
        P("row", "col"),
        P("col", "row"),
    )
    return jax.shard_map(shards, mesh=mesh, in_specs=in_specs, out_specs=out_specs, check_vma=False)
```

```python
import functools
import math

import jax
import jax.numpy as jnp
from jax import lax
from jax.experimental import pallas as pl
from jax.experimental.pallas import tpu as pltpu
from jax.sharding import PartitionSpec as P

HQ = 12
KVH = 2
HD = 128
MAXLEN = 1024

EPSILON = 1e-06
ROPE_BASE = 1000000.0
BF16 = jnp.bfloat16
F32 = jnp.float32
MESH = pl.DeviceIdType.MESH


def seq_starts(slots, lengths):
    bounds = jnp.cumsum(lengths)
    picked = jnp.where(bounds[None, :] <= slots[:, None], lengths[None, :], 0)
    return jnp.sum(picked, axis=1)


def rope_tables(positions, head_dim):
    steps_up = jnp.arange(head_dim // 2, dtype=F32)
    freqs = jnp.exp(-math.log(ROPE_BASE) * (2.0 * steps_up / head_dim))
    angles = positions.astype(F32)[:, None] * freqs[None, :]
    angles = jnp.concatenate([angles, angles], axis=1)
    return (jnp.cos(angles)[:, None, :], jnp.sin(angles)[:, None, :])


def rotate_pairs(values, cosines, sines):
    half_dim = values.shape[-1] // 2
    turned = jnp.concatenate([-values[..., half_dim:], values[..., :half_dim]], axis=-1)
    return values * cosines + turned * sines


def rotate_back(grads_in, cosines, sines):
    half_dim = grads_in.shape[-1] // 2
    moved = grads_in * sines
    return grads_in * cosines + jnp.concatenate(
        [moved[..., half_dim:], -moved[..., :half_dim]], axis=-1
    )


def rms_scale(values):
    return lax.rsqrt(jnp.mean(values * values, axis=-1, keepdims=True) + EPSILON)


def dot_nn(left, right):
    return lax.dot_general(left, right, (((1,), (0,)), ((), ())), preferred_element_type=F32)


def dot_tn(left, right):
    return lax.dot_general(left, right, (((0,), (0,)), ((), ())), preferred_element_type=F32)


def dot_nt(left, right):
    return lax.dot_general(left, right, (((1,), (1,)), ((), ())), preferred_element_type=F32)


def rounded_wide(values):
    return lax.optimization_barrier(values.astype(BF16)).astype(F32)


def plane_places():
    me = lax.axis_index("col")
    chip, core = me // 2, me % 2
    low, high = chip % 2, chip // 2
    beside = high * 2 + (1 - low)
    above = (1 - high) * 2 + low
    across = (1 - high) * 2 + (1 - low)
    return chip, beside, above, across, core


def greet(peers):
    barrier = pltpu.get_barrier_semaphore()
    for peer in peers:
        pl.semaphore_signal(barrier, inc=1, device_id={"col": peer}, device_id_type=MESH)
    pl.semaphore_wait(barrier, len(peers))


def plane_gather_kernel(count, *refs):
    ins, outs = refs[:count], refs[count : 2 * count]
    send_sem, recv_sem, own_sem = refs[2 * count :]
    chip, beside, above, across, core = plane_places()
    mine = chip * 2 + core
    partner = chip * 2 + 1 - core
    to_x, to_y = beside * 2 + core, above * 2 + core
    greet((partner, to_x, to_y))

    def view(i, slot, part):
        size = ins[i].shape[1]
        half = size // 2
        if part is None:
            return outs[i].at[:, pl.ds(pl.multiple_of(slot * size, size), size), :]
        return outs[i].at[:, pl.ds(pl.multiple_of(slot * size + part * half, half), half), :]

    def copies(k, slot, part, peer, own=False):
        return [
            pltpu.make_async_remote_copy(
                src_ref=ins[i] if own else view(i, slot, part),
                dst_ref=view(i, slot, part),
                send_sem=send_sem.at[i, k],
                recv_sem=recv_sem.at[i, k],
                device_id={"col": peer},
                device_id_type=MESH,
            )
            for i in range(count)
        ]

    def start(cs):
        for c in cs:
            c.start()

    def wait_recv(cs):
        for c in cs:
            c.wait_recv()

    sent = [
        copies(1, mine, None, to_x, True),
        copies(2, mine, None, to_y, True),
        copies(0, mine, None, partner, True),
    ]
    for c in sent:
        start(c)
    own = [
        pltpu.make_async_copy(ins[i], view(i, mine, None), own_sem.at[i]) for i in range(count)
    ]
    start(own)
    other = 1 - core
    wait_recv(copies(1, to_x, None, to_x))
    more = [copies(3, to_x, 0, to_y), copies(5, to_x, None, partner)]
    for c in more:
        start(c)
    sent += more
    wait_recv(copies(2, to_y, None, to_y))
    more = [copies(4, to_y, 1, to_x), copies(6, to_y, None, partner)]
    for c in more:
        start(c)
    sent += more
    far = across * 2 + core
    wait_recv(copies(3, far, 0, to_y))
    more = [copies(7, far, 0, partner)]
    start(more[0])
    sent += more
    wait_recv(copies(4, far, 1, to_x))
    more = [copies(8, far, 1, partner)]
    start(more[0])
    sent += more
    wait_recv(copies(0, partner, None, partner))
    wait_recv(copies(5, beside * 2 + other, None, partner))
    wait_recv(copies(6, above * 2 + other, None, partner))
    wait_recv(copies(7, across * 2 + other, 0, partner))
    wait_recv(copies(8, across * 2 + other, 1, partner))
    for cs in sent:
        for c in cs:
            c.wait_send()
    for c in own:
        c.wait()


def plane_gather(shards, ident):
    count = len(shards)
    parts = lax.axis_size("col")
    outs = [
        jax.ShapeDtypeStruct((s.shape[0], s.shape[1] * parts, s.shape[2]), s.dtype)
        for s in shards
    ]
    return pl.pallas_call(
        functools.partial(plane_gather_kernel, count),
        out_shape=outs,
        in_specs=[pl.BlockSpec(memory_space=pl.ANY)] * count,
        out_specs=[pl.BlockSpec(memory_space=pl.ANY)] * count,
        scratch_shapes=[
            pltpu.SemaphoreType.DMA((count, 9)),
            pltpu.SemaphoreType.DMA((count, 9)),
            pltpu.SemaphoreType.DMA((count,)),
        ],
        compiler_params=pltpu.CompilerParams(collective_id=ident, has_side_effects=True),
        name="plane_gather",
    )(*shards)


def plane_scatter_kernel(count, *refs):
    ins, outs = refs[:count], refs[count : 2 * count]
    scratch = refs[2 * count :]
    near, made, side, land = (scratch[i * count : (i + 1) * count] for i in range(4))
    send_sem, recv_sem = scratch[4 * count :]
    chip, beside, above, across, core = plane_places()
    partner = chip * 2 + 1 - core
    to_x, to_y = beside * 2 + core, above * 2 + core
    greet((partner, to_x, to_y))
    order = (across, beside, above, chip)

    def rows(i, slot):
        size = outs[i].shape[1]
        return pl.ds(pl.multiple_of(slot * size, size), size)

    def half(i, part):
        size = outs[i].shape[1] // 2
        return pl.ds(part * size, size)

    def remote(i, k, src, dst, peer):
        return pltpu.make_async_remote_copy(
            src_ref=src,
            dst_ref=dst,
            send_sem=send_sem.at[i, k],
            recv_sem=recv_sem.at[i, k],
            device_id={"col": peer},
            device_id_type=MESH,
        )

    def near_copy(i, j):
        return remote(
            i, j, ins[i].at[:, rows(i, order[j] * 2 + 1 - core), :], near[i].at[j], partner
        )

    def side_copy(i, part):
        return remote(
            i, 4 + part, made[i].at[0, :, half(i, part), :], side[i].at[part],
            to_x if part == 0 else to_y,
        )

    def land_copy(i, which, part):
        return remote(
            i, 6 + which * 2 + part, made[i].at[1 + which, :, half(i, part), :],
            land[i].at[which, :, half(i, part), :], to_x if which == 0 else to_y,
        )

    step = 16

    def each(i, size, body):
        def tile(t, _):
            body(pl.multiple_of(t * step, step))
            return 0

        lax.fori_loop(0, size // step, tile, 0)

    def combine(i, j):
        size = outs[i].shape[1]
        first = (order[j] * 2 + core) * size

        def body(at):
            for a in range(outs[i].shape[0]):
                left = ins[i][a, pl.ds(pl.multiple_of(first + at, step), step), :].astype(F32)
                right = near[i][j, a, pl.ds(at, step), :].astype(F32)
                made[i][j, a, pl.ds(at, step), :] = (left + right).astype(BF16)

        each(i, size, body)

    def fold(i, which, part):
        size = outs[i].shape[1] // 2

        def body(at):
            at2 = pl.multiple_of(part * size + at, step)
            for a in range(outs[i].shape[0]):
                left = made[i][1 + which, a, pl.ds(at2, step), :].astype(F32)
                right = side[i][1 - which, a, pl.ds(at, step), :].astype(F32)
                made[i][1 + which, a, pl.ds(at2, step), :] = (left + right).astype(BF16)

        each(i, size, body)

    every = range(count)
    for j in range(4):
        for i in every:
            near_copy(i, j).start()
    for i in every:
        near_copy(i, 0).wait_recv()
        combine(i, 0)
        side_copy(i, 0).start()
        side_copy(i, 1).start()
    for i in every:
        near_copy(i, 1).wait_recv()
        combine(i, 1)
        land_copy(i, 0, 0).start()
    for i in every:
        near_copy(i, 2).wait_recv()
        combine(i, 2)
        land_copy(i, 1, 1).start()
    for i in every:
        side_copy(i, 0).wait_recv()
        fold(i, 1, 0)
        land_copy(i, 1, 0).start()
        side_copy(i, 1).wait_recv()
        fold(i, 0, 1)
        land_copy(i, 0, 1).start()
    for i in every:
        near_copy(i, 3).wait_recv()
    for i in every:
        for which in range(2):
            for part in range(2):
                land_copy(i, which, part).wait_recv()
        size = outs[i].shape[1]
        first = (chip * 2 + core) * size

        def body(at, i=i, first=first):
            for a in range(outs[i].shape[0]):
                spot = pl.ds(at, step)
                total = ins[i][a, pl.ds(pl.multiple_of(first + at, step), step), :].astype(F32)
                total += near[i][3, a, spot, :].astype(F32)
                total += land[i][0, a, spot, :].astype(F32)
                total += land[i][1, a, spot, :].astype(F32)
                outs[i][a, spot, :] = total.astype(outs[i].dtype)

        each(i, size, body)
    for i in every:
        for j in range(4):
            near_copy(i, j).wait_send()
        for part in range(2):
            side_copy(i, part).wait_send()
            for which in range(2):
                land_copy(i, which, part).wait_send()


def plane_scatter(fulls, ident, out_dtype=F32):
    count = len(fulls)
    parts = lax.axis_size("col")
    shapes = [(f.shape[0], f.shape[1] // parts, f.shape[2]) for f in fulls]
    scratch = []
    scratch += [pltpu.VMEM((4,) + s, BF16) for s in shapes]
    scratch += [pltpu.VMEM((3,) + s, BF16) for s in shapes]
    scratch += [pltpu.VMEM((2, s[0], s[1] // 2, s[2]), BF16) for s in shapes]
    scratch += [pltpu.VMEM((2,) + s, BF16) for s in shapes]
    return pl.pallas_call(
        functools.partial(plane_scatter_kernel, count),
        out_shape=[jax.ShapeDtypeStruct(s, out_dtype) for s in shapes],
        in_specs=[pl.BlockSpec(memory_space=pltpu.VMEM)] * count,
        out_specs=[pl.BlockSpec(memory_space=pltpu.VMEM)] * count,
        scratch_shapes=scratch
        + [pltpu.SemaphoreType.DMA((count, 10)), pltpu.SemaphoreType.DMA((count, 10))],
        compiler_params=pltpu.CompilerParams(collective_id=ident, has_side_effects=True),
        name="plane_scatter",
    )(*fulls)


def spans(total, most):
    return [(at, min(most, total - at)) for at in range(0, total, most)]


def remote(src, dst, send_sem, recv_sem, peer):
    return pltpu.make_async_remote_copy(
        src_ref=src,
        dst_ref=dst,
        send_sem=send_sem,
        recv_sem=recv_sem,
        device_id={"col": peer},
        device_id_type=MESH,
    )


def block_gather(source, land, send_sem, recv_sem):
    chip, beside, above, across, core = plane_places()
    half = source.shape[0] // 2
    mine, partner, other = chip * 2 + core, chip * 2 + 1 - core, 1 - core
    to_x, to_y, far = beside * 2 + core, above * 2 + core, across * 2 + core

    def copy(k, slot, part, peer, own=False):
        spot = land.at[slot] if part is None else land.at[slot, pl.ds(part * half, half), :]
        return remote(source if own else spot, spot, send_sem.at[k], recv_sem.at[k], peer)

    def first():
        greet((partner, to_x, to_y))
        copy(1, mine, None, to_x, True).start()
        copy(2, mine, None, to_y, True).start()
        copy(0, mine, None, partner, True).start()

    def second():
        copy(1, to_x, None, to_x).wait_recv()
        copy(3, to_x, 0, to_y).start()
        copy(5, to_x, None, partner).start()
        copy(2, to_y, None, to_y).wait_recv()
        copy(4, to_y, 1, to_x).start()
        copy(6, to_y, None, partner).start()

    def third():
        copy(3, far, 0, to_y).wait_recv()
        copy(7, far, 0, partner).start()
        copy(4, far, 1, to_x).wait_recv()
        copy(8, far, 1, partner).start()

    def landed(k):
        slot = (partner, beside * 2 + other, above * 2 + other)[k]
        copy((0, 5, 6)[k], slot, None, partner).wait_recv()

    def landed_far():
        copy(7, across * 2 + other, 0, partner).wait_recv()
        copy(8, across * 2 + other, 1, partner).wait_recv()

    def sent():
        for k, slot, part in (
            (0, mine, None), (1, mine, None), (2, mine, None), (3, to_x, 0), (4, to_y, 1),
            (5, to_x, None), (6, to_y, None), (7, far, 0), (8, far, 1),
        ):
            copy(k, slot, part, partner).wait_send()

    return first, second, third, landed, landed_far, sent


def spread(index, rows):
    return pl.ds(pl.multiple_of(index * rows, rows), rows)


def ffn_gate_kernel(
    normed, gate_t, normed_rows, gate_act, land, tiles, send_sem, recv_sem, keep_sem, tile_sem
):
    chip, _, _, _, core = plane_places()
    low, high = chip % 2, chip // 2
    rows = normed.shape[0]
    first, second, third, landed, landed_far, sent = block_gather(
        normed, land, send_sem, recv_sem
    )

    def keep(slot):
        return pltpu.make_async_copy(
            land.at[slot], normed_rows.at[spread(slot, rows), :], keep_sem.at[slot]
        )

    def put(slot, parity):
        return pltpu.make_async_copy(
            tiles.at[parity], gate_act.at[spread(slot, rows), :], tile_sem.at[parity]
        )

    first()
    land[chip * 2 + core] = normed[...]

    def step(s, _):
        flip = s // 2
        at_chip = (high + flip // 2) % 2 * 2 + (low + flip) % 2
        slot = at_chip * 2 + (core + s) % 2
        parity = s % 2

        @pl.when(s == 1)
        def _():
            landed(0)

        @pl.when(s == 2)
        def _():
            second()

        @pl.when(s == 3)
        def _():
            landed(1)

        @pl.when(s == 5)
        def _():
            landed(2)

        @pl.when(s == 6)
        def _():
            third()

        @pl.when(s == 7)
        def _():
            landed_far()

        keep(slot).start()

        @pl.when(s >= 2)
        def _():
            put(slot, parity).wait()

        for at, wide in spans(gate_t.shape[0], 512):
            tiles[parity, :, at : at + wide] = dot_nt(land[slot], gate_t[at : at + wide, :])
        put(slot, parity).start()
        return 0

    lax.fori_loop(0, 8, step, 0)
    for parity in range(2):
        put(0, parity).wait()

    def drain(slot, _):
        keep(slot).wait()
        return 0

    lax.fori_loop(0, 8, drain, 0)
    sent()


def ffn_gate(normed, gate_t, ident):
    rows, depth = normed.shape
    wide = gate_t.shape[0]
    dma = pltpu.SemaphoreType.DMA
    return pl.pallas_call(
        ffn_gate_kernel,
        out_shape=[
            jax.ShapeDtypeStruct((rows * 8, depth), BF16),
            jax.ShapeDtypeStruct((rows * 8, wide), F32),
        ],
        in_specs=[pl.BlockSpec(memory_space=pltpu.VMEM)] * 2,
        out_specs=[pl.BlockSpec(memory_space=pl.ANY)] * 2,
        scratch_shapes=[
            pltpu.VMEM((8, rows, depth), BF16),
            pltpu.VMEM((2, rows, wide), F32),
            dma((9,)),
            dma((9,)),
            dma((8,)),
            dma((2,)),
        ],
        compiler_params=pltpu.CompilerParams(collective_id=ident, has_side_effects=True),
        name="ffn_gate",
    )(normed, gate_t)


def ffn_up_kernel(
    cotangent,
    up_t,
    normed_rows,
    gate_act,
    out_rows,
    hidden,
    silu,
    slope,
    land,
    rows_in,
    gate_in,
    tiles,
    send_sem,
    recv_sem,
    keep_sem,
    in_sem,
    tile_sem,
):
    chip, _, _, _, core = plane_places()
    rows = cotangent.shape[0]
    first, second, third, landed, landed_far, sent = block_gather(
        cotangent, land, send_sem, recv_sem
    )

    def fetch(kind, s, parity):
        source = (normed_rows, gate_act)[kind]
        target = (rows_in, gate_in)[kind]
        return pltpu.make_async_copy(
            source.at[spread(s, rows), :], target.at[parity], in_sem.at[kind, parity]
        )

    def keep(slot):
        return pltpu.make_async_copy(
            land.at[slot], out_rows.at[spread(slot, rows), :], keep_sem.at[slot]
        )

    def put(kind, s, parity):
        target = (hidden, silu, slope)[kind]
        return pltpu.make_async_copy(
            tiles.at[kind, parity], target.at[spread(s, rows), :], tile_sem.at[kind, parity]
        )

    first()
    fetch(0, 0, 0).start()
    fetch(1, 0, 0).start()
    land[chip * 2 + core] = cotangent[...]

    def step(s, _):
        parity = s % 2

        @pl.when(s < 7)
        def _():
            fetch(0, s + 1, 1 - parity).start()
            fetch(1, s + 1, 1 - parity).start()

        @pl.when(s == 7)
        def _():
            second()

        @pl.when(s >= 2)
        def _():
            for kind in range(3):
                put(kind, s, parity).wait()

        fetch(0, s, parity).wait()
        fetch(1, s, parity).wait()
        for at, wide in spans(up_t.shape[0], 512):
            cut = slice(at, at + wide)
            up = dot_nt(rows_in[parity], up_t[cut, :])
            gate = gate_in[parity, :, cut]
            sigma = 1.0 / (1.0 + jnp.exp(-gate))
            smooth = gate * sigma
            tiles[0, parity, :, cut] = (smooth * up).astype(BF16)
            tiles[1, parity, :, cut] = smooth.astype(BF16)
            tiles[2, parity, :, cut] = (up * sigma * (1.0 + gate * (1.0 - sigma))).astype(BF16)
        for kind in range(3):
            put(kind, s, parity).start()
        return 0

    lax.fori_loop(0, 8, step, 0)
    landed(0)
    third()
    landed(1)
    landed(2)
    landed_far()

    def store(slot, _):
        keep(slot).start()
        return 0

    def drain(slot, _):
        keep(slot).wait()
        return 0

    lax.fori_loop(0, 8, store, 0)
    for parity in range(2):
        for kind in range(3):
            put(kind, 0, parity).wait()
    lax.fori_loop(0, 8, drain, 0)
    sent()


def ffn_up(cotangent, up_t, normed_rows, gate_act, ident):
    rows, depth = cotangent.shape
    wide = up_t.shape[0]
    dma = pltpu.SemaphoreType.DMA
    vmem = pl.BlockSpec(memory_space=pltpu.VMEM)
    anywhere = pl.BlockSpec(memory_space=pl.ANY)
    return pl.pallas_call(
        ffn_up_kernel,
        out_shape=[jax.ShapeDtypeStruct((rows * 8, depth), BF16)]
        + [jax.ShapeDtypeStruct((rows * 8, wide), BF16)] * 3,
        in_specs=[vmem, vmem, anywhere, anywhere],
        out_specs=[anywhere] * 4,
        scratch_shapes=[
            pltpu.VMEM((8, rows, depth), BF16),
            pltpu.VMEM((2, rows, depth), BF16),
            pltpu.VMEM((2, rows, wide), F32),
            pltpu.VMEM((3, 2, rows, wide), BF16),
            dma((9,)),
            dma((9,)),
            dma((8,)),
            dma((2, 2)),
            dma((3, 2)),
        ],
        compiler_params=pltpu.CompilerParams(collective_id=ident, has_side_effects=True),
        name="ffn_up",
    )(cotangent, up_t, normed_rows, gate_act)


def ffn_backward_kernel(
    out_rows,
    hidden,
    silu,
    slope,
    gate_t,
    up_t,
    down,
    gate_grad,
    up_grad,
    branch_own,
    normed_own,
    out_in,
    tiles_in,
    tiles_out,
    give,
    near,
    made,
    side,
    land,
    near_send,
    near_recv,
    side_send,
    side_recv,
    land_send,
    land_recv,
    in_sem,
    tile_sem,
):
    chip, beside, above, across, core = plane_places()
    low, high = chip % 2, chip // 2
    own_rows = branch_own.shape[0]
    half = own_rows // 2
    depth = branch_own.shape[1]
    partner = chip * 2 + 1 - core
    to_x, to_y = beside * 2 + core, above * 2 + core
    greet((partner, to_x, to_y))
    finals = (branch_own, normed_own)

    def spread(index):
        return pl.ds(pl.multiple_of(index * own_rows, own_rows), own_rows)

    def slot_of(s):
        flip = 3 - s // 2
        at_chip = (high + flip // 2) % 2 * 2 + (low + flip) % 2
        return at_chip * 2 + (core + 1 + s) % 2

    def near_copy(a, j):
        return remote(
            give.at[a, j], near.at[a, j], near_send.at[a, j], near_recv.at[a, j], partner
        )

    def side_copy(a, part):
        return remote(
            made.at[a, 0, pl.ds(part * half, half), :], side.at[a, part],
            side_send.at[a, part], side_recv.at[a, part], to_x if part == 0 else to_y,
        )

    def land_copy(a, which, part):
        k = which * 2 + part
        return remote(
            made.at[a, 1 + which, pl.ds(part * half, half), :],
            land.at[a, which, pl.ds(part * half, half), :],
            land_send.at[a, k], land_recv.at[a, k], to_x if which == 0 else to_y,
        )

    def fold(a, which, part):
        def tile(t, _):
            at = pl.multiple_of(t * 16, 16)
            spot = pl.ds(pl.multiple_of(part * half + at, 16), 16)
            left = made[a, 1 + which, spot, :].astype(F32)
            right = side[a, 1 - which, pl.ds(at, 16), :].astype(F32)
            made[a, 1 + which, spot, :] = (left + right).astype(BF16)
            return 0

        lax.fori_loop(0, half // 16, tile, 0)

    def fetch(kind, s, parity):
        if kind == 0:
            return pltpu.make_async_copy(
                out_rows.at[spread(slot_of(s)), :], out_in.at[parity], in_sem.at[0, parity]
            )
        source = (hidden, silu, slope)[kind - 1]
        return pltpu.make_async_copy(
            source.at[spread(slot_of(s)), :], tiles_in.at[kind - 1, parity], in_sem.at[kind, parity]
        )

    def put(kind, s, parity):
        target = (gate_grad, up_grad)[kind]
        return pltpu.make_async_copy(
            tiles_out.at[kind, parity], target.at[spread(slot_of(s)), :],
            tile_sem.at[kind, parity],
        )

    def sides(a):
        side_copy(a, 0).wait_recv()
        fold(a, 1, 0)
        land_copy(a, 1, 0).start()
        side_copy(a, 1).wait_recv()
        fold(a, 0, 1)
        land_copy(a, 0, 1).start()

    def deliver(a, s, partial):
        j = s // 2

        @pl.when(s % 2 == 0)
        def _():
            give[a, j] = partial().astype(BF16)
            near_copy(a, j).start()

        @pl.when(s % 2 == 1)
        def _():
            total = partial()
            near_copy(a, j).wait_recv()
            total = total + near[a, j].astype(F32)

            @pl.when(j < 3)
            def _():
                made[a, (3 - j) % 3] = total.astype(BF16)

            @pl.when(j == 0)
            def _():
                side_copy(a, 0).start()
                side_copy(a, 1).start()

            @pl.when(j == 1)
            def _():
                land_copy(a, 1, 1).start()

            @pl.when(j == 2)
            def _():
                land_copy(a, 0, 0).start()
                sides(a)

            @pl.when(j == 3)
            def _():
                finals[a][...] = total

    fetch(1, 0, 0).start()

    def branch_step(s, _):
        parity = s % 2

        @pl.when(s < 7)
        def _():
            fetch(1, s + 1, (s + 1) % 2).start()

        @pl.when(s == 6)
        def _():
            for kind in (0, 2, 3):
                fetch(kind, 0, 0).start()

        fetch(1, s, parity).wait()
        deliver(0, s, lambda: dot_nn(tiles_in[0, parity], down[...]))
        return 0

    lax.fori_loop(0, 8, branch_step, 0)

    def normed_step(s, _):
        parity = s % 2

        @pl.when(s < 7)
        def _():
            for kind in (0, 2, 3):
                fetch(kind, s + 1, (s + 1) % 2).start()

        for kind in (0, 2, 3):
            fetch(kind, s, parity).wait()

        @pl.when(s >= 2)
        def _():
            for kind in range(2):
                put(kind, s, parity).wait()

        for at, wide in spans(down.shape[0], 512):
            cut = slice(at, at + wide)
            hidden_grad = dot_nt(out_in[parity], down[cut, :])
            tiles_out[0, parity, :, cut] = (
                hidden_grad * tiles_in[2, parity, :, cut].astype(F32)
            ).astype(BF16)
            tiles_out[1, parity, :, cut] = (
                hidden_grad * tiles_in[1, parity, :, cut].astype(F32)
            ).astype(BF16)
        for kind in range(2):
            put(kind, s, parity).start()
        deliver(
            1, s,
            lambda: dot_nn(tiles_out[0, parity], gate_t[...])
            + dot_nn(tiles_out[1, parity], up_t[...]),
        )
        return 0

    lax.fori_loop(0, 8, normed_step, 0)
    for a in range(2):
        for which in range(2):
            for part in range(2):
                land_copy(a, which, part).wait_recv()

        def tile(t, _, a=a):
            spot = pl.ds(pl.multiple_of(t * 16, 16), 16)
            finals[a][spot, :] = (
                finals[a][spot, :]
                + land[a, 0, spot, :].astype(F32)
                + land[a, 1, spot, :].astype(F32)
            )
            return 0

        lax.fori_loop(0, own_rows // 16, tile, 0)
    for a in range(2):
        for j in range(4):
            near_copy(a, j).wait_send()
        for part in range(2):
            side_copy(a, part).wait_send()
            for which in range(2):
                land_copy(a, which, part).wait_send()
    for kind in range(2):
        for parity in range(2):
            put(kind, parity, parity).wait()


def ffn_backward(out_rows, hidden, silu, slope, gate_t, up_t, down, ident):
    total, depth = out_rows.shape
    wide = down.shape[0]
    rows = total // 8
    vmem = pl.BlockSpec(memory_space=pltpu.VMEM)
    anywhere = pl.BlockSpec(memory_space=pl.ANY)
    dma = pltpu.SemaphoreType.DMA
    return pl.pallas_call(
        ffn_backward_kernel,
        out_shape=[jax.ShapeDtypeStruct((total, wide), BF16)] * 2
        + [jax.ShapeDtypeStruct((rows, depth), F32)] * 2,
        in_specs=[anywhere] * 4 + [vmem] * 3,
        out_specs=[anywhere] * 2 + [vmem] * 2,
        scratch_shapes=[
            pltpu.VMEM((2, rows, depth), BF16),
            pltpu.VMEM((3, 2, rows, wide), BF16),
            pltpu.VMEM((2, 2, rows, wide), BF16),
            pltpu.VMEM((2, 4, rows, depth), BF16),
            pltpu.VMEM((2, 4, rows, depth), BF16),
            pltpu.VMEM((2, 3, rows, depth), BF16),
            pltpu.VMEM((2, 2, rows // 2, depth), BF16),
            pltpu.VMEM((2, 2, rows, depth), BF16),
            dma((2, 4)),
            dma((2, 4)),
            dma((2, 2)),
            dma((2, 2)),
            dma((2, 4)),
            dma((2, 4)),
            dma((4, 2)),
            dma((2, 2)),
        ],
        compiler_params=pltpu.CompilerParams(collective_id=ident, has_side_effects=True),
        name="ffn_backward",
    )(out_rows, hidden, silu, slope, gate_t, up_t, down)


def weight_grad_kernel(left, right, out):
    for at, wide in spans(right.shape[1], 512):
        out[:, at : at + wide] = lax.dot_general(
            left[...],
            right[:, at : at + wide],
            (((0,), (0,)), ((), ())),
            preferred_element_type=F32,
        ).astype(out.dtype)


def weight_grad(left, right):
    rows, depth = left.shape
    wide = right.shape[1]
    tile = 256
    return pl.pallas_call(
        weight_grad_kernel,
        grid=(depth // tile,),
        out_shape=jax.ShapeDtypeStruct((depth, wide), BF16),
        in_specs=[
            pl.BlockSpec((rows, tile), lambda i: (0, i)),
            pl.BlockSpec((rows, wide), lambda i: (0, 0)),
        ],
        out_specs=pl.BlockSpec((tile, wide), lambda i: (i, 0)),
        cost_estimate=pl.CostEstimate(
            flops=2 * rows * depth * wide,
            bytes_accessed=2 * (rows * depth + rows * wide + depth * wide),
            transcendentals=0,
        ),
        name="weight_grad",
    )(left, right)


def fill_mask(places, starts, mask):
    rows, window = mask.shape
    keys = places[0] + lax.broadcasted_iota(jnp.int32, (rows, window), 1)
    slots = places[1] + lax.broadcasted_iota(jnp.int32, (rows, window), 0)
    mask[...] = jnp.where((keys >= starts[...]) & (keys <= slots), 0.0, -jnp.inf)


def head_probs(query, keys, mask, score_scale):
    scores = dot_nt(query[...], keys[...]) * score_scale + mask[...]
    expanded = jnp.exp(scores - jnp.max(scores, axis=-1, keepdims=True))
    return expanded * (1.0 / jnp.sum(expanded, axis=-1, keepdims=True))


def attention_forward_kernel(score_scale, places, starts, query, keys, values, mixed, mask):
    @pl.when(pl.program_id(0) == 0)
    def _():
        fill_mask(places, starts, mask)

    probs = head_probs(query, keys, mask, score_scale)
    mixed[...] = dot_nn(probs.astype(BF16), values[...]).astype(BF16)


def attention_backward_kernel(
    score_scale,
    group,
    places,
    starts,
    query,
    cotangent,
    keys,
    values,
    query_grad,
    both_grad,
    mask,
    key_acc,
    value_acc,
):
    head = pl.program_id(0)
    window, wide = keys.shape

    @pl.when(head == 0)
    def _():
        fill_mask(places, starts, mask)
        both_grad[...] = jnp.zeros(both_grad.shape, both_grad.dtype)

    @pl.when(head % group == 0)
    def _():
        key_acc[...] = jnp.zeros(key_acc.shape, F32)
        value_acc[...] = jnp.zeros(value_acc.shape, F32)

    probs = head_probs(query, keys, mask, score_scale)
    prob_grad = dot_nt(cotangent[...], values[...])
    value_acc[...] += dot_tn(probs.astype(BF16), cotangent[...])
    centre = jnp.sum(probs * prob_grad, axis=-1, keepdims=True)
    score_grad = (probs * (prob_grad - centre)).astype(BF16)
    query_grad[...] = (dot_nn(score_grad, keys[...]) * score_scale).astype(BF16)
    key_acc[...] += dot_tn(score_grad, query[...])

    @pl.when(head % group == group - 1)
    def _():
        rows = pl.ds(pl.multiple_of(places[0], 128), window)
        half = both_grad.shape[1] // 2
        at = head // group * wide
        both_grad[rows, pl.ds(pl.multiple_of(at, wide), wide)] = (
            key_acc[...] * score_scale
        ).astype(BF16)
        both_grad[rows, pl.ds(pl.multiple_of(half + at, wide), wide)] = value_acc[...].astype(
            BF16
        )


def attention_specs(rows, window, wide, group, kv_heads):
    smem = pl.BlockSpec(memory_space=pltpu.SMEM)
    starts = pl.BlockSpec((rows, 1), lambda h: (0, 0))
    head = pl.BlockSpec((rows, wide), lambda h: (0, h))
    keys = pl.BlockSpec((window, wide), lambda h: (0, h // group))
    values = pl.BlockSpec((window, wide), lambda h: (0, kv_heads + h // group))
    return smem, starts, head, keys, values


def attention_forward(places, starts, queries, both_window, wide, kv_heads):
    rows, window = queries.shape[0], both_window.shape[0]
    heads = queries.shape[1] // wide
    smem, first, head, keys, values = attention_specs(
        rows, window, wide, heads // kv_heads, kv_heads
    )
    return pl.pallas_call(
        functools.partial(attention_forward_kernel, 1.0 / math.sqrt(wide)),
        grid=(heads,),
        out_shape=jax.ShapeDtypeStruct(queries.shape, BF16),
        in_specs=[smem, first, head, keys, values],
        out_specs=head,
        scratch_shapes=[pltpu.VMEM((rows, window), F32)],
        name="attention_forward",
    )(places, starts, queries, both_window, both_window)


def attention_backward(
    places, starts, queries, cotangent, both_window, wide, kv_heads, row_tokens
):
    rows, window = queries.shape[0], both_window.shape[0]
    heads = queries.shape[1] // wide
    group = heads // kv_heads
    smem, first, head, keys, values = attention_specs(rows, window, wide, group, kv_heads)
    full = (row_tokens, 2 * kv_heads * wide)
    return pl.pallas_call(
        functools.partial(attention_backward_kernel, 1.0 / math.sqrt(wide), group),
        grid=(heads,),
        out_shape=[
            jax.ShapeDtypeStruct(queries.shape, BF16),
            jax.ShapeDtypeStruct(full, BF16),
        ],
        in_specs=[smem, first, head, head, keys, values],
        out_specs=[head, pl.BlockSpec(full, lambda h: (0, 0))],
        scratch_shapes=[
            pltpu.VMEM((rows, window), F32),
            pltpu.VMEM((window, wide), F32),
            pltpu.VMEM((window, wide), F32),
        ],
        name="attention_backward",
    )(places, starts, queries, cotangent, both_window, both_window)


def gather_row(block):
    return lax.all_gather(block, "row", axis=block.ndim - 1, tiled=True)


def scatter_row(full):
    return lax.psum_scatter(
        full.astype(BF16), "row", scatter_dimension=0, tiled=True
    )


def gather_col(blocks, ident):
    if lax.axis_size("col") == 8:
        return plane_gather(blocks, ident)
    return [lax.all_gather(block, "col", axis=1, tiled=True) for block in blocks]


def scatter_col(fulls, ident):
    fulls = [full.astype(BF16) for full in fulls]
    if lax.axis_size("col") == 8:
        return plane_scatter(fulls, ident)
    return [
        lax.psum_scatter(full, "col", scatter_dimension=1, tiled=True).astype(F32)
        for full in fulls
    ]


def line_remote(src, dst, send_sem, recv_sem, peer):
    return pltpu.make_async_remote_copy(
        src_ref=src,
        dst_ref=dst,
        send_sem=send_sem,
        recv_sem=recv_sem,
        device_id={"row": peer},
        device_id_type=MESH,
    )


def greet_grid(peers, place, places):
    barrier = pltpu.get_barrier_semaphore()
    for peer in peers:
        pl.semaphore_signal(barrier, inc=1, device_id={"col": peer}, device_id_type=MESH)

    @pl.when(place > 0)
    def _():
        pl.semaphore_signal(barrier, inc=1, device_id={"row": place - 1}, device_id_type=MESH)

    @pl.when(place < places - 1)
    def _():
        pl.semaphore_signal(barrier, inc=1, device_id={"row": place + 1}, device_id_type=MESH)

    edge = (place == 0) | (place == places - 1)

    @pl.when(edge)
    def _():
        pl.semaphore_wait(barrier, len(peers) + 1)

    @pl.when(jnp.logical_not(edge))
    def _():
        pl.semaphore_wait(barrier, len(peers) + 2)


def grid_gather_kernel(count, extra, places, *refs):
    both_count = count + extra
    ins, outs = refs[:both_count], refs[both_count : 2 * both_count]
    send_sem, recv_sem, line_send, line_recv, own_sem = refs[2 * both_count :]
    place = lax.axis_index("row")
    chip, beside, above, across, core = plane_places()
    mine, partner, other = chip * 2 + core, chip * 2 + 1 - core, 1 - core
    to_x, to_y, far = beside * 2 + core, above * 2 + core, across * 2 + core
    every = range(count)
    others = range(count, both_count)
    greet_grid((partner, to_x, to_y) if count else (), place, places)

    def view(i, slot, line, part):
        size, wide = ins[i].shape
        spot = pl.ds(pl.multiple_of(line * wide, wide), wide)
        if i >= count:
            return outs[i].at[:, spot]
        if part is None:
            return outs[i].at[pl.ds(pl.multiple_of(slot * size, size), size), spot]
        half = size // 2
        return outs[i].at[pl.ds(pl.multiple_of(slot * size + part * half, half), half), spot]

    def copies(k, slot, line, part, peer, own=False):
        return [
            remote(
                ins[i] if own else view(i, slot, line, part),
                view(i, slot, line, part),
                send_sem.at[i, line, k],
                recv_sem.at[i, line, k],
                peer,
            )
            for i in every
        ]

    def line_copies(line, sem_at, peer, own=False, which=every):
        return [
            line_remote(
                ins[i] if own else view(i, mine, line, None),
                view(i, mine, line, None),
                line_send.at[i, sem_at],
                line_recv.at[i, line],
                peer,
            )
            for i in which
        ]

    def start(cs):
        for c in cs:
            c.start()

    def wait_recv(cs):
        for c in cs:
            c.wait_recv()

    def first(line, own=False):
        start(copies(1, mine, line, None, to_x, own))
        start(copies(2, mine, line, None, to_y, own))
        start(copies(0, mine, line, None, partner, own))

    def second(line):
        wait_recv(copies(1, to_x, line, None, to_x))
        start(copies(3, to_x, line, 0, to_y))
        start(copies(5, to_x, line, None, partner))
        wait_recv(copies(2, to_y, line, None, to_y))
        start(copies(4, to_y, line, 1, to_x))
        start(copies(6, to_y, line, None, partner))

    def third(line):
        wait_recv(copies(3, far, line, 0, to_y))
        start(copies(7, far, line, 0, partner))
        wait_recv(copies(4, far, line, 1, to_x))
        start(copies(8, far, line, 1, partner))

    def last(line):
        wait_recv(copies(0, partner, line, None, partner))
        wait_recv(copies(5, beside * 2 + other, line, None, partner))
        wait_recv(copies(6, above * 2 + other, line, None, partner))
        wait_recv(copies(7, across * 2 + other, line, 0, partner))
        wait_recv(copies(8, across * 2 + other, line, 1, partner))
        for k, slot, part in (
            (0, mine, None), (1, mine, None), (2, mine, None), (3, to_x, 0), (4, to_y, 1),
            (5, to_x, None), (6, to_y, None), (7, far, 0), (8, far, 1),
        ):
            for c in copies(k, slot, line, part, partner):
                c.wait_send()

    def both(distance, body):
        @pl.when((distance >= 1) & (place - distance >= 0))
        def _():
            body(place - distance)

        @pl.when((distance >= 1) & (place + distance < places))
        def _():
            body(place + distance)

        @pl.when(distance == 0)
        def _():
            body(place)

    @pl.when(place < places - 1)
    def _():
        start(line_copies(place, place, place + 1, True))
        start(line_copies(place, place, place + 1, True, others))

    @pl.when(place > 0)
    def _():
        start(line_copies(place, places, place - 1, True))
        start(line_copies(place, places, place - 1, True, others))

    first(place, True)
    own = [
        pltpu.make_async_copy(ins[i], view(i, mine, place, None), own_sem.at[i])
        for i in range(both_count)
    ]
    start(own)

    def pass_on(line):
        @pl.when(line != place)
        def _():
            wait_recv(line_copies(line, line, place, False, others))

        @pl.when((line < place) & (place < places - 1))
        def _():
            start(line_copies(line, line, place + 1, False, others))

        @pl.when((line > place) & (place > 0))
        def _():
            start(line_copies(line, line, place - 1, False, others))

    def step(t, _):
        @pl.when((t >= 1) & (place - t >= 0))
        def _():
            line = place - t
            wait_recv(line_copies(line, line, place))

            @pl.when(place < places - 1)
            def _():
                start(line_copies(line, line, place + 1))

            first(line)

        @pl.when((t >= 1) & (place + t < places))
        def _():
            line = place + t
            wait_recv(line_copies(line, line, place))

            @pl.when(place > 0)
            def _():
                start(line_copies(line, line, place - 1))

            first(line)

        both(t - 1, second)
        if extra:
            both(t - 1, pass_on)
        both(t - 2, third)
        return 0

    lax.fori_loop(0, places + 2, step, 0)

    everything = range(both_count)

    def finish(line, _):
        last(line)
        relays = ((line < place) & (place < places - 1)) | ((line > place) & (place > 0))

        @pl.when(relays)
        def _():
            for c in line_copies(line, line, place, False, everything):
                c.wait_send()

        return 0

    lax.fori_loop(0, places, finish, 0)

    @pl.when(place < places - 1)
    def _():
        for c in line_copies(place, place, place, False, everything):
            c.wait_send()

    @pl.when(place > 0)
    def _():
        for c in line_copies(place, places, place, False, everything):
            c.wait_send()

    for c in own:
        c.wait()


def grid_gather(shards, lines, ident):
    count, extra = len(shards), len(lines)
    places, parts = lax.axis_size("row"), lax.axis_size("col")
    dma = pltpu.SemaphoreType.DMA
    anywhere = pl.BlockSpec(memory_space=pl.ANY)
    return pl.pallas_call(
        functools.partial(grid_gather_kernel, count, extra, places),
        out_shape=[
            jax.ShapeDtypeStruct((s.shape[0] * parts, s.shape[1] * places), s.dtype)
            for s in shards
        ]
        + [jax.ShapeDtypeStruct((s.shape[0], s.shape[1] * places), s.dtype) for s in lines],
        in_specs=[anywhere] * (count + extra),
        out_specs=[anywhere] * (count + extra),
        scratch_shapes=[
            dma((max(count, 1), places, 9)),
            dma((max(count, 1), places, 9)),
            dma((count + extra, places + 1)),
            dma((count + extra, places)),
            dma((count + extra,)),
        ],
        compiler_params=pltpu.CompilerParams(collective_id=ident, has_side_effects=True),
        name="grid_gather",
    )(*shards, *lines)


def grid_scatter_kernel(count, places, *refs):
    ins, outs = refs[:count], refs[count : 2 * count]
    scratch = refs[2 * count :]
    near, made, side, land, line_in, line_out = (
        scratch[i * count : (i + 1) * count] for i in range(6)
    )
    (
        near_send, near_recv, side_send, side_recv, land_send, land_recv, line_send, line_recv,
    ) = scratch[6 * count :]
    place = lax.axis_index("row")
    chip, beside, above, across, core = plane_places()
    partner = chip * 2 + 1 - core
    to_x, to_y = beside * 2 + core, above * 2 + core
    order = (across, beside, above, chip)
    every = range(count)
    greet_grid((partner, to_x, to_y), place, places)

    def source(i, slot, line, at, size):
        rows, wide = outs[i].shape
        return (
            pl.ds(pl.multiple_of(slot * rows + at, size), size),
            pl.ds(pl.multiple_of(line * wide, wide), wide),
        )

    def near_copy(i, line, j):
        rows = outs[i].shape[0]
        return remote(
            ins[i].at[source(i, order[j] * 2 + 1 - core, line, 0, rows)],
            near[i].at[line, j],
            near_send.at[i, line, j], near_recv.at[i, line, j], partner,
        )

    def halves(i, part):
        half = outs[i].shape[0] // 2
        return pl.ds(part * half, half)

    def side_copy(i, line, part):
        return remote(
            made[i].at[line, 0, halves(i, part), :], side[i].at[line, part],
            side_send.at[i, line, part], side_recv.at[i, line, part],
            to_x if part == 0 else to_y,
        )

    def land_copy(i, line, which, part):
        k = which * 2 + part
        return remote(
            made[i].at[line, 1 + which, halves(i, part), :],
            land[i].at[line, which, halves(i, part), :],
            land_send.at[i, line, k], land_recv.at[i, line, k],
            to_x if which == 0 else to_y,
        )

    def up_copy(i, line):
        return line_remote(
            line_out[i].at[line], line_in[i].at[line],
            line_send.at[i, line], line_recv.at[i, line], place + 1,
        )

    def down_copy(i, line):
        target = jnp.where(line == place - 1, places, line)
        return line_remote(
            line_out[i].at[line], line_in[i].at[target],
            line_send.at[i, line], line_recv.at[i, target], place - 1,
        )

    def each(size, body):
        def tile(t, _):
            body(pl.multiple_of(t * 16, 16))
            return 0

        lax.fori_loop(0, size // 16, tile, 0)

    def combine(i, line, j):
        def body(at):
            spot = pl.ds(at, 16)
            left = ins[i][source(i, order[j] * 2 + core, line, at, 16)].astype(F32)
            made[i][line, j, spot, :] = (left + near[i][line, j, spot, :].astype(F32)).astype(
                BF16
            )

        each(outs[i].shape[0], body)

    def fold(i, line, which, part):
        half = outs[i].shape[0] // 2

        def body(at):
            spot = pl.ds(pl.multiple_of(part * half + at, 16), 16)
            left = made[i][line, 1 + which, spot, :].astype(F32)
            right = side[i][line, 1 - which, pl.ds(at, 16), :].astype(F32)
            made[i][line, 1 + which, spot, :] = (left + right).astype(BF16)

        each(half, body)

    def sequence(q):
        up = places - 1 - place
        return jnp.where(q < up, places - 1 - q, q - up)

    def first(line):
        for i in every:
            near_copy(i, line, 0).wait_recv()
            combine(i, line, 0)
            side_copy(i, line, 0).start()
            side_copy(i, line, 1).start()
        for i in every:
            near_copy(i, line, 1).wait_recv()
            combine(i, line, 1)
            land_copy(i, line, 0, 0).start()
            near_copy(i, line, 2).wait_recv()
            combine(i, line, 2)
            land_copy(i, line, 1, 1).start()

    def second(line):
        for i in every:
            side_copy(i, line, 0).wait_recv()
            fold(i, line, 1, 0)
            land_copy(i, line, 1, 0).start()
            side_copy(i, line, 1).wait_recv()
            fold(i, line, 0, 1)
            land_copy(i, line, 0, 1).start()

    def arrived(i, slot):
        line_remote(
            line_out[i].at[0], line_in[i].at[slot],
            line_send.at[i, 0], line_recv.at[i, slot], place,
        ).wait_recv()

    def third(line):
        for i in every:
            near_copy(i, line, 3).wait_recv()
            for which in range(2):
                for part in range(2):
                    land_copy(i, line, which, part).wait_recv()

        @pl.when((line > place) & (place > 0))
        def _():
            for i in every:
                arrived(i, line)

        @pl.when((line < place) & (place < places - 1))
        def _():
            for i in every:
                arrived(i, line)

        @pl.when((line == place) & (place > 0))
        def _():
            for i in every:
                arrived(i, place)

        @pl.when((line == place) & (place < places - 1))
        def _():
            for i in every:
                arrived(i, places)

        def total(i, at):
            spot = pl.ds(at, 16)
            value = ins[i][source(i, chip * 2 + core, line, at, 16)].astype(F32)
            value += near[i][line, 3, spot, :].astype(F32)
            value += land[i][line, 0, spot, :].astype(F32)
            value += land[i][line, 1, spot, :].astype(F32)
            return value

        for i in every:
            relays = ((line > place) & (place > 0)) | ((line < place) & (place < places - 1))

            @pl.when((line != place) & relays)
            def _(i=i):
                def body(at):
                    spot = pl.ds(at, 16)
                    line_out[i][line, spot, :] = (
                        total(i, at) + line_in[i][line, spot, :].astype(F32)
                    ).astype(BF16)

                each(outs[i].shape[0], body)

            @pl.when((line != place) & jnp.logical_not(relays))
            def _(i=i):
                def body(at):
                    line_out[i][line, pl.ds(at, 16), :] = total(i, at).astype(BF16)

                each(outs[i].shape[0], body)

            @pl.when(line > place)
            def _(i=i):
                up_copy(i, line).start()

            @pl.when(line < place)
            def _(i=i):
                down_copy(i, line).start()

            @pl.when(line == place)
            def _(i=i):
                def body(at):
                    outs[i][pl.ds(at, 16), :] = total(i, at)

                each(outs[i].shape[0], body)

                @pl.when(place > 0)
                def _():
                    def more(at):
                        spot = pl.ds(at, 16)
                        outs[i][spot, :] += line_in[i][place, spot, :].astype(F32)

                    each(outs[i].shape[0], more)

                @pl.when(place < places - 1)
                def _():
                    def more(at):
                        spot = pl.ds(at, 16)
                        outs[i][spot, :] += line_in[i][places, spot, :].astype(F32)

                    each(outs[i].shape[0], more)

    def begin(q, _):
        line = sequence(q)
        for j in range(4):
            for i in every:
                near_copy(i, line, j).start()
        return 0

    lax.fori_loop(0, places, begin, 0)

    def step(t, _):
        @pl.when(t < places)
        def _():
            first(sequence(t))

        @pl.when((t >= 1) & (t - 1 < places))
        def _():
            second(sequence(t - 1))

        @pl.when(t >= 2)
        def _():
            third(sequence(t - 2))

        return 0

    lax.fori_loop(0, places + 2, step, 0)

    def finish(line, _):
        for i in every:
            for j in range(4):
                near_copy(i, line, j).wait_send()
            for part in range(2):
                side_copy(i, line, part).wait_send()
                for which in range(2):
                    land_copy(i, line, which, part).wait_send()

            @pl.when(line != place)
            def _(i=i):
                up_copy(i, line).wait_send()

        return 0

    lax.fori_loop(0, places, finish, 0)


def grid_scatter(fulls, ident):
    count = len(fulls)
    places, parts = lax.axis_size("row"), lax.axis_size("col")
    shapes = [(f.shape[0] // parts, f.shape[1] // places) for f in fulls]
    dma = pltpu.SemaphoreType.DMA
    vmem = pl.BlockSpec(memory_space=pltpu.VMEM)
    scratch = []
    scratch += [pltpu.VMEM((places, 4) + s, BF16) for s in shapes]
    scratch += [pltpu.VMEM((places, 3) + s, BF16) for s in shapes]
    scratch += [pltpu.VMEM((places, 2, s[0] // 2, s[1]), BF16) for s in shapes]
    scratch += [pltpu.VMEM((places, 2) + s, BF16) for s in shapes]
    scratch += [pltpu.VMEM((places + 1,) + s, BF16) for s in shapes]
    scratch += [pltpu.VMEM((places,) + s, BF16) for s in shapes]
    return pl.pallas_call(
        functools.partial(grid_scatter_kernel, count, places),
        out_shape=[jax.ShapeDtypeStruct(s, F32) for s in shapes],
        in_specs=[vmem] * count,
        out_specs=[vmem] * count,
        scratch_shapes=scratch
        + [
            dma((count, places, 4)),
            dma((count, places, 4)),
            dma((count, places, 2)),
            dma((count, places, 2)),
            dma((count, places, 4)),
            dma((count, places, 4)),
            dma((count, places)),
            dma((count, places + 1)),
        ],
        compiler_params=pltpu.CompilerParams(collective_id=ident, has_side_effects=True),
        name="grid_scatter",
    )(*fulls)


def gather_lines(lines, ident):
    places = lax.axis_size("row")
    if lax.axis_size("col") == 8 and places > 1 and lines[0].shape[1] % 128 == 0:
        return grid_gather([], lines, ident)
    return [gather_row(line) for line in lines]


def scatter_weights(fulls, ident):
    places = lax.axis_size("row")
    if lax.axis_size("col") == 8 and places > 1 and fulls[0].shape[1] // places % 128 == 0:
        return grid_scatter(fulls, ident)
    return [
        lax.psum_scatter(
            part[0].astype(BF16), "row", scatter_dimension=1, tiled=True
        ).astype(F32)
        for part in scatter_col([full[None] for full in fulls], ident)
    ]


def shards(
    hidden_in,
    out_grad,
    seq_lengths,
    norm1_gain,
    q_weight,
    q_bias,
    k_weight,
    k_bias,
    v_weight,
    v_bias,
    o_weight,
    norm2_gain,
    gate_weight,
    up_weight,
    down_weight,
):
    row_parts = lax.axis_size("row")
    col_parts = lax.axis_size("col")
    col_place = lax.axis_index("col")
    depth_own = q_weight.shape[0]
    depth = depth_own * row_parts
    q_own, k_own = q_weight.shape[1], k_weight.shape[1]
    smalls = (q_bias, k_bias, v_bias, norm1_gain, norm2_gain)
    small_sizes = [member.shape[0] for member in smalls]
    packed_small = jnp.concatenate(smalls)
    packed_small = jnp.pad(packed_small, (0, k_own * depth_own - packed_small.shape[0]))
    *plane_lines, output_line = gather_lines(
        [
            q_weight.T,
            k_weight.T,
            v_weight.T,
            packed_small.reshape(k_own, depth_own),
            o_weight.T,
        ],
        1,
    )
    gate_own, up_own, down_own, output_line = lax.optimization_barrier(
        (gate_weight.T, up_weight.T, down_weight, output_line)
    )
    query_t, key_t, value_t, small_t = (
        member[0] for member in gather_col([line[None] for line in plane_lines], 8)
    )
    gate_t = gather_row(gate_own)
    up_t = gather_row(up_own)
    down_block = gather_row(down_own)
    small_flat = small_t.reshape(col_parts, k_own, row_parts, depth_own)
    small_flat = small_flat.transpose(2, 0, 1, 3).reshape(row_parts * col_parts, -1)
    small_full, offset = [], 0
    for size in small_sizes:
        small_full.append(small_flat[:, offset : offset + size].reshape(-1))
        offset += size
    query_offset, key_offset, value_offset, first_gain, second_gain = small_full


    own_rows = hidden_in.shape[0]
    row_tokens = own_rows * col_parts
    lengths = seq_lengths[0]
    query_slots = col_place * own_rows + jnp.arange(own_rows, dtype=jnp.int32)
    query_starts = seq_starts(query_slots, lengths)
    cosines, sines = rope_tables(query_slots - query_starts, HD)
    inputs_wide = hidden_in.astype(F32)
    first_rms = rms_scale(inputs_wide)
    first_unit = inputs_wide * first_rms
    first_normed = (first_unit * first_gain.astype(F32)).astype(BF16)
    query_base = dot_nt(first_normed, query_t) + query_offset.astype(F32)
    key_base = dot_nt(first_normed, key_t) + key_offset.astype(F32)
    value_own = (dot_nt(first_normed, value_t) + value_offset.astype(F32)).astype(BF16)
    queries = rotate_pairs(query_base.reshape(own_rows, HQ, HD), cosines, sines).astype(BF16)
    keys_own = rotate_pairs(key_base.reshape(own_rows, KVH, HD), cosines, sines).astype(BF16)
    both_own = jnp.concatenate([keys_own.reshape(own_rows, KVH * HD), value_own], axis=1)
    both_all, output_t = (
        member[0] for member in gather_col([both_own[None], output_line[None]], 2)
    )
    window = min(own_rows + MAXLEN, row_tokens)
    window_start = jnp.clip(col_place * own_rows - MAXLEN, 0, row_tokens - window)
    both_window = lax.dynamic_slice_in_dim(both_all, window_start, window, 0)
    places = jnp.stack([window_start, col_place * own_rows]).astype(jnp.int32)
    starts = query_starts.astype(jnp.int32)[:, None]
    queries = queries.reshape(own_rows, HQ * HD)
    mixed = attention_forward(places, starts, queries, both_window, HD, KVH)
    residual = inputs_wide + dot_nt(mixed, output_t)
    second_rms = rms_scale(residual)
    second_unit = residual * second_rms
    second_normed = (second_unit * second_gain.astype(F32)).astype(BF16)
    kernels = col_parts == 8
    if kernels:
        normed_rows, gate_act = ffn_gate(second_normed, gate_t, 3)
        out_rows, hidden, silu_gate, slope = ffn_up(out_grad, up_t, normed_rows, gate_act, 7)
    else:
        normed_rows, out_rows = (
            member[0] for member in gather_col([second_normed[None], out_grad[None]], 3)
        )
        gate_act = dot_nt(normed_rows, gate_t)
        up_act = dot_nt(normed_rows, up_t)
        sigmoid_gate = jax.nn.sigmoid(gate_act)
        silu_gate = gate_act * sigmoid_gate
        slope = up_act * sigmoid_gate * (1.0 + gate_act * (1.0 - sigmoid_gate))
        hidden = (silu_gate * up_act).astype(BF16)
    down_grad = weight_grad(out_rows, hidden)
    down_grad, out_rows = lax.optimization_barrier((down_grad, out_rows))
    down_grad_own = scatter_row(down_grad)
    if kernels:
        gate_grad_act, up_grad_act, branch_out, normed_grad = ffn_backward(
            out_rows, hidden, silu_gate, slope, gate_t, up_t, down_block, 4
        )
    else:
        hidden_grad = dot_nt(out_rows, down_block)
        up_grad_act = (hidden_grad * silu_gate).astype(BF16)
        gate_grad_act = (hidden_grad * slope).astype(BF16)
        normed_part = dot_nn(gate_grad_act, gate_t) + dot_nn(up_grad_act, up_t)
        branch_part = dot_nn(hidden, down_block)
        normed_grad, branch_out = (
            member[0] for member in scatter_col([normed_part[None], branch_part[None]], 4)
        )
    gate_grad = weight_grad(normed_rows, gate_grad_act)
    gate_grad, up_grad_act = lax.optimization_barrier((gate_grad, up_grad_act))
    gate_grad_own = scatter_row(gate_grad)
    up_grad = weight_grad(normed_rows, up_grad_act)
    up_grad, normed_grad = lax.optimization_barrier((up_grad, normed_grad))
    up_grad_own = scatter_row(up_grad)
    layer_out = residual + branch_out
    second_gain_grad = jnp.sum(normed_grad * second_unit, axis=0)
    unit_grad = normed_grad * second_gain.astype(F32)
    residual_grad = out_grad.astype(F32) + second_rms * (
        unit_grad - second_unit * jnp.mean(unit_grad * second_unit, axis=-1, keepdims=True)
    )
    attended_grad = residual_grad.astype(BF16)
    mixed_grad = dot_nn(attended_grad, output_t).astype(BF16)
    query_grad, both_rows = attention_backward(
        places, starts, queries, mixed_grad, both_window, HD, KVH, row_tokens
    )
    both_rows, down_grad_own = lax.optimization_barrier((both_rows, down_grad_own))
    both_grad = scatter_col([both_rows[None]], 5)[0][0]
    key_grad, value_grad = both_grad[:, : KVH * HD], both_grad[:, KVH * HD :]
    query_wide = query_grad.reshape(own_rows, HQ, HD).astype(F32)
    query_base_grad = (
        rotate_back(query_wide, cosines, sines).reshape(own_rows, HQ * HD).astype(BF16)
    )
    key_wide = rounded_wide(key_grad.reshape(own_rows, KVH, HD))
    key_base_grad = (
        rotate_back(key_wide, cosines, sines).reshape(own_rows, KVH * HD).astype(BF16)
    )
    value_base_grad = value_grad.astype(BF16)
    query_b_grad = jnp.sum(query_base_grad.astype(F32), axis=0)
    key_b_grad = jnp.sum(key_base_grad.astype(F32), axis=0)
    value_b_grad = jnp.sum(value_base_grad.astype(F32), axis=0)
    first_normed_grad = (
        dot_nn(query_base_grad, query_t)
        + dot_nn(key_base_grad, key_t)
        + dot_nn(value_base_grad, value_t)
    )
    first_gain_grad = jnp.sum(first_normed_grad * first_unit, axis=0)
    first_unit_grad = first_normed_grad * first_gain.astype(F32)
    input_grad = residual_grad + first_rms * (
        first_unit_grad
        - first_unit * jnp.mean(first_unit_grad * first_unit, axis=-1, keepdims=True)
    )
    small_grads = (query_b_grad, key_b_grad, value_b_grad, first_gain_grad, second_gain_grad)
    small_flat = jnp.concatenate(
        [member.reshape(row_parts * col_parts, -1) for member in small_grads], axis=1
    )
    small_flat = jnp.pad(
        small_flat, ((0, 0), (0, k_own * depth_own - small_flat.shape[1]))
    ).reshape(row_parts, col_parts, k_own, depth_own)
    small_flat = small_flat.transpose(1, 2, 0, 3).reshape(col_parts * k_own, depth)
    query_w = dot_tn(query_base_grad, first_normed).astype(BF16)
    query_w, gate_grad_own = lax.optimization_barrier((query_w, gate_grad_own))
    query_w_out, output_w_out, key_w_out, value_w_out, small_out = scatter_weights(
        [
            query_w,
            dot_tn(attended_grad, mixed).astype(BF16),
            dot_tn(key_base_grad, first_normed).astype(BF16),
            dot_tn(value_base_grad, first_normed).astype(BF16),
            small_flat.astype(BF16),
        ],
        6,
    )
    small_out = small_out.reshape(-1)
    small_list, offset = [], 0
    for size in small_sizes:
        small_list.append(small_out[offset : offset + size])
        offset += size
    return (
        layer_out,
        input_grad,
        small_list[3],
        query_w_out.T,
        small_list[0],
        key_w_out.T,
        small_list[1],
        value_w_out.T,
        small_list[2],
        output_w_out.T,
        small_list[4],
        gate_grad_own.astype(F32),
        up_grad_own.astype(F32),
        down_grad_own.astype(F32).T,
    )


def solution(mesh):
    in_specs = (
        P(("row", "col"), None),
        P(("row", "col"), None),
        P("row", None),
        P(("row", "col")),
        P("row", "col"),
        P(("row", "col")),
        P("row", "col"),
        P(("row", "col")),
        P("row", "col"),
        P(("row", "col")),
        P("row", "col"),
        P(("row", "col")),
        P("row", "col"),
        P("row", "col"),
        P("col", "row"),
    )
    out_specs = (
        P(("row", "col"), None),
        P(("row", "col"), None),
        P(("row", "col")),
        P("row", "col"),
        P(("row", "col")),
        P("row", "col"),
        P(("row", "col")),
        P("row", "col"),
        P(("row", "col")),
        P("row", "col"),
        P(("row", "col")),
        P("row", "col"),
        P("row", "col"),
        P("col", "row"),
    )
    return jax.shard_map(shards, mesh=mesh, in_specs=in_specs, out_specs=out_specs, check_vma=False)
```
